128 devices in a mesh: row: 2 (over x_lo), circ: 16 (over z, y), rad: 4 (over x_hi, core).
Axes of the slice: x: 4 (x_hi: 2, x_lo: 2; x = x_hi * 2 + x_lo), y: 4, z: 4, core: 2. Of those that a mesh axis runs over, the one named last changes fastest.
Arguments:
- state: float32 [2, 5, 512, 64, 512], P('row', None, 'circ', 'rad'), as said below
- time_source: float32 [2, 5, 512, 64, 512], P('row', None, 'circ', 'rad'), may hold values from -3 to 3
- pseudo_step: float32 [2, 512, 64, 512], P('row', 'circ', 'rad'), may hold values from 0.05 to 0.5
- offsets: int32 [64], P('rad'), may hold values from 0 to 511
- weights: float32 [64], P('rad'), may hold values from 0 to 1
Outputs:
- increment: float32 [2, 5, 512, 64, 512], P('row', None, 'circ', 'rad')
The draws below stay inside these ranges and needn't reach their ends.
Inputs may be any that keep to these rules, and one draw needn't show every extreme that they name: In every cell the density lies between 0.5 and 1.5 and the pressure computed from the state between 0.6 and 1.1.
All inputs are finite; a program needn't handle non-finite values.
Results may differ from the reference program's by a relative error of at most 0.000057.
Values sent between devices are 32-bit elements; how exact they have to be, the bound alone decides.
No kernel may reach another device: no remote copies, remote signals or barrier semaphores. Data moves between devices by JAX's collectives and lax.ppermute only.
A program may use at most 128 MiB of HBM per device.

```python
import math
import jax
import jax.numpy as jnp
import numpy as np
from jax import lax

CA = 512
SWEEPS = 2
NT = 512
NR = 64
N_ROW = 2


def draw_state(key, part):
    keys = jax.random.split(jax.random.fold_in(key, 11), 5)
    shape = (N_ROW, NT, NR, CA)
    density = jax.random.uniform(keys[0], shape, jnp.float32, 0.6, 1.4)
    pressure = 0.9 * (1.0 + 0.1 * jax.random.uniform(keys[1], shape, jnp.float32, -1.0, 1.0))
    axial_speed = 0.4 + 0.2 * jax.random.uniform(keys[2], shape, jnp.float32, -1.0, 1.0)
    swirl_speed = 0.2 * jax.random.truncated_normal(keys[3], -3.0, 3.0, shape, jnp.float32)
    radial_speed = 0.1 * jax.random.truncated_normal(keys[4], -3.0, 3.0, shape, jnp.float32)
    energy = pressure / 0.4 + 0.5 * density * (axial_speed * axial_speed + swirl_speed * swirl_speed + radial_speed * radial_speed)
    return jnp.stack([density, density * axial_speed, density * swirl_speed, density * radial_speed, energy], axis=1)


def draw_offsets(key, part):
    spacing = NT // NR
    base = jax.random.randint(jax.random.fold_in(key, 23), (1,), 0, NT, dtype=jnp.int32)
    jitter = jax.random.randint(jax.random.fold_in(key, 29), (NR,), 0, spacing, dtype=jnp.int32)
    strips = jnp.arange(NR, dtype=jnp.int32) * spacing
    return ((base + strips + jitter) % NT).astype(jnp.int32)


def draw_weights(key, part):
    fraction = jax.random.uniform(jax.random.fold_in(key, 37), (NR,), jnp.float32, 0.2, 0.8)
    return fraction.astype(jnp.float32)


def levels(own_key, dims, cuts, low, high):
    level = 1.0
    for axis_at, shards_of in cuts:
        draws = jax.random.uniform(jax.random.fold_in(jax.random.fold_in(own_key, 6), axis_at), (shards_of,), jnp.float32, low / len(cuts), high / len(cuts))
        level = level * jnp.repeat(jnp.exp(draws), dims[axis_at] // shards_of).reshape((-1,) + (1,) * (len(dims) - 1 - axis_at))
    return level


def normal_values(stream_key, dims, spread, bound, shards=(), kind=jnp.bfloat16):
    gain = levels(stream_key, dims, shards, -0.22, 0.18) if shards else 1.0
    entries = jax.random.normal(stream_key, dims, jnp.float32) * spread * gain
    return jnp.minimum(jnp.maximum(entries, -bound), bound).astype(kind)


def setup_inputs(seed: int = 0) -> dict:
    streams_of = jax.random.split(jax.random.key(seed), 6)
    state = draw_state(jax.random.fold_in(streams_of[5], 71), 0)
    time_source = normal_values(streams_of[1], (N_ROW, 5, NT, NR, CA), 0.5, 3.0, ((0, 2), (2, 16), (3, 4)), jnp.float32)
    pseudo_step = jnp.clip(jnp.exp(math.log(0.5) - 2.3025851 * jax.random.uniform(streams_of[2], (N_ROW, NT, NR, CA), jnp.float32) ** levels(streams_of[2], (N_ROW, NT, NR, CA), ((0, 2), (1, 16), (2, 4)), -0.2, 0.2)), 0.05, 0.5)
    offsets = draw_offsets(jax.random.fold_in(streams_of[5], 71), 0)
    weights = draw_weights(jax.random.fold_in(streams_of[5], 71), 0)
    return dict(state=state, time_source=time_source, pseudo_step=pseudo_step, offsets=offsets, weights=weights)


GAMMA = 1.4
GAMMA_LESS = 0.4
SECOND_COEF = 0.5
FOURTH_COEF = 0.03125
RATE = 0.75
GRID_SPEED = 0.5
AXIAL_COUPLING = 0.8
CIRC_COUPLING = 0.6
RADIAL_COUPLING = 0.6

def axial_table(length):
    modes_index = np.arange(1, length + 1) * 1.0
    angle = np.pi / (length + 1)
    modes = np.sin(np.outer(modes_index, modes_index) * angle)
    eigen = 1.0 + 2.0 * AXIAL_COUPLING - 2.0 * AXIAL_COUPLING * np.cos(modes_index * angle)
    return modes / eigen[None, :] @ modes.T * (2.0 / (length + 1))

def slab_cut(field, start_at, length, direction):
    return lax.slice_in_dim(field, start_at, start_at + length, axis=direction)

def flux_balance(margin, direction, component, grid_speed):
    length = margin.shape[direction] - 4
    density = margin[0]
    velocity = margin[1:4] / density
    pressure = GAMMA_LESS * (margin[4] - 0.5 * density * (velocity[0] * velocity[0] + velocity[1] * velocity[1] + velocity[2] * velocity[2]))
    normal = velocity[component - 1]
    relative = normal - grid_speed
    radius = jnp.abs(relative) + jnp.sqrt(GAMMA * pressure / density)
    fluxes = margin * relative
    fluxes = fluxes.at[component].add(pressure)
    fluxes = fluxes.at[4].add(pressure * normal)
    upper_p = slab_cut(pressure, 2, length + 2, direction)
    middle_p = slab_cut(pressure, 1, length + 2, direction)
    lower_p = slab_cut(pressure, 0, length + 2, direction)
    sensor = jnp.abs(upper_p - 2.0 * middle_p + lower_p) / (upper_p + 2.0 * middle_p + lower_p)
    second_coef = SECOND_COEF * jnp.maximum(slab_cut(sensor, 0, length + 1, direction), slab_cut(sensor, 1, length + 1, direction))
    fourth_coef = jnp.maximum(0.0, FOURTH_COEF - second_coef)
    face_speed = 0.5 * (slab_cut(radius, 1, length + 1, direction) + slab_cut(radius, 2, length + 1, direction))
    before_cell = slab_cut(margin, 0, length + 1, direction)
    near_cell = slab_cut(margin, 1, length + 1, direction)
    far_cell = slab_cut(margin, 2, length + 1, direction)
    beyond_cell = slab_cut(margin, 3, length + 1, direction)
    first_jump = far_cell - near_cell
    third_jump = beyond_cell - 3.0 * far_cell + 3.0 * near_cell - before_cell
    face_flux = 0.5 * (slab_cut(fluxes, 1, length + 1, direction) + slab_cut(fluxes, 2, length + 1, direction)) - face_speed * (second_coef * first_jump - fourth_coef * third_jump)
    return slab_cut(face_flux, 1, length, direction) - slab_cut(face_flux, 0, length, direction)

def jacobi(field, direction, coupling):
    length = field.shape[direction] - 2
    centre = slab_cut(field, 1, length, direction)
    return (centre + coupling * (slab_cut(field, 2, length, direction) + slab_cut(field, 0, length, direction))) / (1.0 + 2.0 * coupling)

def pick_cells(face, index_table):
    return jnp.take_along_axis(face, jnp.broadcast_to(index_table[None, :, :, None], face.shape), axis=1)

def row_update(packed):
    cells, left_rim, right_rim, grid_speed, pseudo, source = packed
    mirror_sign = jnp.array([1.0, 1.0, 1.0, -1.0, 1.0], jnp.float32)[:, None, None, None]
    circ_margin = jnp.concatenate([cells[:, NT - 2:], cells, cells[:, :2]], axis=1)
    lower_rim = jnp.flip(cells[:, :, 0:2], axis=2) * mirror_sign
    upper_rim = jnp.flip(cells[:, :, NR - 2:], axis=2) * mirror_sign
    radial_margin = jnp.concatenate([lower_rim, cells, upper_rim], axis=2)
    axial_margin = jnp.concatenate([left_rim, cells, right_rim], axis=3)
    balance = flux_balance(axial_margin, -1, 1, 0.0) + flux_balance(circ_margin, -3, 2, grid_speed) + flux_balance(radial_margin, -2, 3, 0.0)
    increment_raw = -(pseudo[None] * (balance + RATE * cells + source))
    inverse = jnp.asarray(axial_table(CA), dtype=jnp.float32)
    smooth = jnp.dot(increment_raw.reshape(-1, CA), inverse, precision=lax.Precision.HIGHEST, preferred_element_type=jnp.float32).reshape(increment_raw.shape)
    for _ in range(SWEEPS):
        widened = jnp.concatenate([smooth[:, NT - 1:], smooth, smooth[:, :1]], axis=1)
        smooth = jacobi(widened, -3, CIRC_COUPLING)
    for _ in range(SWEEPS):
        widened = jnp.pad(smooth, ((0, 0), (0, 0), (1, 1), (0, 0)))
        smooth = jacobi(widened, -2, RADIAL_COUPLING)
    return smooth

def reference(state, time_source, pseudo_step, offsets, weights):
    stator_face = state[0, :, :, :, CA - 2:]
    rotor_face = state[1, :, :, :, :2]
    theta_cells = jnp.arange(NT, dtype=jnp.int32)[:, None]
    offset_row = offsets.astype(jnp.int32)[None, :]
    weight_row = weights[None, :]
    rotor_first = (theta_cells + offset_row) % NT
    rotor_second = (theta_cells + offset_row + 1) % NT
    stator_first = (theta_cells - offset_row - 1) % NT
    stator_second = (theta_cells - offset_row) % NT
    rotor_ghost = (1.0 - weight_row)[None, :, :, None] * pick_cells(stator_face, rotor_first) + weight_row[None, :, :, None] * pick_cells(stator_face, rotor_second)
    stator_ghost = weight_row[None, :, :, None] * pick_cells(rotor_face, stator_first) + (1.0 - weight_row)[None, :, :, None] * pick_cells(rotor_face, stator_second)
    stator_edge = jnp.concatenate([state[0, :, :, :, :1], state[0, :, :, :, :1]], axis=3)
    rotor_edge = jnp.concatenate([state[1, :, :, :, CA - 1:], state[1, :, :, :, CA - 1:]], axis=3)
    left_rims = jnp.stack([stator_edge, rotor_ghost])
    right_rims = jnp.stack([stator_ghost, rotor_edge])
    speeds = jnp.array([0.0, GRID_SPEED], jnp.float32)
    return lax.map(row_update, (state, left_rims, right_rims, speeds, pseudo_step, time_source))
```

```python
import functools

import jax
import jax.numpy as jnp
import numpy as np
from jax import lax
from jax.experimental import pallas as pl
from jax.experimental.pallas import tpu as pltpu
from jax.sharding import PartitionSpec as P

GAMMA = 1.4
GAMMA_LESS = 0.4
SECOND_COEF = 0.5
FOURTH_COEF = 0.03125
RATE = 0.75
GRID_SPEED = 0.5
AXIAL_COUPLING = 0.8
CIRC_COUPLING = 0.6
RADIAL_COUPLING = 0.6

NCOMP = 5
LANES = 128
ROWS = 32
FIRST = 8
MIB = 1 << 20


def axial_table(length):
    modes_index = np.arange(1, length + 1) * 1.0
    angle = np.pi / (length + 1)
    modes = np.sin(np.outer(modes_index, modes_index) * angle)
    eigen = 1.0 + 2.0 * AXIAL_COUPLING - 2.0 * AXIAL_COUPLING * np.cos(modes_index * angle)
    return modes / eigen[None, :] @ modes.T * (2.0 / (length + 1))


def vmem():
    return pl.BlockSpec(memory_space=pltpu.VMEM)


def smem():
    return pl.BlockSpec(memory_space=pltpu.SMEM)


def hbm():
    return pl.BlockSpec(memory_space=pl.ANY)


def lane_index(rows):
    return lax.broadcasted_iota(jnp.int32, (rows, LANES), 1)


def edges_kernel(flags, state, rad_low, rad_high, circ_low, circ_high, face, buf, sems):
    planes = state.shape[1]
    chunks = state.shape[3] // LANES
    group = 8
    copies = []
    for g in range(planes // group):
        copy = pltpu.make_async_copy(
            state.at[:, pl.ds(g * group, group)], buf.at[:, pl.ds(g * group, group)], sems.at[g]
        )
        copy.start()
        copies.append(copy)
    rotor = flags[2]
    lane = lane_index(8)
    sub = lax.broadcasted_iota(jnp.int32, (8, LANES), 0)
    for g in range(planes // group):
        copies[g].wait()

        def body(j, carry):
            for m in range(NCOMP):
                for c in range(chunks):
                    cols = pl.ds(c * LANES, LANES)
                    rad_low[m, j, pl.ds(2 * c, 2), :] = buf[m, j, 0:2, cols]
                    rad_high[m, j, pl.ds(2 * c, 2), :] = buf[m, j, 14:16, cols]
            for h in range(2):
                total = jnp.zeros((8, LANES), jnp.float32)
                for m in range(NCOMP):
                    front = buf[m, j, 8 * h : 8 * h + 8, 0:LANES]
                    back = buf[m, j, 8 * h : 8 * h + 8, (chunks - 1) * LANES : chunks * LANES]
                    first = pltpu.roll(front, 2 * m, 1, stride=16, stride_axis=0)
                    last = pltpu.roll(back, 2 * m + 2, 1, stride=16, stride_axis=0)
                    moved = jnp.where(rotor == 1, first, last)
                    at = lane - sub * 16 - 2 * m
                    total = jnp.where((at >= 0) & (at < 2), moved, total)
                face[h, pl.ds(j, 1), :] = jnp.sum(total, axis=0, keepdims=True)
            return carry

        lax.fori_loop(g * group, (g + 1) * group, body, 0)
    circ_low[...] = buf[:, 0:2]
    circ_high[...] = buf[:, planes - 2 : planes]


def edges(flags, cells):
    planes, rows, length = cells.shape[1:]
    rad = jax.ShapeDtypeStruct((NCOMP, planes, 8, LANES), jnp.float32)
    circ = jax.ShapeDtypeStruct((NCOMP, 2, rows, length), jnp.float32)
    face = jax.ShapeDtypeStruct((2, planes, LANES), jnp.float32)
    return pl.pallas_call(
        edges_kernel,
        out_shape=(rad, rad, circ, circ, face),
        in_specs=[smem(), hbm()],
        out_specs=(vmem(),) * 5,
        scratch_shapes=[pltpu.VMEM(cells.shape, jnp.float32), pltpu.SemaphoreType.DMA((4,))],
        compiler_params=pltpu.CompilerParams(vmem_limit_bytes=24 * MIB),
        name="state_edges",
    )(flags, cells)


def primitives(cons):
    inverse = 1.0 / cons[0]
    velocity = [cons[m] * inverse for m in (1, 2, 3)]
    kinetic = cons[1] * velocity[0] + cons[2] * velocity[1] + cons[3] * velocity[2]
    pressure = GAMMA_LESS * (cons[4] - 0.5 * kinetic)
    square = GAMMA * pressure * inverse
    sound = square * lax.rsqrt(square)
    return [pressure, sound, *velocity]


def sensor_of(upper, middle, lower):
    outer = upper + lower
    twice = 2.0 * middle
    return jnp.abs(outer - twice) / (outer + twice)


def face_flux(component, cons, pressure, sound, velocity, sensor, grid_speed):
    half = [0.5 * (v - grid_speed) if grid_speed is not None else 0.5 * v for v in velocity]
    speed = jnp.abs(half[0]) + jnp.abs(half[1]) + 0.5 * (sound[0] + sound[1])
    second = SECOND_COEF * jnp.maximum(sensor[0], sensor[1])
    fourth = jnp.maximum(0.0, FOURTH_COEF - second)
    outer = speed * fourth
    inner = speed * (second + 3.0 * fourth)
    near = half[0] + inner
    far = half[1] - inner
    fluxes = []
    for m in range(NCOMP):
        before, left, right, beyond = cons[m]
        flux = right * far + left * near + outer * (beyond - before)
        if m == component:
            flux = flux + 0.5 * (pressure[0] + pressure[1])
        if m == 4:
            flux = flux + 0.5 * (pressure[0] * velocity[0] + pressure[1] * velocity[1])
        fluxes.append(flux)
    return fluxes


def flux_kernel(
    flags,
    starts,
    lead_weight,
    trail_weight,
    state,
    source,
    pseudo,
    circ_low,
    circ_high,
    rad_low,
    rad_high,
    plane,
    table_high,
    table_low,
    out,
    out_circ_low,
    out_circ_high,
    out_rad_low,
    out_rad_high,
    cons,
    prim,
    src,
    step,
    raw_high,
    raw_low,
    result,
    tables,
    halo_low,
    halo_high,
    cycle,
    ghosts,
    circ_flux,
    circ_sensor,
    rad_flux,
    sems,
):
    planes = state.shape[1]
    chunks = state.shape[3] // LANES
    group = 8
    groups = planes // group
    cells = pl.ds(FIRST, 16)

    def start(a, b, s):
        copy = pltpu.make_async_copy(a, b, s)
        copy.start()
        return copy

    loads = []
    for g in range(groups):
        part = [
            start(
                state.at[:, pl.ds(g * group, group), :, pl.ds(c * LANES, LANES)],
                cons.at[:, pl.ds(2 + g * group, group), c, cells, :],
                sems.at[g * chunks + c],
            )
            for c in range(chunks)
        ]
        loads.append(part)
    k = groups * chunks
    halos = []
    for c in range(chunks):
        cols = pl.ds(c * LANES, LANES)
        halos.append(start(circ_low.at[:, :, :, cols], cons.at[:, 0:2, c, cells, :], sems.at[k]))
        halos.append(
            start(
                circ_high.at[:, :, :, cols],
                cons.at[:, planes + 2 : planes + 4, c, cells, :],
                sems.at[k + 1],
            )
        )
        k += 2
    halos.append(start(rad_low, halo_low, sems.at[k]))
    halos.append(start(rad_high, halo_high, sems.at[k + 1]))
    k += 2
    late = [
        start(pseudo, step, sems.at[k]),
        start(source, src, sems.at[k + 1]),
        start(table_high, tables.at[0], sems.at[k + 2]),
        start(table_low, tables.at[1], sems.at[k + 3]),
    ]
    k += 4

    rotor = flags[2]
    lane8 = lane_index(8)
    lane = lane_index(16)

    count = plane.shape[0]
    width = plane.shape[2]
    for h in range(2):
        for s in range(count):
            cycle[h, pl.ds(s * width, width), :] = plane[s, h]
        cycle[h, pl.ds(count * width, width), :] = plane[0, h]
        cycle[h, pl.ds((count + 1) * width, 8), :] = plane[1, h, 0:8]
    for h in range(2):
        for jt in range(planes // 8):
            total = jnp.zeros((8, LANES), jnp.float32)
            for r in range(8):
                at = starts[8 * h + r] + 8 * jt
                value = (
                    lead_weight[8 * h + r] * cycle[h, pl.ds(at, 8), :]
                    + trail_weight[8 * h + r] * cycle[h, pl.ds(at + 1, 8), :]
                )
                to = (8 - r) % 8
                if to != r:
                    value = pltpu.roll(value, (to - r) % 8 * 16, 1)
                total = jnp.where(lane8 // 16 == to, value, total)
            ghosts[h, pl.ds(8 * jt, 8), :] = jnp.where(
                rotor == 1, pltpu.roll(total, LANES - 2, 1), total
            )

    for part in loads:
        for copy in part:
            copy.wait()
    for copy in halos:
        copy.wait()

    def mirror(edge, first):
        def body(j, carry):
            for m in range(NCOMP):
                for c in range(chunks):
                    a = cons[m, j + 2, c, pl.ds(first, 1), :]
                    b = cons[m, j + 2, c, pl.ds(first + 1, 1), :]
                    if m == 3:
                        a, b = -a, -b
                    edge[m, j, pl.ds(2 * c, 1), :] = b
                    edge[m, j, pl.ds(2 * c + 1, 1), :] = a
            return carry

        lax.fori_loop(0, planes, body, 0)

    @pl.when(flags[0] == 1)
    def _():
        mirror(halo_low, FIRST)

    @pl.when(flags[1] == 1)
    def _():
        mirror(halo_high, FIRST + 14)

    def prepare(j, carry):
        for c in range(chunks):
            fields = primitives([cons[m, j, c, cells, :] for m in range(NCOMP)])
            for f in range(NCOMP):
                prim[f, j, c, cells, :] = fields[f]
        return carry

    lax.fori_loop(0, planes + 4, prepare, 0)

    def prepare_halo(j, carry):
        for edge, row in ((halo_low, FIRST - 2), (halo_high, FIRST + 16)):
            packed = [edge[m, j] for m in range(NCOMP)]
            fields = primitives(packed)
            for c in range(chunks):
                for m in range(NCOMP):
                    cons[m, j + 2, c, pl.ds(row, 2), :] = edge[m, j, pl.ds(2 * c, 2), :]
                    prim[m, j + 2, c, pl.ds(row, 2), :] = fields[m][2 * c : 2 * c + 2]
        return carry

    lax.fori_loop(0, planes, prepare_halo, 0)
    for copy in late:
        copy.wait()

    spin = GRID_SPEED * rotor.astype(jnp.float32)

    def circ_face(j, c, sensor_before):
        p = [prim[0, j + d, c, cells, :] for d in (0, 1, 2)]
        sensor = sensor_of(p[2], p[1], p[0])
        flux = face_flux(
            2,
            [[cons[m, j + d, c, cells, :] for d in (-1, 0, 1, 2)] for m in range(NCOMP)],
            p[:2],
            [prim[1, j + d, c, cells, :] for d in (0, 1)],
            [prim[3, j + d, c, cells, :] for d in (0, 1)],
            [sensor_before, sensor],
            spin,
        )
        return flux, sensor

    for c in range(chunks):
        p = [prim[0, d, c, cells, :] for d in (0, 1, 2)]
        flux, sensor = circ_face(1, c, sensor_of(p[2], p[1], p[0]))
        circ_sensor[c] = sensor
        for m in range(NCOMP):
            circ_flux[m, c] = flux[m]

    ghost_lanes = jnp.where(lane < 64, 1 - rotor, rotor) == 1

    def behind(parts, by):
        turned = [pltpu.roll(x, by, 1) for x in parts]
        return [jnp.where(lane < by, turned[c - 1], turned[c]) for c in range(chunks + 1)]

    def ahead(parts):
        turned = [pltpu.roll(x, LANES - 1, 1) for x in parts]
        return [
            jnp.where(lane < LANES - 1, turned[c], turned[(c + 1) % (chunks + 1)])
            for c in range(chunks + 1)
        ]

    def plane_body(j, carry):
        at = j + 2
        spread = jnp.concatenate(
            [
                pltpu.roll(
                    jnp.broadcast_to(ghosts[h, pl.ds(j, 1), :], (8, LANES)),
                    0,
                    1,
                    stride=16,
                    stride_axis=0,
                )
                for h in range(2)
            ],
            axis=0,
        )
        axial = []
        for m in range(NCOMP):
            parts = [cons[m, at, c, cells, :] for c in range(chunks)]
            moved = pltpu.roll(spread, LANES - 2 * m, 1) if m else spread
            edge = jnp.where(
                rotor == 1,
                jnp.broadcast_to(parts[chunks - 1][:, LANES - 1 : LANES], (16, LANES)),
                jnp.broadcast_to(parts[0][:, 0:1], (16, LANES)),
            )
            parts.append(jnp.where(ghost_lanes, moved, edge))
            axial.append(parts)
        fields = [[prim[f, at, c, cells, :] for c in range(chunks)] for f in (0, 1, 2)]
        extra = primitives([axial[m][chunks] for m in range(NCOMP)])
        for f in range(3):
            fields[f].append(extra[f])
        p, sound, speed = fields
        p_before = behind(p, 1)
        p_after = ahead(p)
        sensor = [sensor_of(p_after[c], p[c], p_before[c]) for c in range(chunks + 1)]
        sensor_before = behind(sensor, 1)
        sound_before = behind(sound, 1)
        speed_before = behind(speed, 1)
        shifted = [(behind(x, 2), behind(x, 1), x, ahead(x)) for x in axial]
        axial_flux = [
            face_flux(
                1,
                [[shifted[m][d][c] for d in range(4)] for m in range(NCOMP)],
                [p_before[c], p[c]],
                [sound_before[c], sound[c]],
                [speed_before[c], speed[c]],
                [sensor_before[c], sensor[c]],
                None,
            )
            for c in range(chunks + 1)
        ]
        balance = []
        for m in range(NCOMP):
            parts = [axial_flux[c][m] for c in range(chunks + 1)]
            upper = ahead(parts)
            balance.append([upper[c] - parts[c] for c in range(chunks)])

        for c in range(chunks):
            flux, sensor_next = circ_face(at, c, circ_sensor[c])
            circ_sensor[c] = sensor_next
            def rows(ref, f, d):
                return ref[f, at, c, pl.ds(FIRST + d, 24 if d < 1 else 23), :]

            tall = pl.ds(FIRST - 0, 24)
            pressures = [prim[0, at, c, pl.ds(FIRST + d, 17), :] for d in (-2, -1, 0, 1)]
            radial = face_flux(
                3,
                [
                    [cons[m, at, c, pl.ds(FIRST + d, 17), :] for d in (-2, -1, 0, 1)]
                    for m in range(NCOMP)
                ],
                pressures[1:3],
                [prim[1, at, c, pl.ds(FIRST + d, 17), :] for d in (-1, 0)],
                [prim[4, at, c, pl.ds(FIRST + d, 17), :] for d in (-1, 0)],
                [
                    sensor_of(pressures[2], pressures[1], pressures[0]),
                    sensor_of(pressures[3], pressures[2], pressures[1]),
                ],
                None,
            )
            pace = step[j, :, pl.ds(c * LANES, LANES)]
            for m in range(NCOMP):
                rad_flux[m, c, 0:17, :] = radial[m]
                total = balance[m][c] + (flux[m] - circ_flux[m, c])
                circ_flux[m, c] = flux[m]
                total = total + (rad_flux[m, c, pl.ds(1, 16), :] - rad_flux[m, c, pl.ds(0, 16), :])
                raw = pace * (
                    total + RATE * cons[m, at, c, cells, :] + src[m, j, :, pl.ds(c * LANES, LANES)]
                )
                high = raw.astype(jnp.bfloat16)
                raw_high[m, j, :, pl.ds(c * LANES, LANES)] = high
                raw_low[m, j, :, pl.ds(c * LANES, LANES)] = (raw - high.astype(jnp.float32)).astype(
                    jnp.bfloat16
                )
        return carry

    lax.fori_loop(0, planes, plane_body, 0)

    def solve(q, carry):
        length = chunks * LANES
        for m in range(NCOMP):
            high = raw_high[m, pl.ds(q * 8, 8)].reshape(128, length)
            low = raw_low[m, pl.ds(q * 8, 8)].reshape(128, length)
            value = (
                jnp.dot(high, tables[0], preferred_element_type=jnp.float32)
                + jnp.dot(high, tables[1], preferred_element_type=jnp.float32)
                + jnp.dot(low, tables[0], preferred_element_type=jnp.float32)
            )
            result[m, pl.ds(q * 8, 8)] = value.reshape(8, 16, length)
        return carry

    lax.fori_loop(0, planes // 8, solve, 0)

    stores = [
        start(result, out, sems.at[k]),
        start(result.at[:, 0:2], out_circ_low, sems.at[k + 1]),
        start(result.at[:, planes - 2 : planes], out_circ_high, sems.at[k + 2]),
    ]

    def pick(j, carry):
        for m in range(NCOMP):
            for c in range(chunks):
                cols = pl.ds(c * LANES, LANES)
                out_rad_low[m, j, pl.ds(2 * c, 2), :] = result[m, j, 0:2, cols]
                out_rad_high[m, j, pl.ds(2 * c, 2), :] = result[m, j, 14:16, cols]
        return carry

    lax.fori_loop(0, planes, pick, 0)
    for copy in stores:
        copy.wait()


def fluxes(flags, starts, lead, trail, cells, source, pseudo, halos, plane):
    planes, rows, length = cells.shape[1:]
    chunks = length // LANES
    table = -axial_table(length).astype(np.float32)
    table_high = table.astype(jnp.bfloat16)
    table_low = (table - table_high.astype(np.float32)).astype(jnp.bfloat16)
    f32 = jnp.float32
    rad = jax.ShapeDtypeStruct((NCOMP, planes, 8, LANES), f32)
    circ = jax.ShapeDtypeStruct((NCOMP, 2, rows, length), f32)
    groups = planes // 8
    return pl.pallas_call(
        flux_kernel,
        out_shape=(jax.ShapeDtypeStruct(cells.shape, f32), circ, circ, rad, rad),
        in_specs=[smem()] * 4 + [hbm()] * 7 + [vmem()] + [hbm()] * 2,
        out_specs=(hbm(),) * 3 + (vmem(),) * 2,
        scratch_shapes=[
            pltpu.VMEM((NCOMP, planes + 4, chunks, ROWS, LANES), f32),
            pltpu.VMEM((NCOMP, planes + 4, chunks, ROWS, LANES), f32),
            pltpu.VMEM(cells.shape, f32),
            pltpu.VMEM(pseudo.shape, f32),
            pltpu.VMEM(cells.shape, jnp.bfloat16),
            pltpu.VMEM(cells.shape, jnp.bfloat16),
            pltpu.VMEM(cells.shape, f32),
            pltpu.VMEM((2, length, length), jnp.bfloat16),
            pltpu.VMEM((NCOMP, planes, 8, LANES), f32),
            pltpu.VMEM((NCOMP, planes, 8, LANES), f32),
            pltpu.VMEM((2, plane.shape[0] * planes + planes + 8, LANES), f32),
            pltpu.VMEM((2, planes, LANES), f32),
            pltpu.VMEM((NCOMP, chunks, rows, LANES), f32),
            pltpu.VMEM((chunks, rows, LANES), f32),
            pltpu.VMEM((NCOMP, chunks, 24, LANES), f32),
            pltpu.SemaphoreType.DMA((groups * chunks + 2 * chunks + 9,)),
        ],
        compiler_params=pltpu.CompilerParams(vmem_limit_bytes=58 * MIB),
        name="row_fluxes",
    )(
        flags,
        starts,
        lead,
        trail,
        cells,
        source,
        pseudo,
        *halos,
        plane,
        jnp.asarray(table_high),
        jnp.asarray(table_low),
    )


def smooth_kernel(flags, field, circ_low, circ_high, rad_low, rad_high, ll, lh, hl, hh, out, buf, mid, done, sems):
    planes = field.shape[1]
    chunks = field.shape[3] // LANES
    cells = pl.ds(FIRST, 16)
    group = 8

    def start(a, b, s):
        copy = pltpu.make_async_copy(a, b, s)
        copy.start()
        return copy

    copies = []
    k = 0
    for c in range(chunks):
        cols = pl.ds(c * LANES, LANES)
        copies.append(start(field.at[:, :, :, cols], buf.at[:, 2 : planes + 2, c, cells, :], sems.at[k]))
        copies.append(start(circ_low.at[:, :, :, cols], buf.at[:, 0:2, c, cells, :], sems.at[k + 1]))
        copies.append(
            start(circ_high.at[:, :, :, cols], buf.at[:, planes + 2 : planes + 4, c, cells, :], sems.at[k + 2])
        )
        k += 3

    def put(low, high, first, count):
        def body(j, carry):
            for m in range(NCOMP):
                for c in range(chunks):
                    buf[m, first + j, c, pl.ds(FIRST - 2, 2), :] = low[m, j, pl.ds(2 * c, 2), :]
                    buf[m, first + j, c, pl.ds(FIRST + 16, 2), :] = high[m, j, pl.ds(2 * c, 2), :]
            return carry

        lax.fori_loop(0, count, body, 0)

    put(rad_low, rad_high, 2, planes)
    put(ll, lh, 0, 2)
    put(hl, hh, planes + 2, 2)
    for copy in copies:
        copy.wait()

    def wall(zero_row, odd_row, from_row):
        def body(j, carry):
            for m in range(NCOMP):
                for c in range(chunks):
                    buf[m, j, c, pl.ds(zero_row, 1), :] = jnp.zeros((1, LANES), jnp.float32)
                    buf[m, j, c, pl.ds(odd_row, 1), :] = -buf[m, j, c, pl.ds(from_row, 1), :]
            return carry

        lax.fori_loop(0, planes + 4, body, 0)

    @pl.when(flags[0] == 1)
    def _():
        wall(FIRST - 1, FIRST - 2, FIRST)

    @pl.when(flags[1] == 1)
    def _():
        wall(FIRST + 16, FIRST + 17, FIRST + 15)

    def weights(coupling):
        own = 1.0 / (1.0 + 2.0 * coupling)
        side = coupling / (1.0 + 2.0 * coupling)
        return own * own + 2.0 * side * side, 2.0 * own * side, side * side

    def radial(j, carry):
        w0, w1, w2 = weights(RADIAL_COUPLING)
        for m in range(NCOMP):
            for c in range(chunks):
                x = [buf[m, j, c, pl.ds(FIRST + d, 16), :] for d in (-2, -1, 0, 1, 2)]
                mid[m, j, c] = w0 * x[2] + w1 * (x[1] + x[3]) + w2 * (x[0] + x[4])
        return carry

    lax.fori_loop(0, planes + 4, radial, 0)

    def around(j, carry):
        w0, w1, w2 = weights(CIRC_COUPLING)
        for m in range(NCOMP):
            for c in range(chunks):
                x = [mid[m, j + d, c] for d in range(5)]
                done[m, j, :, pl.ds(c * LANES, LANES)] = (
                    w0 * x[2] + w1 * (x[1] + x[3]) + w2 * (x[0] + x[4])
                )
        return carry

    stores = []
    for g in range(planes // group):
        lax.fori_loop(g * group, (g + 1) * group, around, 0)
        stores.append(
            start(done.at[:, pl.ds(g * group, group)], out.at[:, pl.ds(g * group, group)], sems.at[k])
        )
        k += 1
    for copy in stores:
        copy.wait()


def smoothed(flags, field, halos):
    planes, rows, length = field.shape[1:]
    chunks = length // LANES
    f32 = jnp.float32
    return pl.pallas_call(
        smooth_kernel,
        out_shape=jax.ShapeDtypeStruct(field.shape, f32),
        in_specs=[smem()] + [hbm()] * 3 + [vmem()] * 6,
        out_specs=hbm(),
        scratch_shapes=[
            pltpu.VMEM((NCOMP, planes + 4, chunks, ROWS, LANES), f32),
            pltpu.VMEM((NCOMP, planes + 4, chunks, rows, LANES), f32),
            pltpu.VMEM(field.shape, f32),
            pltpu.SemaphoreType.DMA((3 * chunks + planes // 8,)),
        ],
        compiler_params=pltpu.CompilerParams(vmem_limit_bytes=50 * MIB),
        name="smoothing",
    )(flags, field, *halos)


def ring(count):
    return [(i, (i + 1) % count) for i in range(count)]


def line(count):
    return [(i, i + 1) for i in range(count - 1)]


def back(pairs):
    return [(b, a) for a, b in pairs]


def diagonal(circ_pairs, rad_pairs, rads):
    return [(a * rads + c, b * rads + d) for a, b in circ_pairs for c, d in rad_pairs]


def on_device(state, time_source, pseudo_step, offsets, weights):
    cells = state[0]
    source = time_source[0]
    pseudo = pseudo_step[0]
    planes = cells.shape[1]
    circs = lax.axis_size("circ")
    rads = lax.axis_size("rad")
    total = planes * circs
    row = lax.axis_index("row")
    rad = lax.axis_index("rad")
    rotor = row == 1
    flags = jnp.stack(
        [(rad == 0).astype(jnp.int32), (rad == rads - 1).astype(jnp.int32), row.astype(jnp.int32)]
    )
    up_circ, up_rad = ring(circs), line(rads)

    rad_low, rad_high, circ_low, circ_high, face = edges(flags, cells)
    facing = lax.ppermute(face, "row", [(0, 1), (1, 0)])
    halo_circ_low = lax.ppermute(circ_high, "circ", up_circ)
    halo_circ_high = lax.ppermute(circ_low, "circ", back(up_circ))
    halo_rad_low = lax.ppermute(rad_high, "rad", up_rad)
    halo_rad_high = lax.ppermute(rad_low, "rad", back(up_rad))
    plane = lax.all_to_all(
        jnp.broadcast_to(facing[None], (circs, *facing.shape)), "circ", 0, 0, tiled=True
    )

    here = lax.axis_index("circ") * planes
    shift = offsets.astype(jnp.int32)
    starts = jnp.where(rotor, here + shift, here - shift - 1) % total
    lead = jnp.where(rotor, 1.0 - weights, weights)
    trail = jnp.where(rotor, weights, 1.0 - weights)

    field, circ_low, circ_high, rad_low, rad_high = fluxes(
        flags,
        starts,
        lead,
        trail,
        cells,
        source,
        pseudo,
        (halo_circ_low, halo_circ_high, halo_rad_low, halo_rad_high),
        plane,
    )
    both = ("circ", "rad")
    halos = (
        lax.ppermute(circ_high, "circ", up_circ),
        lax.ppermute(circ_low, "circ", back(up_circ)),
        lax.ppermute(rad_high, "rad", up_rad),
        lax.ppermute(rad_low, "rad", back(up_rad)),
        lax.ppermute(rad_high[:, planes - 2 :], both, diagonal(up_circ, up_rad, rads)),
        lax.ppermute(rad_low[:, planes - 2 :], both, diagonal(up_circ, back(up_rad), rads)),
        lax.ppermute(rad_high[:, :2], both, diagonal(back(up_circ), up_rad, rads)),
        lax.ppermute(rad_low[:, :2], both, diagonal(back(up_circ), back(up_rad), rads)),
    )
    return smoothed(flags, field, halos)[None]


def solution(mesh):
    return jax.shard_map(
        on_device,
        mesh=mesh,
        in_specs=(
            P("row", None, "circ", "rad", None),
            P("row", None, "circ", "rad", None),
            P("row", "circ", "rad", None),
            P("rad"),
            P("rad"),
        ),
        out_specs=P("row", None, "circ", "rad", None),
        check_vma=False,
    )
```

```python
import jax
import jax.numpy as jnp
import numpy as np
from jax import lax
from jax.experimental import pallas as pl
from jax.experimental.pallas import tpu as pltpu
from jax.sharding import PartitionSpec as P

GAMMA = 1.4
GAMMA_LESS = 0.4
SECOND_COEF = 0.5
FOURTH_COEF = 0.03125
RATE = 0.75
GRID_SPEED = 0.5
AXIAL_COUPLING = 0.8
CIRC_COUPLING = 0.6
RADIAL_COUPLING = 0.6

NCOMP = 5
LANES = 128
ROWS = 32
FIRST = 8
MIB = 1 << 20


def axial_table(length):
    modes_index = np.arange(1, length + 1) * 1.0
    angle = np.pi / (length + 1)
    modes = np.sin(np.outer(modes_index, modes_index) * angle)
    eigen = 1.0 + 2.0 * AXIAL_COUPLING - 2.0 * AXIAL_COUPLING * np.cos(modes_index * angle)
    return modes / eigen[None, :] @ modes.T * (2.0 / (length + 1))


def vmem():
    return pl.BlockSpec(memory_space=pltpu.VMEM)


def smem():
    return pl.BlockSpec(memory_space=pltpu.SMEM)


def hbm():
    return pl.BlockSpec(memory_space=pl.ANY)


def lane_index(rows):
    return lax.broadcasted_iota(jnp.int32, (rows, LANES), 1)


def begin(a, b, s):
    copy = pltpu.make_async_copy(a, b, s)
    copy.start()
    return copy


def edges_kernel(flags, state, pack_a, pack_b, circ_low, circ_high, face, buf, packs, sems):
    planes = state.shape[1]
    chunks = state.shape[3] // LANES
    group = 8
    groups = planes // group
    loads = []
    for g in range(groups):
        loads.append(
            [
                begin(
                    state.at[:, pl.ds(g * group, group), :, pl.ds(c * LANES, LANES)],
                    buf.at[:, pl.ds(g * group, group), c],
                    sems.at[g * chunks + c],
                )
                for c in range(chunks)
            ]
        )
    k = groups * chunks
    edge = [
        begin(state.at[:, 0:2], circ_low, sems.at[k]),
        begin(state.at[:, planes - 2 : planes], circ_high, sems.at[k + 1]),
    ]
    rotor = flags[2]
    odd = flags[3]
    end_chunk = jnp.where(rotor == 1, 0, chunks - 1)
    lane = lane_index(8)
    sub = lax.broadcasted_iota(jnp.int32, (8, LANES), 0)
    behind_by = jnp.where(rotor == 1, 0, 2)
    for g in range(groups):
        for copy in loads[g]:
            copy.wait()

        def body(q, carry):
            for m in range(NCOMP):
                for e in range(2):
                    for c in range(chunks):
                        at = pl.ds(4 * e + c, 1)
                        for i in range(2):
                            low = buf[m, 2 * q + e, c, i : i + 1, :]
                            high = buf[m, 2 * q + e, c, 14 + i : 15 + i, :]
                            packs[1 - odd, m, q, i, at, :] = low
                            packs[odd, m, q, i, at, :] = high
            for e in range(2):
                j = 2 * q + e
                for h in range(2):
                    total = jnp.zeros((8, LANES), jnp.float32)
                    for m in range(NCOMP):
                        moved = pltpu.roll(
                            buf[m, j, end_chunk, 8 * h : 8 * h + 8, :], 2 * m, 1, stride=16, stride_axis=0
                        )
                        at = (lane + behind_by - sub * 16 - 2 * m) & (LANES - 1)
                        total = jnp.where(at < 2, moved, total)
                    face[h, pl.ds(j, 1), :] = jnp.sum(total, axis=0, keepdims=True)
            return carry

        lax.fori_loop(g * group // 2, (g + 1) * group // 2, body, 0)
    edge += [
        begin(packs.at[0], pack_a, sems.at[k + 2]),
        begin(packs.at[1], pack_b, sems.at[k + 3]),
    ]
    for copy in edge:
        copy.wait()


def edges(flags, cells):
    planes, rows, length = cells.shape[1:]
    chunks = length // LANES
    f32 = jnp.float32
    rad = jax.ShapeDtypeStruct((NCOMP, planes // 2, 2, 8, LANES), f32)
    circ = jax.ShapeDtypeStruct((NCOMP, 2, rows, length), f32)
    face = jax.ShapeDtypeStruct((2, planes, LANES), f32)
    return pl.pallas_call(
        edges_kernel,
        out_shape=(rad, rad, circ, circ, face),
        in_specs=[smem(), hbm()],
        out_specs=(hbm(),) * 4 + (vmem(),),
        scratch_shapes=[
            pltpu.VMEM((NCOMP, planes, chunks, rows, LANES), f32),
            pltpu.VMEM((2,) + rad.shape, f32),
            pltpu.SemaphoreType.DMA((planes // 8 * chunks + 4,)),
        ],
        compiler_params=pltpu.CompilerParams(vmem_limit_bytes=24 * MIB),
        name="state_edges",
    )(flags, cells)


def primitives(cons):
    inverse = 1.0 / cons[0]
    velocity = [cons[m] * inverse for m in (1, 2, 3)]
    kinetic = cons[1] * velocity[0] + cons[2] * velocity[1] + cons[3] * velocity[2]
    pressure = GAMMA_LESS * (cons[4] - 0.5 * kinetic)
    square = GAMMA * pressure * inverse
    sound = square * lax.rsqrt(square)
    return [pressure, sound, *velocity]


def sensor_of(upper, middle, lower):
    outer = upper + lower
    twice = 2.0 * middle
    return jnp.abs(outer - twice) / (outer + twice)


def face_flux(component, cons, pressure, sound, velocity, sensor, grid_speed):
    half = [0.5 * (v - grid_speed) if grid_speed is not None else 0.5 * v for v in velocity]
    speed = jnp.abs(half[0]) + jnp.abs(half[1]) + 0.5 * (sound[0] + sound[1])
    second = SECOND_COEF * jnp.maximum(sensor[0], sensor[1])
    fourth = jnp.maximum(0.0, FOURTH_COEF - second)
    outer = speed * fourth
    inner = speed * (second + 3.0 * fourth)
    near = half[0] + inner
    far = half[1] - inner
    fluxes = []
    for m in range(NCOMP):
        before, left, right, beyond = cons[m]
        flux = right * far + left * near + outer * (beyond - before)
        if m == component:
            flux = flux + 0.5 * (pressure[0] + pressure[1])
        if m == 4:
            flux = flux + 0.5 * (pressure[0] * velocity[0] + pressure[1] * velocity[1])
        fluxes.append(flux)
    return fluxes


def circ_face(cons, at, pressure, sound, velocity, sensor_before, spin):
    sensor = sensor_of(pressure[2], pressure[1], pressure[0])
    flux = face_flux(
        2,
        [[cons(m, d) for d in (-1, 0, 1, 2)] for m in range(NCOMP)],
        pressure[:2],
        sound,
        velocity,
        [sensor_before, sensor],
        spin,
    )
    return flux, sensor


def inner_kernel(flags, state, source, out, cons, prim, src, partial, circ_flux, circ_sensor, sems):
    planes = state.shape[1]
    chunks = state.shape[3] // LANES
    group = 8
    groups = planes // group
    loads = []
    for g in range(groups):
        part = [
            begin(
                state.at[:, pl.ds(g * group, group), :, pl.ds(c * LANES, LANES)],
                cons.at[:, pl.ds(g * group, group), c],
                sems.at[g * (chunks + 1) + c],
            )
            for c in range(chunks)
        ]
        part.append(
            begin(
                source.at[:, pl.ds(g * group, group)],
                src.at[:, pl.ds(g * group, group)],
                sems.at[g * (chunks + 1) + chunks],
            )
        )
        loads.append(part)
    k = groups * (chunks + 1)
    spin = GRID_SPEED * flags[2].astype(jnp.float32)
    lane = lane_index(16)

    def prepare(j, carry):
        for c in range(chunks):
            fields = primitives([cons[m, j, c] for m in range(NCOMP)])
            for f in range(4):
                prim[f, j, c] = fields[f]
        return carry

    def behind(parts, by):
        turned = [pltpu.roll(x, by, 1) for x in parts]
        return [jnp.where(lane < by, turned[c - 1], turned[c]) for c in range(chunks)]

    def ahead(parts):
        turned = [pltpu.roll(x, LANES - 1, 1) for x in parts]
        return [jnp.where(lane < LANES - 1, turned[c], turned[(c + 1) % chunks]) for c in range(chunks)]

    def axial_part(j):
        state_parts = [[cons[m, j, c] for c in range(chunks)] for m in range(NCOMP)]
        p, sound, speed = [[prim[f, j, c] for c in range(chunks)] for f in (0, 1, 2)]
        p_before = behind(p, 1)
        p_after = ahead(p)
        sensor = [sensor_of(p_after[c], p[c], p_before[c]) for c in range(chunks)]
        sensor_before = behind(sensor, 1)
        sound_before = behind(sound, 1)
        speed_before = behind(speed, 1)
        shifted = [(behind(x, 2), behind(x, 1), x, ahead(x)) for x in state_parts]
        flux = [
            face_flux(
                1,
                [[shifted[m][d][c] for d in range(4)] for m in range(NCOMP)],
                [p_before[c], p[c]],
                [sound_before[c], sound[c]],
                [speed_before[c], speed[c]],
                [sensor_before[c], sensor[c]],
                None,
            )
            for c in range(chunks)
        ]
        for m in range(NCOMP):
            parts = [flux[c][m] for c in range(chunks)]
            upper = ahead(parts)
            for c in range(chunks):
                value = upper[c] - parts[c]
                if c == 0:
                    value = jnp.where(lane < 2, 0.0, value)
                if c == chunks - 1:
                    value = jnp.where(lane < LANES - 2, value, 0.0)
                cols = pl.ds(c * LANES, LANES)
                partial[m, j, :, cols] = value + RATE * state_parts[m][c] + src[m, j, :, cols]

    def circ_part(j):
        for c in range(chunks):
            flux, sensor = circ_face(
                lambda m, d: cons[m, j + d, c],
                j,
                [prim[0, j + d, c] for d in (0, 1, 2)],
                [prim[1, j + d, c] for d in (0, 1)],
                [prim[3, j + d, c] for d in (0, 1)],
                circ_sensor[c],
                spin,
            )
            circ_sensor[c] = sensor
            cols = pl.ds(c * LANES, LANES)
            for m in range(NCOMP):
                value = flux[m] - circ_flux[m, c]
                circ_flux[m, c] = flux[m]
                partial[m, j, :, cols] = partial[m, j, :, cols] + jnp.where(j >= 2, value, 0.0)

    def body(j, carry):
        prepare(j + 2, 0)
        axial_part(j)
        circ_part(j)
        return carry

    stores = []

    def store(g):
        stores.append(
            begin(
                partial.at[:, pl.ds(g * group, group)],
                out.at[:, pl.ds(g * group, group)],
                sems.at[k + g],
            )
        )

    for copy in loads[0]:
        copy.wait()
    lax.fori_loop(0, 3, prepare, 0)
    for c in range(chunks):
        circ_sensor[c] = sensor_of(prim[0, 2, c], prim[0, 1, c], prim[0, 0, c])
    axial_part(0)
    done = 1
    for g in range(groups):
        stop = (g + 1) * group - 2
        lax.fori_loop(done, stop, body, 0)
        done = stop
        if g + 1 < groups:
            for copy in loads[g + 1]:
                copy.wait()
        if g > 0:
            store(g - 1)

    def last(j, carry):
        axial_part(j)
        return carry

    lax.fori_loop(planes - 2, planes, last, 0)
    store(groups - 1)
    for copy in stores:
        copy.wait()


def inner_parts(flags, cells, source):
    planes, rows, length = cells.shape[1:]
    chunks = length // LANES
    f32 = jnp.float32
    chunked = (planes, chunks, rows, LANES)
    return pl.pallas_call(
        inner_kernel,
        out_shape=jax.ShapeDtypeStruct(cells.shape, f32),
        in_specs=[smem()] + [hbm()] * 2,
        out_specs=hbm(),
        scratch_shapes=[
            pltpu.VMEM((NCOMP,) + chunked, f32),
            pltpu.VMEM((4,) + chunked, f32),
            pltpu.VMEM(cells.shape, f32),
            pltpu.VMEM(cells.shape, f32),
            pltpu.VMEM((NCOMP, chunks, rows, LANES), f32),
            pltpu.VMEM((chunks, rows, LANES), f32),
            pltpu.SemaphoreType.DMA((planes // 8 * (chunks + 2),)),
        ],
        compiler_params=pltpu.CompilerParams(vmem_limit_bytes=50 * MIB),
        cost_estimate=pl.CostEstimate(
            flops=30_000_000_000, transcendentals=0, bytes_accessed=15_000_000
        ),
        name="inner_parts",
    )(flags, cells, source)


def outer_kernel(
    flags,
    starts,
    lead_weight,
    trail_weight,
    state,
    partial_in,
    pseudo,
    circ_low,
    circ_high,
    own_a,
    own_b,
    halo_a,
    halo_b,
    plane,
    table_high,
    table_low,
    out,
    out_circ_low,
    out_circ_high,
    out_a,
    out_b,
    out_low_a,
    out_low_b,
    out_high_a,
    out_high_b,
    cons,
    prim,
    partial,
    step,
    raw_high,
    raw_low,
    result,
    tables,
    own,
    halo,
    top_flux,
    cycle,
    ghosts,
    rad_flux,
    packs,
    sems,
):
    planes = state.shape[1]
    chunks = state.shape[3] // LANES
    group = 8
    groups = planes // group
    cells = pl.ds(FIRST, 16)
    rotor = flags[2]
    odd = flags[3]

    loads = []
    for g in range(groups):
        loads += [
            begin(
                state.at[:, pl.ds(g * group, group), :, pl.ds(c * LANES, LANES)],
                cons.at[:, pl.ds(2 + g * group, group), c, cells, :],
                sems.at[g * chunks + c],
            )
            for c in range(chunks)
        ]
    k = groups * chunks
    rims = [
        begin(own_a, own.at[1 - odd], sems.at[k]),
        begin(own_b, own.at[odd], sems.at[k + 1]),
        begin(halo_a, halo.at[1 - odd], sems.at[k + 2]),
        begin(halo_b, halo.at[odd], sems.at[k + 3]),
    ]
    k += 4
    for c in range(chunks):
        cols = pl.ds(c * LANES, LANES)
        loads.append(begin(circ_low.at[:, :, :, cols], cons.at[:, 0:2, c, cells, :], sems.at[k]))
        loads.append(
            begin(
                circ_high.at[:, :, :, cols],
                cons.at[:, planes + 2 : planes + 4, c, cells, :],
                sems.at[k + 1],
            )
        )
        k += 2
    late = [
        begin(partial_in, partial, sems.at[k]),
        begin(pseudo, step, sems.at[k + 1]),
        begin(table_high, tables.at[0], sems.at[k + 2]),
        begin(table_low, tables.at[1], sems.at[k + 3]),
    ]
    k += 4
    lane8 = lane_index(8)
    lane = lane_index(16)

    count = plane.shape[0]
    width = plane.shape[2]
    for h in range(2):
        for s in range(count):
            cycle[h, pl.ds(s * width, width), :] = plane[s, h]
        cycle[h, pl.ds(count * width, width), :] = plane[0, h]
        cycle[h, pl.ds((count + 1) * width, 8), :] = plane[1, h, 0:8]
    turn = jnp.where(rotor == 1, 0, 64)
    for h in range(2):
        for jt in range(planes // 8):
            total = jnp.zeros((8, LANES), jnp.float32)
            for r in range(8):
                at = starts[8 * h + r] + 8 * jt
                value = (
                    lead_weight[8 * h + r] * cycle[h, pl.ds(at, 8), :]
                    + trail_weight[8 * h + r] * cycle[h, pl.ds(at + 1, 8), :]
                )
                to = (8 - r) % 8
                if to != r:
                    value = pltpu.roll(value, (to - r) % 8 * 16, 1)
                total = jnp.where(((lane8 + 2) & (LANES - 1)) // 16 == to, value, total)
            ghosts[h, pl.ds(8 * jt, 8), :] = pltpu.roll(total, turn, 1)

    for copy in rims:
        copy.wait()

    def mirror(side):
        def body(q, carry):
            for m in range(NCOMP):
                sign = -1.0 if m == 3 else 1.0
                for i in range(2):
                    halo[side, m, q, i] = sign * own[side, m, q, 1 - i]
            return carry

        lax.fori_loop(0, planes // 2, body, 0)

    @pl.when(flags[0] == 1)
    def _():
        mirror(0)

    @pl.when(flags[1] == 1)
    def _():
        mirror(1)

    for copy in loads:
        copy.wait()

    def rim(q, carry):
        low = [[halo[0, m, q, i] for m in range(NCOMP)] for i in range(2)]
        high = [[own[1, m, q, i] for m in range(NCOMP)] for i in range(2)]
        high += [[halo[1, m, q, i] for m in range(NCOMP)] for i in range(2)]
        low_fields = [primitives(x) for x in low]
        fields = [primitives(x) for x in high]
        p = [x[0] for x in fields]
        flux = face_flux(
            3,
            [[high[d][m] for d in range(4)] for m in range(NCOMP)],
            p[1:3],
            [fields[1][1], fields[2][1]],
            [fields[1][4], fields[2][4]],
            [sensor_of(p[2], p[1], p[0]), sensor_of(p[3], p[2], p[1])],
            None,
        )
        for m in range(NCOMP):
            top_flux[m, q] = flux[m]
        for e in range(2):
            at = 2 * q + e + 2
            for c in range(chunks):
                w = 4 * e + c
                for m in range(NCOMP):
                    for i in range(2):
                        cons[m, at, c, FIRST - 2 + i : FIRST - 1 + i, :] = low[i][m][w : w + 1]
                    cons[m, at, c, FIRST + 16 : FIRST + 17, :] = high[2][m][w : w + 1]
                for i in range(2):
                    prim[0, at, c, FIRST - 2 + i : FIRST - 1 + i, :] = low_fields[i][0][w : w + 1]
                prim[0, at, c, FIRST + 16 : FIRST + 17, :] = fields[2][0][w : w + 1]
                prim[1, at, c, FIRST - 1 : FIRST, :] = low_fields[1][1][w : w + 1]
                prim[2, at, c, FIRST - 1 : FIRST, :] = low_fields[1][4][w : w + 1]
        return carry

    lax.fori_loop(0, planes // 2, rim, 0)

    def prepare(j, carry):
        for c in range(chunks):
            fields = primitives([cons[m, j, c, cells, :] for m in range(NCOMP)])
            prim[0, j, c, cells, :] = fields[0]
            prim[1, j, c, cells, :] = fields[1]
            prim[2, j, c, cells, :] = fields[4]
        return carry

    lax.fori_loop(0, planes + 4, prepare, 0)
    for copy in late:
        copy.wait()

    spin = GRID_SPEED * rotor.astype(jnp.float32)

    def swirl(j, c):
        return cons[2, j, c, cells, :] / cons[0, j, c, cells, :]

    def circ_edges(c, carry):
        cols = pl.ds(pl.multiple_of(c * LANES, LANES), LANES)
        for base in (1, planes - 1):
            before = sensor_of(*[prim[0, base + d, c, cells, :] for d in (1, 0, -1)])
            fluxes = []
            for f in range(3):
                at = base + f
                flux, before = circ_face(
                    lambda m, d: cons[m, at + d, c, cells, :],
                    at,
                    [prim[0, at + d, c, cells, :] for d in (0, 1, 2)],
                    [prim[1, at + d, c, cells, :] for d in (0, 1)],
                    [swirl(at + d, c) for d in (0, 1)],
                    before,
                    spin,
                )
                fluxes.append(flux)
            for f in range(2):
                j = base - 1 + f
                for m in range(NCOMP):
                    partial[m, j, :, cols] = (
                        partial[m, j, :, cols] + fluxes[f + 1][m] - fluxes[f][m]
                    )
        return carry

    lax.fori_loop(0, chunks, circ_edges, 0)

    ghost_lanes = jnp.where(lane < 96, 1 - rotor, rotor) == 1

    def ends(j, carry):
        at = j + 2
        spread = jnp.concatenate(
            [
                pltpu.roll(
                    jnp.broadcast_to(ghosts[h, pl.ds(j, 1), :], (8, LANES)),
                    0,
                    1,
                    stride=16,
                    stride_axis=0,
                )
                for h in range(2)
            ],
            axis=0,
        )
        joined = []
        for m in range(NCOMP):
            first = cons[m, at, 0, cells, :]
            last = cons[m, at, chunks - 1, cells, :]
            moved = pltpu.roll(spread, LANES - 2 * m, 1) if m else spread
            edge = jnp.where(
                rotor == 1,
                jnp.broadcast_to(last[:, LANES - 1 : LANES], (16, LANES)),
                jnp.broadcast_to(first[:, 0:1], (16, LANES)),
            )
            outside = jnp.where(ghost_lanes, moved, edge)
            inside = jnp.where(lane < 32, first, pltpu.roll(last, 64, 1))
            joined.append(jnp.where(lane < 64, inside, outside))
        p, sound, speed = primitives(joined)[:3]
        p_before = pltpu.roll(p, 1, 1)
        sensor = sensor_of(pltpu.roll(p, LANES - 1, 1), p, p_before)
        flux = face_flux(
            1,
            [
                (pltpu.roll(x, 2, 1), pltpu.roll(x, 1, 1), x, pltpu.roll(x, LANES - 1, 1))
                for x in joined
            ],
            [p_before, p],
            [pltpu.roll(sound, 1, 1), sound],
            [pltpu.roll(speed, 1, 1), speed],
            [pltpu.roll(sensor, 1, 1), sensor],
            None,
        )
        for m in range(NCOMP):
            value = pltpu.roll(flux[m], LANES - 1, 1) - flux[m]
            head = partial[m, j, :, 0:LANES]
            partial[m, j, :, 0:LANES] = head + jnp.where(lane < 2, value, 0.0)
            cols = pl.ds((chunks - 1) * LANES, LANES)
            partial[m, j, :, cols] = partial[m, j, :, cols] + jnp.where(
                lane < LANES - 2, 0.0, pltpu.roll(value, 64, 1)
            )
        return carry

    lax.fori_loop(0, planes, ends, 0)

    def radial_chunk(j, c, e, q):
        at = j + 2
        p = [prim[0, at, c, pl.ds(FIRST + d, 16), :] for d in (-2, -1, 0, 1)]
        flux = face_flux(
            3,
            [
                [cons[m, at, c, pl.ds(FIRST + d, 16), :] for d in (-2, -1, 0, 1)]
                for m in range(NCOMP)
            ],
            p[1:3],
            [prim[1, at, c, pl.ds(FIRST + d, 16), :] for d in (-1, 0)],
            [prim[2, at, c, pl.ds(FIRST + d, 16), :] for d in (-1, 0)],
            [sensor_of(p[2], p[1], p[0]), sensor_of(p[3], p[2], p[1])],
            None,
        )
        cols = pl.ds(c * LANES, LANES)
        pace = step[j, :, cols]
        for m in range(NCOMP):
            rad_flux[m, e, c, 0:16, :] = flux[m]
            rad_flux[m, e, c, 16:17, :] = top_flux[m, q, 4 * e + c : 4 * e + c + 1, :]
            raw = pace * (partial[m, j, :, cols] + (rad_flux[m, e, c, 1:17, :] - flux[m]))
            high = raw.astype(jnp.bfloat16)
            raw_high[m, j, :, cols] = high
            raw_low[m, j, :, cols] = (raw - high.astype(jnp.float32)).astype(jnp.bfloat16)

    def radial(q, carry):
        for e in range(2):
            for c in range(chunks):
                radial_chunk(2 * q + e, c, e, q)
        return carry

    lax.fori_loop(0, planes // 2, radial, 0)

    def solve(q, carry):
        length = chunks * LANES
        for m in range(NCOMP):
            high = raw_high[m, pl.ds(q * 8, 8)].reshape(128, length)
            low = raw_low[m, pl.ds(q * 8, 8)].reshape(128, length)
            value = (
                jnp.dot(high, tables[0], preferred_element_type=jnp.float32)
                + jnp.dot(high, tables[1], preferred_element_type=jnp.float32)
                + jnp.dot(low, tables[0], preferred_element_type=jnp.float32)
            )
            result[m, pl.ds(q * 8, 8)] = value.reshape(8, 16, length)
        return carry

    lax.fori_loop(0, planes // 8, solve, 0)

    stores = [
        begin(result.at[:, 0:2], out_circ_low, sems.at[k]),
        begin(result.at[:, planes - 2 : planes], out_circ_high, sems.at[k + 1]),
        begin(result, out, sems.at[k + 2]),
    ]
    k += 3

    def pick(j, carry):
        for m in range(NCOMP):
            for c in range(chunks):
                cols = pl.ds(c * LANES, LANES)
                packs[1 - odd, m, j, pl.ds(2 * c, 2), :] = result[m, j, 0:2, cols]
                packs[odd, m, j, pl.ds(2 * c, 2), :] = result[m, j, 14:16, cols]
        return carry

    lax.fori_loop(0, planes, pick, 0)
    for i, (whole, low, high) in enumerate(
        ((out_a, out_low_a, out_high_a), (out_b, out_low_b, out_high_b))
    ):
        stores.append(begin(packs.at[i], whole, sems.at[k]))
        stores.append(begin(packs.at[i, :, 0:2], low, sems.at[k + 1]))
        stores.append(begin(packs.at[i, :, planes - 2 : planes], high, sems.at[k + 2]))
        k += 3
    for copy in stores:
        copy.wait()


def outer_parts(flags, starts, lead, trail, cells, partial, pseudo, circs, own, halos, plane):
    planes, rows, length = cells.shape[1:]
    chunks = length // LANES
    table = -axial_table(length).astype(np.float32)
    table_high = table.astype(jnp.bfloat16)
    table_low = (table - table_high.astype(np.float32)).astype(jnp.bfloat16)
    f32 = jnp.float32
    rad = jax.ShapeDtypeStruct((NCOMP, planes, 8, LANES), f32)
    corner = jax.ShapeDtypeStruct((NCOMP, 2, 8, LANES), f32)
    circ = jax.ShapeDtypeStruct((NCOMP, 2, rows, length), f32)
    groups = planes // 8
    buffer = (planes + 4, chunks, ROWS, LANES)
    rims = (2, NCOMP, planes // 2, 2, 8, LANES)
    return pl.pallas_call(
        outer_kernel,
        out_shape=(jax.ShapeDtypeStruct(cells.shape, f32), circ, circ, rad, rad) + (corner,) * 4,
        in_specs=[smem()] * 4 + [hbm()] * 9 + [vmem()] + [hbm()] * 2,
        out_specs=(hbm(),) * 9,
        scratch_shapes=[
            pltpu.VMEM((NCOMP,) + buffer, f32),
            pltpu.VMEM((3,) + buffer, f32),
            pltpu.VMEM(cells.shape, f32),
            pltpu.VMEM(pseudo.shape, f32),
            pltpu.VMEM(cells.shape, jnp.bfloat16),
            pltpu.VMEM(cells.shape, jnp.bfloat16),
            pltpu.VMEM(cells.shape, f32),
            pltpu.VMEM((2, length, length), jnp.bfloat16),
            pltpu.VMEM(rims, f32),
            pltpu.VMEM(rims, f32),
            pltpu.VMEM((NCOMP, planes // 2, 8, LANES), f32),
            pltpu.VMEM((2, plane.shape[0] * planes + planes + 8, LANES), f32),
            pltpu.VMEM((2, planes, LANES), f32),
            pltpu.VMEM((NCOMP, 2, chunks, 24, LANES), f32),
            pltpu.VMEM((2, NCOMP, planes, 8, LANES), f32),
            pltpu.SemaphoreType.DMA((groups * chunks + 2 * chunks + 17,)),
        ],
        compiler_params=pltpu.CompilerParams(vmem_limit_bytes=58 * MIB),
        name="outer_parts",
    )(
        flags,
        starts,
        lead,
        trail,
        cells,
        partial,
        pseudo,
        *circs,
        *own,
        *halos,
        plane,
        jnp.asarray(table_high),
        jnp.asarray(table_low),
    )


def smooth_kernel(
    flags,
    field,
    circ_low,
    circ_high,
    rim_a,
    rim_b,
    low_a,
    low_b,
    high_a,
    high_b,
    out,
    buf,
    mid,
    done,
    rims,
    sems,
):
    planes = field.shape[1]
    chunks = field.shape[3] // LANES
    cells = pl.ds(FIRST, 16)
    group = 8

    odd = flags[3]
    copies = []
    k = 0
    for c in range(chunks):
        cols = pl.ds(c * LANES, LANES)
        copies.append(begin(field.at[:, :, :, cols], buf.at[:, 2 : planes + 2, c, cells, :], sems.at[k]))
        copies.append(begin(circ_low.at[:, :, :, cols], buf.at[:, 0:2, c, cells, :], sems.at[k + 1]))
        copies.append(
            begin(circ_high.at[:, :, :, cols], buf.at[:, planes + 2 : planes + 4, c, cells, :], sems.at[k + 2])
        )
        k += 3

    pieces = []
    for side, parts in ((1 - odd, (low_a, rim_a, high_a)), (odd, (low_b, rim_b, high_b))):
        for part, first, count in zip(parts, (0, 2, planes + 2), (2, planes, 2)):
            pieces.append(begin(part, rims.at[side, :, pl.ds(first, count)], sems.at[k]))
            k += 1
    for copy in pieces:
        copy.wait()

    def put(j, carry):
        for m in range(NCOMP):
            for c in range(chunks):
                buf[m, j, c, pl.ds(FIRST - 2, 2), :] = rims[0, m, j, pl.ds(2 * c, 2), :]
                buf[m, j, c, pl.ds(FIRST + 16, 2), :] = rims[1, m, j, pl.ds(2 * c, 2), :]
        return carry

    lax.fori_loop(0, planes + 4, put, 0)
    for copy in copies:
        copy.wait()

    def wall(zero_row, odd_row, from_row):
        def body(j, carry):
            for m in range(NCOMP):
                for c in range(chunks):
                    buf[m, j, c, pl.ds(zero_row, 1), :] = jnp.zeros((1, LANES), jnp.float32)
                    buf[m, j, c, pl.ds(odd_row, 1), :] = -buf[m, j, c, pl.ds(from_row, 1), :]
            return carry

        lax.fori_loop(0, planes + 4, body, 0)

    @pl.when(flags[0] == 1)
    def _():
        wall(FIRST - 1, FIRST - 2, FIRST)

    @pl.when(flags[1] == 1)
    def _():
        wall(FIRST + 16, FIRST + 17, FIRST + 15)

    def weights(coupling):
        own = 1.0 / (1.0 + 2.0 * coupling)
        side = coupling / (1.0 + 2.0 * coupling)
        return own * own + 2.0 * side * side, 2.0 * own * side, side * side

    def radial(j, carry):
        w0, w1, w2 = weights(RADIAL_COUPLING)
        for m in range(NCOMP):
            for c in range(chunks):
                x = [buf[m, j, c, pl.ds(FIRST + d, 16), :] for d in (-2, -1, 0, 1, 2)]
                mid[m, j, c] = w0 * x[2] + w1 * (x[1] + x[3]) + w2 * (x[0] + x[4])
        return carry

    lax.fori_loop(0, planes + 4, radial, 0)

    def around(j, carry):
        w0, w1, w2 = weights(CIRC_COUPLING)
        for m in range(NCOMP):
            for c in range(chunks):
                x = [mid[m, j + d, c] for d in range(5)]
                done[m, j, :, pl.ds(c * LANES, LANES)] = (
                    w0 * x[2] + w1 * (x[1] + x[3]) + w2 * (x[0] + x[4])
                )
        return carry

    stores = []
    for g in range(planes // group):
        lax.fori_loop(g * group, (g + 1) * group, around, 0)
        stores.append(
            begin(done.at[:, pl.ds(g * group, group)], out.at[:, pl.ds(g * group, group)], sems.at[k])
        )
        k += 1
    for copy in stores:
        copy.wait()


def smoothed(flags, field, halos):
    planes, rows, length = field.shape[1:]
    chunks = length // LANES
    f32 = jnp.float32
    return pl.pallas_call(
        smooth_kernel,
        out_shape=jax.ShapeDtypeStruct(field.shape, f32),
        in_specs=[smem()] + [hbm()] * 9,
        out_specs=hbm(),
        scratch_shapes=[
            pltpu.VMEM((NCOMP, planes + 4, chunks, ROWS, LANES), f32),
            pltpu.VMEM((NCOMP, planes + 4, chunks, rows, LANES), f32),
            pltpu.VMEM(field.shape, f32),
            pltpu.VMEM((2, NCOMP, planes + 4, 8, LANES), f32),
            pltpu.SemaphoreType.DMA((3 * chunks + planes // 8 + 6,)),
        ],
        compiler_params=pltpu.CompilerParams(vmem_limit_bytes=50 * MIB),
        name="smoothing",
    )(flags, field, *halos)


def ring(count):
    return [(i, (i + 1) % count) for i in range(count)]


def back(pairs):
    return [(b, a) for a, b in pairs]


def rims_of(count):
    first = [(i, i ^ 1) for i in range(count)]
    second = [(i, ((i + 1) ^ 1) - 1 if 0 < i < count - 1 else i) for i in range(count)]
    return first, second


def crossed(circ_pairs, rad_pairs, rads):
    return [(a * rads + c, b * rads + d) for a, b in circ_pairs for c, d in rad_pairs]


def on_device(state, time_source, pseudo_step, offsets, weights):
    cells = state[0]
    source = time_source[0]
    pseudo = pseudo_step[0]
    planes = cells.shape[1]
    circs = lax.axis_size("circ")
    rads = lax.axis_size("rad")
    total = planes * circs
    row = lax.axis_index("row")
    rad = lax.axis_index("rad")
    rotor = row == 1
    flags = jnp.stack(
        [
            (rad == 0).astype(jnp.int32),
            (rad == rads - 1).astype(jnp.int32),
            row.astype(jnp.int32),
            (rad % 2).astype(jnp.int32),
        ]
    )
    up = ring(circs)
    down = back(up)
    pairs_a, pairs_b = rims_of(rads)

    own_a, own_b, circ_low, circ_high, face = edges(flags, cells)
    facing = lax.ppermute(face, "row", [(0, 1), (1, 0)])
    halo_circs = (lax.ppermute(circ_high, "circ", up), lax.ppermute(circ_low, "circ", down))
    halo_rads = (lax.ppermute(own_a, "rad", pairs_a), lax.ppermute(own_b, "rad", pairs_b))
    plane = lax.all_to_all(
        jnp.broadcast_to(facing[None], (circs, *facing.shape)), "circ", 0, 0, tiled=True
    )
    partial = inner_parts(flags, cells, source)

    here = lax.axis_index("circ") * planes
    shift = offsets.astype(jnp.int32)
    starts = jnp.where(rotor, here + shift, here - shift - 1) % total
    lead = jnp.where(rotor, 1.0 - weights, weights)
    trail = jnp.where(rotor, weights, 1.0 - weights)

    field, circ_low, circ_high, rim_a, rim_b, low_a, low_b, high_a, high_b = outer_parts(
        flags,
        starts,
        lead,
        trail,
        cells,
        partial,
        pseudo,
        halo_circs,
        (own_a, own_b),
        halo_rads,
        plane,
    )
    both = ("circ", "rad")
    halos = (
        lax.ppermute(circ_high, "circ", up),
        lax.ppermute(circ_low, "circ", down),
        lax.ppermute(rim_a, "rad", pairs_a),
        lax.ppermute(rim_b, "rad", pairs_b),
        lax.ppermute(high_a, both, crossed(up, pairs_a, rads)),
        lax.ppermute(high_b, both, crossed(up, pairs_b, rads)),
        lax.ppermute(low_a, both, crossed(down, pairs_a, rads)),
        lax.ppermute(low_b, both, crossed(down, pairs_b, rads)),
    )
    return smoothed(flags, field, halos)[None]


def solution(mesh):
    return jax.shard_map(
        on_device,
        mesh=mesh,
        in_specs=(
            P("row", None, "circ", "rad", None),
            P("row", None, "circ", "rad", None),
            P("row", "circ", "rad", None),
            P("rad"),
            P("rad"),
        ),
        out_specs=P("row", None, "circ", "rad", None),
        check_vma=False,
    )
```

```python
import jax
import jax.numpy as jnp
import numpy as np
from jax import lax
from jax.experimental import pallas as pl
from jax.experimental.pallas import tpu as pltpu
from jax.sharding import PartitionSpec as P

GAMMA = 1.4
GAMMA_LESS = 0.4
SECOND_COEF = 0.5
FOURTH_COEF = 0.03125
RATE = 0.75
GRID_SPEED = 0.5
AXIAL_COUPLING = 0.8
CIRC_COUPLING = 0.6
RADIAL_COUPLING = 0.6

NCOMP = 5
LANES = 128
ROWS = 32
FIRST = 8
MIB = 1 << 20


def axial_table(length):
    modes_index = np.arange(1, length + 1) * 1.0
    angle = np.pi / (length + 1)
    modes = np.sin(np.outer(modes_index, modes_index) * angle)
    eigen = 1.0 + 2.0 * AXIAL_COUPLING - 2.0 * AXIAL_COUPLING * np.cos(modes_index * angle)
    return modes / eigen[None, :] @ modes.T * (2.0 / (length + 1))


def vmem():
    return pl.BlockSpec(memory_space=pltpu.VMEM)


def smem():
    return pl.BlockSpec(memory_space=pltpu.SMEM)


def hbm():
    return pl.BlockSpec(memory_space=pltpu.HBM)


def lane_index(rows):
    return lax.broadcasted_iota(jnp.int32, (rows, LANES), 1)


def begin(a, b, s):
    copy = pltpu.make_async_copy(a, b, s)
    copy.start()
    return copy


def edges_kernel(flags, state, pack_a, pack_b, circ_low, circ_high, face, buf, packs, sems):
    planes = state.shape[1]
    chunks = state.shape[3] // LANES
    group = 8
    groups = planes // group
    loads = []
    for g in range(groups):
        part = pl.ds(g * group, group)
        loads.append(begin(state.at[:, part], buf.at[:, part], sems.at[g]))
    k = groups
    rotor = flags[2]
    odd = flags[3]
    end_cols = pl.ds(pl.multiple_of(jnp.where(rotor == 1, 0, (chunks - 1) * LANES), LANES), LANES)
    lane = lane_index(8)
    sub = lax.broadcasted_iota(jnp.int32, (8, LANES), 0)
    behind_by = jnp.where(rotor == 1, 0, 2)
    for g in range(groups):
        loads[g].wait()

        def body(q, carry):
            for m in range(NCOMP):
                for e in range(2):
                    for c in range(chunks):
                        at = pl.ds(4 * e + c, 1)
                        for i in range(2):
                            cols = pl.ds(c * LANES, LANES)
                            low = buf[m, 2 * q + e, i : i + 1, cols]
                            high = buf[m, 2 * q + e, 14 + i : 15 + i, cols]
                            packs[1 - odd, m, q, i, at, :] = low
                            packs[odd, m, q, i, at, :] = high
            for e in range(2):
                j = 2 * q + e
                for h in range(2):
                    total = jnp.zeros((8, LANES), jnp.float32)
                    for m in range(NCOMP):
                        moved = pltpu.roll(
                            buf[m, j, 8 * h : 8 * h + 8, end_cols], 2 * m, 1, stride=16, stride_axis=0
                        )
                        at = (lane + behind_by - sub * 16 - 2 * m) & (LANES - 1)
                        total = jnp.where(at < 2, moved, total)
                    face[h, pl.ds(j, 1), :] = jnp.sum(total, axis=0, keepdims=True)
            return carry

        lax.fori_loop(g * group // 2, (g + 1) * group // 2, body, 0)
    edge = [
        begin(buf.at[:, 0:2], circ_low, sems.at[k]),
        begin(buf.at[:, planes - 2 : planes], circ_high, sems.at[k + 1]),
        begin(packs.at[0], pack_a, sems.at[k + 2]),
        begin(packs.at[1], pack_b, sems.at[k + 3]),
    ]
    for copy in edge:
        copy.wait()


def edges(flags, cells):
    planes, rows, length = cells.shape[1:]
    chunks = length // LANES
    f32 = jnp.float32
    rad = jax.ShapeDtypeStruct((NCOMP, planes // 2, 2, 8, LANES), f32)
    circ = jax.ShapeDtypeStruct((NCOMP, 2, rows, length), f32)
    face = jax.ShapeDtypeStruct((2, planes, LANES), f32)
    return pl.pallas_call(
        edges_kernel,
        out_shape=(rad, rad, circ, circ, face),
        in_specs=[smem(), hbm()],
        out_specs=(hbm(),) * 4 + (vmem(),),
        scratch_shapes=[
            pltpu.VMEM(cells.shape, f32),
            pltpu.VMEM((2,) + rad.shape, f32),
            pltpu.SemaphoreType.DMA((planes // 8 + 4,)),
        ],
        compiler_params=pltpu.CompilerParams(vmem_limit_bytes=59 * MIB),
        name="state_edges",
    )(flags, cells)


def primitives(cons):
    inverse = 1.0 / cons[0]
    velocity = [cons[m] * inverse for m in (1, 2, 3)]
    kinetic = cons[1] * velocity[0] + cons[2] * velocity[1] + cons[3] * velocity[2]
    pressure = GAMMA_LESS * (cons[4] - 0.5 * kinetic)
    square = GAMMA * pressure * inverse
    sound = square * lax.rsqrt(square)
    return [pressure, sound, *velocity]


def sensor_of(upper, middle, lower):
    outer = upper + lower
    twice = 2.0 * middle
    return jnp.abs(outer - twice) / (outer + twice)


def face_flux(component, cons, pressure, sound, velocity, sensor, grid_speed):
    half = [0.5 * (v - grid_speed) if grid_speed is not None else 0.5 * v for v in velocity]
    speed = jnp.abs(half[0]) + jnp.abs(half[1]) + 0.5 * (sound[0] + sound[1])
    second = SECOND_COEF * jnp.maximum(sensor[0], sensor[1])
    fourth = jnp.maximum(0.0, FOURTH_COEF - second)
    outer = speed * fourth
    inner = speed * (second + 3.0 * fourth)
    near = half[0] + inner
    far = half[1] - inner
    fluxes = []
    for m in range(NCOMP):
        before, left, right, beyond = cons[m]
        flux = right * far + left * near + outer * (beyond - before)
        if m == component:
            flux = flux + 0.5 * (pressure[0] + pressure[1])
        if m == 4:
            flux = flux + 0.5 * (pressure[0] * velocity[0] + pressure[1] * velocity[1])
        fluxes.append(flux)
    return fluxes


def circ_face(cons, at, pressure, sound, velocity, sensor_before, spin):
    sensor = sensor_of(pressure[2], pressure[1], pressure[0])
    flux = face_flux(
        2,
        [[cons(m, d) for d in (-1, 0, 1, 2)] for m in range(NCOMP)],
        pressure[:2],
        sound,
        velocity,
        [sensor_before, sensor],
        spin,
    )
    return flux, sensor


def inner_kernel(flags, state, source, out, cons, prim, src, partial, circ_flux, circ_sensor, sems):
    planes = state.shape[1]
    chunks = state.shape[3] // LANES
    group = 8
    groups = planes // group
    loads = []
    for g in range(groups):
        part = pl.ds(g * group, group)
        loads.append(
            [
                begin(state.at[:, part], cons.at[:, part], sems.at[2 * g]),
                begin(source.at[:, part], src.at[:, part], sems.at[2 * g + 1]),
            ]
        )
    k = 2 * groups
    rotor = flags[2]
    spin = GRID_SPEED * rotor.astype(jnp.float32)
    lane = lane_index(16)

    def cell(m, j, c):
        return cons[m, j, :, c * LANES : (c + 1) * LANES]

    def prepare(j, carry):
        for c in range(chunks):
            fields = primitives([cell(m, j, c) for m in range(NCOMP)])
            for f in range(4):
                prim[f, j, c] = fields[f]
        return carry

    keep_first = lane >= jnp.where(rotor == 1, 2, 0)
    keep_last = lane < jnp.where(rotor == 1, LANES, LANES - 2)

    def behind(parts):
        turned = [pltpu.roll(x, 1, 1) for x in parts]
        before = [parts[0]] + turned[:-1]
        return [jnp.where(lane < 1, before[c], turned[c]) for c in range(chunks)]

    def behind_two(parts, behind_one):
        turned = [pltpu.roll(x, 2, 1) for x in parts]
        before = [behind_one[0]] + turned[:-1]
        return [jnp.where(lane < 2, before[c], turned[c]) for c in range(chunks)]

    def ahead(parts, end):
        turned = [pltpu.roll(x, LANES - 1, 1) for x in parts]
        after = turned[1:] + [end]
        return [jnp.where(lane < LANES - 1, turned[c], after[c]) for c in range(chunks)]

    def axial_part(j):
        state_parts = [[cell(m, j, c) for c in range(chunks)] for m in range(NCOMP)]
        p, sound, speed = [[prim[f, j, c] for c in range(chunks)] for f in (0, 1, 2)]
        p_before = behind(p)
        p_after = ahead(p, p[-1])
        sensor = [sensor_of(p_after[c], p[c], p_before[c]) for c in range(chunks)]
        turned = [pltpu.roll(x, 1, 1) for x in sensor]
        before = [jnp.zeros((16, LANES), jnp.float32)] + turned[:-1]
        sensor_before = [jnp.where(lane < 1, before[c], turned[c]) for c in range(chunks)]
        sound_before = behind(sound)
        speed_before = behind(speed)
        shifted = []
        for x in state_parts:
            one = behind(x)
            shifted.append((behind_two(x, one), one, x, ahead(x, x[-1])))
        flux = [
            face_flux(
                1,
                [[shifted[m][d][c] for d in range(4)] for m in range(NCOMP)],
                [p_before[c], p[c]],
                [sound_before[c], sound[c]],
                [speed_before[c], speed[c]],
                [sensor_before[c], sensor[c]],
                None,
            )
            for c in range(chunks)
        ]
        e = chunks - 1
        end = face_flux(
            1,
            [
                (shifted[m][1][e], state_parts[m][e], state_parts[m][e], state_parts[m][e])
                for m in range(NCOMP)
            ],
            [p[e], p[e]],
            [sound[e], sound[e]],
            [speed[e], speed[e]],
            [sensor[e], sensor[e]],
            None,
        )
        for m in range(NCOMP):
            parts = [flux[c][m] for c in range(chunks)]
            upper = ahead(parts, end[m])
            for c in range(chunks):
                value = upper[c] - parts[c]
                if c == 0:
                    value = jnp.where(keep_first, value, 0.0)
                if c == chunks - 1:
                    value = jnp.where(keep_last, value, 0.0)
                cols = pl.ds(c * LANES, LANES)
                partial[m, j, :, cols] = value + RATE * state_parts[m][c] + src[m, j, :, cols]

    def circ_part(j):
        for c in range(chunks):
            flux, sensor = circ_face(
                lambda m, d: cell(m, j + d, c),
                j,
                [prim[0, j + d, c] for d in (0, 1, 2)],
                [prim[1, j + d, c] for d in (0, 1)],
                [prim[3, j + d, c] for d in (0, 1)],
                circ_sensor[c],
                spin,
            )
            circ_sensor[c] = sensor
            cols = pl.ds(c * LANES, LANES)
            for m in range(NCOMP):
                value = flux[m] - circ_flux[m, c]
                circ_flux[m, c] = flux[m]
                partial[m, j, :, cols] = partial[m, j, :, cols] + jnp.where(j >= 2, value, 0.0)

    def body(j, carry):
        prepare(j + 2, 0)
        axial_part(j)
        circ_part(j)
        return carry

    stores = []

    def store(g):
        stores.append(
            begin(
                partial.at[:, pl.ds(g * group, group)],
                out.at[:, pl.ds(g * group, group)],
                sems.at[k + g],
            )
        )

    for copy in loads[0]:
        copy.wait()
    lax.fori_loop(0, 3, prepare, 0)
    for c in range(chunks):
        circ_sensor[c] = sensor_of(prim[0, 2, c], prim[0, 1, c], prim[0, 0, c])
    axial_part(0)
    done = 1
    for g in range(groups):
        stop = (g + 1) * group - 2
        lax.fori_loop(done, stop, body, 0)
        done = stop
        if g + 1 < groups:
            for copy in loads[g + 1]:
                copy.wait()
        if g > 0:
            store(g - 1)

    def last(j, carry):
        axial_part(j)
        return carry

    lax.fori_loop(planes - 2, planes, last, 0)
    store(groups - 1)
    for copy in stores:
        copy.wait()


def inner_parts(flags, cells, source):
    planes, rows, length = cells.shape[1:]
    chunks = length // LANES
    f32 = jnp.float32
    chunked = (planes, chunks, rows, LANES)
    return pl.pallas_call(
        inner_kernel,
        out_shape=jax.ShapeDtypeStruct(cells.shape, f32),
        in_specs=[smem()] + [hbm()] * 2,
        out_specs=hbm(),
        scratch_shapes=[
            pltpu.VMEM(cells.shape, f32),
            pltpu.VMEM((4,) + chunked, f32),
            pltpu.VMEM(cells.shape, f32),
            pltpu.VMEM(cells.shape, f32),
            pltpu.VMEM((NCOMP, chunks, rows, LANES), f32),
            pltpu.VMEM((chunks, rows, LANES), f32),
            pltpu.SemaphoreType.DMA((planes // 8 * (chunks + 2),)),
        ],
        compiler_params=pltpu.CompilerParams(vmem_limit_bytes=50 * MIB),
        cost_estimate=pl.CostEstimate(
            flops=30_000_000_000, transcendentals=0, bytes_accessed=15_000_000
        ),
        name="inner_parts",
    )(flags, cells, source)


def outer_kernel(
    flags,
    offsets,
    weights,
    state,
    partial_in,
    pseudo,
    circ_low,
    circ_high,
    own_a,
    own_b,
    halo_a,
    halo_b,
    plane,
    table_high,
    table_low,
    out,
    out_circ_low,
    out_circ_high,
    out_a,
    out_b,
    out_low_a,
    out_low_b,
    out_high_a,
    out_high_b,
    cons,
    prim,
    partial,
    step,
    raw_high,
    raw_low,
    result,
    tables,
    own,
    halo,
    top_flux,
    cycle,
    ghosts,
    rad_flux,
    packs,
    beside,
    sems,
):
    planes = state.shape[1]
    chunks = state.shape[3] // LANES
    group = 8
    groups = planes // group
    cells = pl.ds(FIRST, 16)
    rotor = flags[2]
    odd = flags[3]

    loads = []
    for g in range(groups):
        part = pl.ds(g * group, group)
        loads.append(begin(state.at[:, part], result.at[:, part], sems.at[g]))
    k = groups
    rims = [
        begin(own_a, own.at[1 - odd], sems.at[k]),
        begin(own_b, own.at[odd], sems.at[k + 1]),
        begin(halo_a, halo.at[1 - odd], sems.at[k + 2]),
        begin(halo_b, halo.at[odd], sems.at[k + 3]),
    ]
    k += 4
    sides = [
        begin(circ_low, beside.at[0], sems.at[k]),
        begin(circ_high, beside.at[1], sems.at[k + 1]),
    ]
    k += 2
    late = [
        begin(partial_in, partial, sems.at[k]),
        begin(pseudo, step, sems.at[k + 1]),
        begin(table_high, tables.at[0], sems.at[k + 2]),
        begin(table_low, tables.at[1], sems.at[k + 3]),
    ]
    k += 4
    lane8 = lane_index(8)
    lane = lane_index(16)

    count = plane.shape[0]
    width = plane.shape[2]
    for h in range(2):
        for s in range(count):
            cycle[h, pl.ds(s * width, width), :] = plane[s, h]
        cycle[h, pl.ds(count * width, width), :] = plane[0, h]
        cycle[h, pl.ds((count + 1) * width, 8), :] = plane[1, h, 0:8]
    around = count * width
    starts, leads, trails = [], [], []
    for r in range(16):
        ahead_by = jnp.where(rotor == 1, flags[4] + offsets[r], flags[4] - offsets[r] - 1 + around)
        starts.append(jnp.where(ahead_by >= around, ahead_by - around, ahead_by))
        leads.append(jnp.where(rotor == 1, 1.0 - weights[r], weights[r]))
        trails.append(jnp.where(rotor == 1, weights[r], 1.0 - weights[r]))
    for h in range(2):
        for jt in range(planes // 8):
            total = jnp.zeros((8, LANES), jnp.float32)
            for r in range(8):
                at = starts[8 * h + r] + 8 * jt
                value = (
                    leads[8 * h + r] * cycle[h, pl.ds(at, 8), :]
                    + trails[8 * h + r] * cycle[h, pl.ds(at + 1, 8), :]
                )
                to = (8 - r) % 8
                if to != r:
                    value = pltpu.roll(value, (to - r) % 8 * 16, 1)
                total = jnp.where(((lane8 + 2) & (LANES - 1)) // 16 == to, value, total)
            ghosts[h, pl.ds(8 * jt, 8), :] = total

    for copy in rims:
        copy.wait()

    def mirror(side):
        def body(q, carry):
            for m in range(NCOMP):
                sign = -1.0 if m == 3 else 1.0
                for i in range(2):
                    halo[side, m, q, i] = sign * own[side, m, q, 1 - i]
            return carry

        lax.fori_loop(0, planes // 2, body, 0)

    @pl.when(flags[0] == 1)
    def _():
        mirror(0)

    @pl.when(flags[1] == 1)
    def _():
        mirror(1)

    def rim(q, carry):
        low = [[halo[0, m, q, i] for m in range(NCOMP)] for i in range(2)]
        high = [[own[1, m, q, i] for m in range(NCOMP)] for i in range(2)]
        high += [[halo[1, m, q, i] for m in range(NCOMP)] for i in range(2)]
        low_fields = [primitives(x) for x in low]
        fields = [primitives(x) for x in high]
        p = [x[0] for x in fields]
        flux = face_flux(
            3,
            [[high[d][m] for d in range(4)] for m in range(NCOMP)],
            p[1:3],
            [fields[1][1], fields[2][1]],
            [fields[1][4], fields[2][4]],
            [sensor_of(p[2], p[1], p[0]), sensor_of(p[3], p[2], p[1])],
            None,
        )
        for m in range(NCOMP):
            top_flux[m, q] = flux[m]
        for e in range(2):
            at = 2 * q + e + 2
            for c in range(chunks):
                w = 4 * e + c
                for m in range(NCOMP):
                    for i in range(2):
                        cons[m, at, c, FIRST - 2 + i : FIRST - 1 + i, :] = low[i][m][w : w + 1]
                    cons[m, at, c, FIRST + 16 : FIRST + 17, :] = high[2][m][w : w + 1]
                for i in range(2):
                    prim[0, at, c, FIRST - 2 + i : FIRST - 1 + i, :] = low_fields[i][0][w : w + 1]
                prim[0, at, c, FIRST + 16 : FIRST + 17, :] = fields[2][0][w : w + 1]
                prim[1, at, c, FIRST - 1 : FIRST, :] = low_fields[1][1][w : w + 1]
                prim[2, at, c, FIRST - 1 : FIRST, :] = low_fields[1][4][w : w + 1]
        return carry

    lax.fori_loop(0, planes // 2, rim, 0)

    def place(source_of, at):
        for c in range(chunks):
            values = [source_of(m, pl.ds(c * LANES, LANES)) for m in range(NCOMP)]
            fields = primitives(values)
            for m in range(NCOMP):
                cons[m, at, c, cells, :] = values[m]
            prim[0, at, c, cells, :] = fields[0]
            prim[1, at, c, cells, :] = fields[1]
            prim[2, at, c, cells, :] = fields[4]

    def prepare(j, carry):
        place(lambda m, cols: result[m, j, :, cols], j + 2)
        return carry

    def prepare_side(i, carry):
        for side, first in ((0, 0), (1, planes + 2)):
            place(lambda m, cols: beside[side, m, i, :, cols], first + i)
        return carry

    for g in range(groups):
        loads[g].wait()
        lax.fori_loop(g * group, (g + 1) * group, prepare, 0)
    for copy in sides:
        copy.wait()
    lax.fori_loop(0, 2, prepare_side, 0)
    for copy in late:
        copy.wait()

    spin = GRID_SPEED * rotor.astype(jnp.float32)

    def swirl(j, c):
        return cons[2, j, c, cells, :] / cons[0, j, c, cells, :]

    def circ_edges(c, carry):
        cols = pl.ds(pl.multiple_of(c * LANES, LANES), LANES)
        for base in (1, planes - 1):
            before = sensor_of(*[prim[0, base + d, c, cells, :] for d in (1, 0, -1)])
            fluxes = []
            for f in range(3):
                at = base + f
                flux, before = circ_face(
                    lambda m, d: cons[m, at + d, c, cells, :],
                    at,
                    [prim[0, at + d, c, cells, :] for d in (0, 1, 2)],
                    [prim[1, at + d, c, cells, :] for d in (0, 1)],
                    [swirl(at + d, c) for d in (0, 1)],
                    before,
                    spin,
                )
                fluxes.append(flux)
            for f in range(2):
                j = base - 1 + f
                for m in range(NCOMP):
                    partial[m, j, :, cols] = (
                        partial[m, j, :, cols] + fluxes[f + 1][m] - fluxes[f][m]
                    )
        return carry

    lax.fori_loop(0, chunks, circ_edges, 0)

    ghost_lanes = (lane < 64) == (jnp.where(rotor == 1, 1, 0) == 0)
    end_chunk = jnp.where(rotor == 1, 0, chunks - 1)
    end_cols = pl.ds(pl.multiple_of(end_chunk * LANES, LANES), LANES)
    end_lanes = (lane - jnp.where(rotor == 1, 0, LANES - 2)).astype(jnp.uint32) < 2

    def ends_at(j):
        at = j + 2
        spread = jnp.concatenate(
            [
                pltpu.roll(
                    jnp.broadcast_to(ghosts[h, pl.ds(j, 1), :], (8, LANES)),
                    0,
                    1,
                    stride=16,
                    stride_axis=0,
                )
                for h in range(2)
            ],
            axis=0,
        )
        joined = []
        for m in range(NCOMP):
            moved = pltpu.roll(spread, LANES - 2 * m, 1) if m else spread
            joined.append(jnp.where(ghost_lanes, moved, cons[m, at, end_chunk, cells, :]))
        p, sound, speed = primitives(joined)[:3]
        p_before = pltpu.roll(p, 1, 1)
        sensor = sensor_of(pltpu.roll(p, LANES - 1, 1), p, p_before)
        flux = face_flux(
            1,
            [
                (pltpu.roll(x, 2, 1), pltpu.roll(x, 1, 1), x, pltpu.roll(x, LANES - 1, 1))
                for x in joined
            ],
            [p_before, p],
            [pltpu.roll(sound, 1, 1), sound],
            [pltpu.roll(speed, 1, 1), speed],
            [pltpu.roll(sensor, 1, 1), sensor],
            None,
        )
        for m in range(NCOMP):
            value = pltpu.roll(flux[m], LANES - 1, 1) - flux[m]
            partial[m, j, :, end_cols] = partial[m, j, :, end_cols] + jnp.where(
                end_lanes, value, 0.0
            )

    def ends(q, carry):
        for e in range(8):
            ends_at(8 * q + e)
        return carry

    lax.fori_loop(0, planes // 8, ends, 0)

    def radial_chunk(j, c, e, q):
        at = j + 2
        p = [prim[0, at, c, pl.ds(FIRST + d, 16), :] for d in (-2, -1, 0, 1)]
        flux = face_flux(
            3,
            [
                [cons[m, at, c, pl.ds(FIRST + d, 16), :] for d in (-2, -1, 0, 1)]
                for m in range(NCOMP)
            ],
            p[1:3],
            [prim[1, at, c, pl.ds(FIRST + d, 16), :] for d in (-1, 0)],
            [prim[2, at, c, pl.ds(FIRST + d, 16), :] for d in (-1, 0)],
            [sensor_of(p[2], p[1], p[0]), sensor_of(p[3], p[2], p[1])],
            None,
        )
        cols = pl.ds(c * LANES, LANES)
        pace = step[j, :, cols]
        for m in range(NCOMP):
            rad_flux[m, e, c, 0:16, :] = flux[m]
            rad_flux[m, e, c, 16:17, :] = top_flux[m, q, 4 * e + c : 4 * e + c + 1, :]
            raw = pace * (partial[m, j, :, cols] + (rad_flux[m, e, c, 1:17, :] - flux[m]))
            high = raw.astype(jnp.bfloat16)
            raw_high[m, j, :, cols] = high
            raw_low[m, j, :, cols] = (raw - high.astype(jnp.float32)).astype(jnp.bfloat16)

    def radial(q, carry):
        for e in range(2):
            for c in range(chunks):
                radial_chunk(2 * q + e, c, e, q)
        return carry

    lax.fori_loop(0, planes // 2, radial, 0)

    stores = []
    length = chunks * LANES
    for g in range(groups):
        part = pl.ds(g * group, group)
        high = raw_high[:, part].reshape(NCOMP * group * 16, length)
        low = raw_low[:, part].reshape(NCOMP * group * 16, length)
        value = (
            jnp.dot(high, tables[0], preferred_element_type=jnp.float32)
            + jnp.dot(high, tables[1], preferred_element_type=jnp.float32)
            + jnp.dot(low, tables[0], preferred_element_type=jnp.float32)
        )
        result[:, part] = value.reshape(NCOMP, group, 16, length)
        stores.append(begin(result.at[:, part], out.at[:, part], sems.at[k]))
        k += 1
    stores += [
        begin(result.at[:, 0:2], out_circ_low, sems.at[k]),
        begin(result.at[:, planes - 2 : planes], out_circ_high, sems.at[k + 1]),
    ]
    k += 2

    def pick(j, carry):
        for m in range(NCOMP):
            for c in range(chunks):
                cols = pl.ds(c * LANES, LANES)
                packs[1 - odd, m, j, pl.ds(2 * c, 2), :] = result[m, j, 0:2, cols]
                packs[odd, m, j, pl.ds(2 * c, 2), :] = result[m, j, 14:16, cols]
        return carry

    lax.fori_loop(0, planes, pick, 0)
    for i, (whole, low, high) in enumerate(
        ((out_a, out_low_a, out_high_a), (out_b, out_low_b, out_high_b))
    ):
        stores.append(begin(packs.at[i], whole, sems.at[k]))
        stores.append(begin(packs.at[i, :, 0:2], low, sems.at[k + 1]))
        stores.append(begin(packs.at[i, :, planes - 2 : planes], high, sems.at[k + 2]))
        k += 3
    for copy in stores:
        copy.wait()


def outer_parts(flags, offsets, weights, cells, partial, pseudo, circs, own, halos, plane):
    planes, rows, length = cells.shape[1:]
    chunks = length // LANES
    table = -axial_table(length).astype(np.float32)
    table_high = table.astype(jnp.bfloat16)
    table_low = (table - table_high.astype(np.float32)).astype(jnp.bfloat16)
    f32 = jnp.float32
    rad = jax.ShapeDtypeStruct((NCOMP, planes, 8, LANES), f32)
    corner = jax.ShapeDtypeStruct((NCOMP, 2, 8, LANES), f32)
    circ = jax.ShapeDtypeStruct((NCOMP, 2, rows, length), f32)
    groups = planes // 8
    buffer = (planes + 4, chunks, ROWS, LANES)
    rims = (2, NCOMP, planes // 2, 2, 8, LANES)
    return pl.pallas_call(
        outer_kernel,
        out_shape=(jax.ShapeDtypeStruct(cells.shape, f32), circ, circ, rad, rad) + (corner,) * 4,
        in_specs=[smem()] * 3 + [hbm()] * 9 + [vmem()] + [hbm()] * 2,
        out_specs=(hbm(),) * 9,
        scratch_shapes=[
            pltpu.VMEM((NCOMP,) + buffer, f32),
            pltpu.VMEM((3,) + buffer, f32),
            pltpu.VMEM(cells.shape, f32),
            pltpu.VMEM(pseudo.shape, f32),
            pltpu.VMEM(cells.shape, jnp.bfloat16),
            pltpu.VMEM(cells.shape, jnp.bfloat16),
            pltpu.VMEM(cells.shape, f32),
            pltpu.VMEM((2, length, length), jnp.bfloat16),
            pltpu.VMEM(rims, f32),
            pltpu.VMEM(rims, f32),
            pltpu.VMEM((NCOMP, planes // 2, 8, LANES), f32),
            pltpu.VMEM((2, plane.shape[0] * planes + planes + 8, LANES), f32),
            pltpu.VMEM((2, planes, LANES), f32),
            pltpu.VMEM((NCOMP, 2, chunks, 24, LANES), f32),
            pltpu.VMEM((2, NCOMP, planes, 8, LANES), f32),
            pltpu.VMEM((2,) + circ.shape, f32),
            pltpu.SemaphoreType.DMA((2 * groups + 18,)),
        ],
        compiler_params=pltpu.CompilerParams(vmem_limit_bytes=58 * MIB),
        name="outer_parts",
    )(
        flags,
        offsets,
        weights,
        cells,
        partial,
        pseudo,
        *circs,
        *own,
        *halos,
        plane,
        jnp.asarray(table_high),
        jnp.asarray(table_low),
    )


def smooth_kernel(
    flags,
    field,
    circ_low,
    circ_high,
    rim_a,
    rim_b,
    low_a,
    low_b,
    high_a,
    high_b,
    out,
    buf,
    mid,
    done,
    rims,
    land,
    beside,
    sems,
):
    planes = field.shape[1]
    chunks = field.shape[3] // LANES
    cells = pl.ds(FIRST, 16)
    group = 8

    odd = flags[3]
    groups = planes // group
    copies = []
    for g in range(groups):
        part = pl.ds(g * group, group)
        copies.append(begin(field.at[:, part], land.at[:, part], sems.at[g]))
    k = groups
    copies += [
        begin(circ_low, beside.at[0], sems.at[k]),
        begin(circ_high, beside.at[1], sems.at[k + 1]),
    ]
    k += 2
    pieces = []
    for side, parts in ((1 - odd, (low_a, rim_a, high_a)), (odd, (low_b, rim_b, high_b))):
        for part, first, count in zip(parts, (0, 2, planes + 2), (2, planes, 2)):
            pieces.append(begin(part, rims.at[side, :, pl.ds(first, count)], sems.at[k]))
            k += 1
    for copy in pieces:
        copy.wait()

    def put(j, carry):
        for m in range(NCOMP):
            for c in range(chunks):
                buf[m, j, c, pl.ds(FIRST - 2, 2), :] = rims[0, m, j, pl.ds(2 * c, 2), :]
                buf[m, j, c, pl.ds(FIRST + 16, 2), :] = rims[1, m, j, pl.ds(2 * c, 2), :]
        return carry

    lax.fori_loop(0, planes + 4, put, 0)

    def place(j, carry):
        for m in range(NCOMP):
            for c in range(chunks):
                buf[m, j + 2, c, cells, :] = land[m, j, :, c * LANES : (c + 1) * LANES]
        return carry

    for g in range(groups):
        copies[g].wait()
        lax.fori_loop(g * group, (g + 1) * group, place, 0)
    for copy in copies[groups:]:
        copy.wait()

    def place_side(i, carry):
        for side, first in ((0, 0), (1, planes + 2)):
            for m in range(NCOMP):
                for c in range(chunks):
                    buf[m, first + i, c, cells, :] = beside[side, m, i, :, c * LANES : (c + 1) * LANES]
        return carry

    lax.fori_loop(0, 2, place_side, 0)

    def wall(zero_row, odd_row, from_row):
        def body(j, carry):
            for m in range(NCOMP):
                for c in range(chunks):
                    buf[m, j, c, pl.ds(zero_row, 1), :] = jnp.zeros((1, LANES), jnp.float32)
                    buf[m, j, c, pl.ds(odd_row, 1), :] = -buf[m, j, c, pl.ds(from_row, 1), :]
            return carry

        lax.fori_loop(0, planes + 4, body, 0)

    @pl.when(flags[0] == 1)
    def _():
        wall(FIRST - 1, FIRST - 2, FIRST)

    @pl.when(flags[1] == 1)
    def _():
        wall(FIRST + 16, FIRST + 17, FIRST + 15)

    def weights(coupling):
        own = 1.0 / (1.0 + 2.0 * coupling)
        side = coupling / (1.0 + 2.0 * coupling)
        return own * own + 2.0 * side * side, 2.0 * own * side, side * side

    def radial(j, carry):
        w0, w1, w2 = weights(RADIAL_COUPLING)
        for m in range(NCOMP):
            for c in range(chunks):
                x = [buf[m, j, c, pl.ds(FIRST + d, 16), :] for d in (-2, -1, 0, 1, 2)]
                mid[m, j, c] = w0 * x[2] + w1 * (x[1] + x[3]) + w2 * (x[0] + x[4])
        return carry

    lax.fori_loop(0, planes + 4, radial, 0)

    def around(j, carry):
        w0, w1, w2 = weights(CIRC_COUPLING)
        for m in range(NCOMP):
            for c in range(chunks):
                x = [mid[m, j + d, c] for d in range(5)]
                done[m, j, :, pl.ds(c * LANES, LANES)] = (
                    w0 * x[2] + w1 * (x[1] + x[3]) + w2 * (x[0] + x[4])
                )
        return carry

    stores = []
    for g in range(planes // group):
        lax.fori_loop(g * group, (g + 1) * group, around, 0)
        stores.append(
            begin(done.at[:, pl.ds(g * group, group)], out.at[:, pl.ds(g * group, group)], sems.at[k])
        )
        k += 1
    for copy in stores:
        copy.wait()


def smoothed(flags, field, halos):
    planes, rows, length = field.shape[1:]
    chunks = length // LANES
    f32 = jnp.float32
    return pl.pallas_call(
        smooth_kernel,
        out_shape=jax.ShapeDtypeStruct(field.shape, f32),
        in_specs=[smem()] + [hbm()] * 9,
        out_specs=hbm(),
        scratch_shapes=[
            pltpu.VMEM((NCOMP, planes + 4, chunks, ROWS, LANES), f32),
            pltpu.VMEM((NCOMP, planes + 4, chunks, rows, LANES), f32),
            pltpu.VMEM(field.shape, f32),
            pltpu.VMEM((2, NCOMP, planes + 4, 8, LANES), f32),
            pltpu.VMEM(field.shape, f32),
            pltpu.VMEM((2, NCOMP, 2, rows, length), f32),
            pltpu.SemaphoreType.DMA((2 * (planes // 8) + 8,)),
        ],
        compiler_params=pltpu.CompilerParams(vmem_limit_bytes=50 * MIB),
        name="smoothing",
    )(flags, field, *halos)


def ring(count):
    return [(i, (i + 1) % count) for i in range(count)]


def back(pairs):
    return [(b, a) for a, b in pairs]


def rims_of(count):
    first = [(i, i ^ 1) for i in range(count)]
    second = [(i, ((i + 1) ^ 1) - 1 if 0 < i < count - 1 else i) for i in range(count)]
    return first, second


def crossed(circ_pairs, rad_pairs, rads):
    return [(a * rads + c, b * rads + d) for a, b in circ_pairs for c, d in rad_pairs]


def on_device(state, time_source, pseudo_step, offsets, weights):
    cells = state[0]
    source = time_source[0]
    pseudo = pseudo_step[0]
    planes = cells.shape[1]
    circs = lax.axis_size("circ")
    rads = lax.axis_size("rad")
    row = lax.axis_index("row")
    rad = lax.axis_index("rad")
    flags = jnp.stack(
        [
            (rad == 0).astype(jnp.int32),
            (rad == rads - 1).astype(jnp.int32),
            row.astype(jnp.int32),
            (rad % 2).astype(jnp.int32),
            (lax.axis_index("circ") * planes).astype(jnp.int32),
        ]
    )
    up = ring(circs)
    down = back(up)
    pairs_a, pairs_b = rims_of(rads)

    own_a, own_b, circ_low, circ_high, face = edges(flags, cells)
    facing = lax.ppermute(face, "row", [(0, 1), (1, 0)])
    spread = jnp.broadcast_to(facing[None], (circs, *facing.shape))
    own_a, own_b, circ_low, circ_high, spread = lax.optimization_barrier(
        (own_a, own_b, circ_low, circ_high, spread)
    )
    plane = lax.all_to_all(spread, "circ", 0, 0, tiled=True)
    halo_circs = (lax.ppermute(circ_high, "circ", up), lax.ppermute(circ_low, "circ", down))
    halo_rads = (lax.ppermute(own_a, "rad", pairs_a), lax.ppermute(own_b, "rad", pairs_b))
    partial = inner_parts(flags, cells, source)

    field, circ_low, circ_high, rim_a, rim_b, low_a, low_b, high_a, high_b = outer_parts(
        flags,
        offsets,
        weights,
        cells,
        partial,
        pseudo,
        halo_circs,
        (own_a, own_b),
        halo_rads,
        plane,
    )
    both = ("circ", "rad")
    halos = (
        lax.ppermute(circ_high, "circ", up),
        lax.ppermute(circ_low, "circ", down),
        lax.ppermute(rim_a, "rad", pairs_a),
        lax.ppermute(rim_b, "rad", pairs_b),
        lax.ppermute(high_a, both, crossed(up, pairs_a, rads)),
        lax.ppermute(high_b, both, crossed(up, pairs_b, rads)),
        lax.ppermute(low_a, both, crossed(down, pairs_a, rads)),
        lax.ppermute(low_b, both, crossed(down, pairs_b, rads)),
    )
    return smoothed(flags, field, halos)[None]


def solution(mesh):
    return jax.shard_map(
        on_device,
        mesh=mesh,
        in_specs=(
            P("row", None, "circ", "rad", None),
            P("row", None, "circ", "rad", None),
            P("row", "circ", "rad", None),
            P("rad"),
            P("rad"),
        ),
        out_specs=P("row", None, "circ", "rad", None),
        check_vma=False,
    )
```

```python
import math

import jax
import jax.numpy as jnp
import numpy as np
from jax import lax
from jax.experimental import pallas as pl
from jax.experimental.pallas import tpu as pltpu
from jax.sharding import PartitionSpec as P

GAMMA = 1.4
GAMMA_LESS = 0.4
SECOND_COEF = 0.5
FOURTH_COEF = 0.03125
RATE = 0.75
GRID_SPEED = 0.5
AXIAL_COUPLING = 0.8
CIRC_COUPLING = 0.6
RADIAL_COUPLING = 0.6

NCOMP = 5
LANES = 128
ROWS = 32
FIRST = 8
MIB = 1 << 20


def axial_table(length):
    modes_index = np.arange(1, length + 1) * 1.0
    angle = np.pi / (length + 1)
    modes = np.sin(np.outer(modes_index, modes_index) * angle)
    eigen = 1.0 + 2.0 * AXIAL_COUPLING - 2.0 * AXIAL_COUPLING * np.cos(modes_index * angle)
    return modes / eigen[None, :] @ modes.T * (2.0 / (length + 1))


def vmem():
    return pl.BlockSpec(memory_space=pltpu.VMEM)


def smem():
    return pl.BlockSpec(memory_space=pltpu.SMEM)


def hbm():
    return pl.BlockSpec(memory_space=pltpu.HBM)


def lane_index(rows):
    return lax.broadcasted_iota(jnp.int32, (rows, LANES), 1)


def begin(a, b, s):
    copy = pltpu.make_async_copy(a, b, s)
    copy.start()
    return copy


def edges_kernel(flags, state, pack_a, pack_b, circ_low, circ_high, face, buf, packs, sems):
    planes = state.shape[1]
    chunks = state.shape[3] // LANES
    group = 8
    groups = planes // group
    loads = []
    for g in range(groups):
        part = pl.ds(g * group, group)
        loads.append(begin(state.at[:, part], buf.at[:, part], sems.at[g]))
    k = groups
    rotor = flags[2]
    odd = flags[3]
    end_cols = pl.ds(pl.multiple_of(jnp.where(rotor == 1, 0, (chunks - 1) * LANES), LANES), LANES)
    lane = lane_index(8)
    sub = lax.broadcasted_iota(jnp.int32, (8, LANES), 0)
    behind_by = jnp.where(rotor == 1, 0, 2)
    for g in range(groups):
        loads[g].wait()

        def body(q, carry):
            for m in range(NCOMP):
                for e in range(2):
                    for c in range(chunks):
                        at = pl.ds(4 * e + c, 1)
                        for i in range(2):
                            cols = pl.ds(c * LANES, LANES)
                            low = buf[m, 2 * q + e, i : i + 1, cols]
                            high = buf[m, 2 * q + e, 14 + i : 15 + i, cols]
                            packs[1 - odd, m, q, i, at, :] = low
                            packs[odd, m, q, i, at, :] = high
            for e in range(2):
                j = 2 * q + e
                for h in range(2):
                    total = jnp.zeros((8, LANES), jnp.float32)
                    for m in range(NCOMP):
                        moved = pltpu.roll(
                            buf[m, j, 8 * h : 8 * h + 8, end_cols], 2 * m, 1, stride=16, stride_axis=0
                        )
                        at = (lane + behind_by - sub * 16 - 2 * m) & (LANES - 1)
                        total = jnp.where(at < 2, moved, total)
                    face[h, pl.ds(j, 1), :] = jnp.sum(total, axis=0, keepdims=True)
            return carry

        lax.fori_loop(g * group // 2, (g + 1) * group // 2, body, 0)
    edge = [
        begin(buf.at[:, 0:2], circ_low, sems.at[k]),
        begin(buf.at[:, planes - 2 : planes], circ_high, sems.at[k + 1]),
        begin(packs.at[0], pack_a, sems.at[k + 2]),
        begin(packs.at[1], pack_b, sems.at[k + 3]),
    ]
    for copy in edge:
        copy.wait()


def edges(flags, cells):
    planes, rows, length = cells.shape[1:]
    chunks = length // LANES
    f32 = jnp.float32
    rad = jax.ShapeDtypeStruct((NCOMP, planes // 2, 2, 8, LANES), f32)
    circ = jax.ShapeDtypeStruct((NCOMP, 2, rows, length), f32)
    face = jax.ShapeDtypeStruct((2, planes, LANES), f32)
    return pl.pallas_call(
        edges_kernel,
        out_shape=(rad, rad, circ, circ, face),
        in_specs=[smem(), hbm()],
        out_specs=(hbm(),) * 4 + (vmem(),),
        scratch_shapes=[
            pltpu.VMEM(cells.shape, f32),
            pltpu.VMEM((2,) + rad.shape, f32),
            pltpu.SemaphoreType.DMA((planes // 8 + 4,)),
        ],
        compiler_params=pltpu.CompilerParams(vmem_limit_bytes=59 * MIB),
        name="state_edges",
    )(flags, cells)


def primitives(cons):
    inverse = 1.0 / cons[0]
    velocity = [cons[m] * inverse for m in (1, 2, 3)]
    kinetic = cons[1] * velocity[0] + cons[2] * velocity[1] + cons[3] * velocity[2]
    pressure = GAMMA_LESS * (cons[4] - 0.5 * kinetic)
    square = GAMMA * pressure * inverse
    sound = square * lax.rsqrt(square)
    return [pressure, sound, *velocity]


def sensor_of(upper, middle, lower):
    outer = upper + lower
    twice = 2.0 * middle
    return jnp.abs(outer - twice) / (outer + twice)


def face_flux(component, cons, pressure, sound, velocity, sensor, grid_speed):
    half = [0.5 * (v - grid_speed) if grid_speed is not None else 0.5 * v for v in velocity]
    speed = jnp.abs(half[0]) + jnp.abs(half[1]) + 0.5 * (sound[0] + sound[1])
    second = SECOND_COEF * jnp.maximum(sensor[0], sensor[1])
    fourth = jnp.maximum(0.0, FOURTH_COEF - second)
    outer = speed * fourth
    inner = speed * (second + 3.0 * fourth)
    near = half[0] + inner
    far = half[1] - inner
    fluxes = []
    for m in range(NCOMP):
        before, left, right, beyond = cons[m]
        flux = right * far + left * near + outer * (beyond - before)
        if m == component:
            flux = flux + 0.5 * (pressure[0] + pressure[1])
        if m == 4:
            flux = flux + 0.5 * (pressure[0] * velocity[0] + pressure[1] * velocity[1])
        fluxes.append(flux)
    return fluxes


def circ_face(cons, at, pressure, sound, velocity, sensor_before, spin):
    sensor = sensor_of(pressure[2], pressure[1], pressure[0])
    flux = face_flux(
        2,
        [[cons(m, d) for d in (-1, 0, 1, 2)] for m in range(NCOMP)],
        pressure[:2],
        sound,
        velocity,
        [sensor_before, sensor],
        spin,
    )
    return flux, sensor


def inner_kernel(flags, state, source, out, cons, prim, src, partial, circ_flux, circ_sensor, sems):
    planes = state.shape[1]
    chunks = state.shape[3] // LANES
    group = 8
    groups = planes // group
    loads = []
    for g in range(groups):
        part = pl.ds(g * group, group)
        loads.append(
            [
                begin(state.at[:, part], cons.at[:, part], sems.at[2 * g]),
                begin(source.at[:, part], src.at[:, part], sems.at[2 * g + 1]),
            ]
        )
    k = 2 * groups
    rotor = flags[2]
    spin = GRID_SPEED * rotor.astype(jnp.float32)
    lane = lane_index(16)

    def cell(m, j, c):
        return cons[m, j, :, c * LANES : (c + 1) * LANES]

    def prepare(j, carry):
        for c in range(chunks):
            fields = primitives([cell(m, j, c) for m in range(NCOMP)])
            for f in range(4):
                prim[f, j, c] = fields[f]
        return carry

    keep_first = lane >= jnp.where(rotor == 1, 2, 0)
    keep_last = lane < jnp.where(rotor == 1, LANES, LANES - 2)

    def behind(parts):
        turned = [pltpu.roll(x, 1, 1) for x in parts]
        before = [parts[0]] + turned[:-1]
        return [jnp.where(lane < 1, before[c], turned[c]) for c in range(chunks)]

    def behind_two(parts, behind_one):
        turned = [pltpu.roll(x, 2, 1) for x in parts]
        before = [behind_one[0]] + turned[:-1]
        return [jnp.where(lane < 2, before[c], turned[c]) for c in range(chunks)]

    def ahead(parts, end):
        turned = [pltpu.roll(x, LANES - 1, 1) for x in parts]
        after = turned[1:] + [end]
        return [jnp.where(lane < LANES - 1, turned[c], after[c]) for c in range(chunks)]

    def axial_part(j):
        state_parts = [[cell(m, j, c) for c in range(chunks)] for m in range(NCOMP)]
        p, sound, speed = [[prim[f, j, c] for c in range(chunks)] for f in (0, 1, 2)]
        p_before = behind(p)
        p_after = ahead(p, p[-1])
        sensor = [sensor_of(p_after[c], p[c], p_before[c]) for c in range(chunks)]
        turned = [pltpu.roll(x, 1, 1) for x in sensor]
        before = [jnp.zeros((16, LANES), jnp.float32)] + turned[:-1]
        sensor_before = [jnp.where(lane < 1, before[c], turned[c]) for c in range(chunks)]
        sound_before = behind(sound)
        speed_before = behind(speed)
        shifted = []
        for x in state_parts:
            one = behind(x)
            shifted.append((behind_two(x, one), one, x, ahead(x, x[-1])))
        flux = [
            face_flux(
                1,
                [[shifted[m][d][c] for d in range(4)] for m in range(NCOMP)],
                [p_before[c], p[c]],
                [sound_before[c], sound[c]],
                [speed_before[c], speed[c]],
                [sensor_before[c], sensor[c]],
                None,
            )
            for c in range(chunks)
        ]
        e = chunks - 1
        end = face_flux(
            1,
            [
                (shifted[m][1][e], state_parts[m][e], state_parts[m][e], state_parts[m][e])
                for m in range(NCOMP)
            ],
            [p[e], p[e]],
            [sound[e], sound[e]],
            [speed[e], speed[e]],
            [sensor[e], sensor[e]],
            None,
        )
        for m in range(NCOMP):
            parts = [flux[c][m] for c in range(chunks)]
            upper = ahead(parts, end[m])
            for c in range(chunks):
                value = upper[c] - parts[c]
                if c == 0:
                    value = jnp.where(keep_first, value, 0.0)
                if c == chunks - 1:
                    value = jnp.where(keep_last, value, 0.0)
                cols = pl.ds(c * LANES, LANES)
                partial[m, j, :, cols] = value + RATE * state_parts[m][c] + src[m, j, :, cols]

    def circ_part(j):
        for c in range(chunks):
            flux, sensor = circ_face(
                lambda m, d: cell(m, j + d, c),
                j,
                [prim[0, j + d, c] for d in (0, 1, 2)],
                [prim[1, j + d, c] for d in (0, 1)],
                [prim[3, j + d, c] for d in (0, 1)],
                circ_sensor[c],
                spin,
            )
            circ_sensor[c] = sensor
            cols = pl.ds(c * LANES, LANES)
            for m in range(NCOMP):
                value = flux[m] - circ_flux[m, c]
                circ_flux[m, c] = flux[m]
                partial[m, j, :, cols] = partial[m, j, :, cols] + jnp.where(j >= 2, value, 0.0)

    def body(j, carry):
        prepare(j + 2, 0)
        axial_part(j)
        circ_part(j)
        return carry

    stores = []

    def store(g):
        stores.append(
            begin(
                partial.at[:, pl.ds(g * group, group)],
                out.at[:, pl.ds(g * group, group)],
                sems.at[k + g],
            )
        )

    for copy in loads[0]:
        copy.wait()
    lax.fori_loop(0, 3, prepare, 0)
    for c in range(chunks):
        circ_sensor[c] = sensor_of(prim[0, 2, c], prim[0, 1, c], prim[0, 0, c])
    axial_part(0)
    done = 1
    for g in range(groups):
        stop = (g + 1) * group - 2
        lax.fori_loop(done, stop, body, 0)
        done = stop
        if g + 1 < groups:
            for copy in loads[g + 1]:
                copy.wait()
        if g > 0:
            store(g - 1)

    def last(j, carry):
        axial_part(j)
        return carry

    lax.fori_loop(planes - 2, planes, last, 0)
    store(groups - 1)
    for copy in stores:
        copy.wait()


def inner_parts(flags, cells, source):
    planes, rows, length = cells.shape[1:]
    chunks = length // LANES
    f32 = jnp.float32
    chunked = (planes, chunks, rows, LANES)
    return pl.pallas_call(
        inner_kernel,
        out_shape=jax.ShapeDtypeStruct(cells.shape, f32),
        in_specs=[smem()] + [hbm()] * 2,
        out_specs=hbm(),
        scratch_shapes=[
            pltpu.VMEM(cells.shape, f32),
            pltpu.VMEM((4,) + chunked, f32),
            pltpu.VMEM(cells.shape, f32),
            pltpu.VMEM(cells.shape, f32),
            pltpu.VMEM((NCOMP, chunks, rows, LANES), f32),
            pltpu.VMEM((chunks, rows, LANES), f32),
            pltpu.SemaphoreType.DMA((planes // 8 * (chunks + 2),)),
        ],
        compiler_params=pltpu.CompilerParams(vmem_limit_bytes=50 * MIB),
        cost_estimate=pl.CostEstimate(
            flops=30_000_000_000, transcendentals=0, bytes_accessed=15_000_000
        ),
        name="inner_parts",
    )(flags, cells, source)


def outer_kernel(
    flags,
    offsets,
    weights,
    state,
    partial_in,
    pseudo,
    circ_low,
    circ_high,
    own_a,
    own_b,
    halo_a,
    halo_b,
    plane,
    table_high,
    table_low,
    out,
    out_circ_low,
    out_circ_high,
    out_a,
    out_b,
    out_low_a,
    out_low_b,
    out_high_a,
    out_high_b,
    cons,
    prim,
    partial,
    step,
    raw_high,
    raw_low,
    result,
    tables,
    own,
    halo,
    top_flux,
    cycle,
    ghosts,
    rad_flux,
    packs,
    beside,
    sems,
):
    planes = state.shape[1]
    chunks = state.shape[3] // LANES
    group = 8
    groups = planes // group
    cells = pl.ds(FIRST, 16)
    rotor = flags[2]
    odd = flags[3]

    loads = []
    for g in range(groups):
        part = pl.ds(g * group, group)
        loads.append(begin(state.at[:, part], result.at[:, part], sems.at[g]))
    k = groups
    rims = [
        begin(own_a, own.at[1 - odd], sems.at[k]),
        begin(own_b, own.at[odd], sems.at[k + 1]),
        begin(halo_a, halo.at[1 - odd], sems.at[k + 2]),
        begin(halo_b, halo.at[odd], sems.at[k + 3]),
    ]
    k += 4
    sides = [
        begin(circ_low, beside.at[0], sems.at[k]),
        begin(circ_high, beside.at[1], sems.at[k + 1]),
    ]
    k += 2
    first_partial = k

    def partial_copy(g):
        part = pl.ds(g * group, group)
        return pltpu.make_async_copy(
            partial_in.at[:, part], partial.at[:, part], sems.at[first_partial + g]
        )

    for g in range(groups):
        partial_copy(g).start()
    k += groups
    late = [
        begin(pseudo, step, sems.at[k]),
        begin(table_high, tables.at[0], sems.at[k + 1]),
        begin(table_low, tables.at[1], sems.at[k + 2]),
    ]
    k += 3
    lane8 = lane_index(8)
    lane = lane_index(16)

    count = plane.shape[0]
    width = plane.shape[2]
    for h in range(2):
        for s in range(count):
            cycle[h, pl.ds(s * width, width), :] = plane[s, h]
        cycle[h, pl.ds(count * width, width), :] = plane[0, h]
        cycle[h, pl.ds((count + 1) * width, 8), :] = plane[1, h, 0:8]
    around = count * width
    starts, leads, trails = [], [], []
    for r in range(16):
        ahead_by = jnp.where(rotor == 1, flags[4] + offsets[r], flags[4] - offsets[r] - 1 + around)
        starts.append(jnp.where(ahead_by >= around, ahead_by - around, ahead_by))
        leads.append(jnp.where(rotor == 1, 1.0 - weights[r], weights[r]))
        trails.append(jnp.where(rotor == 1, weights[r], 1.0 - weights[r]))
    for h in range(2):
        for jt in range(planes // 8):
            total = jnp.zeros((8, LANES), jnp.float32)
            for r in range(8):
                at = starts[8 * h + r] + 8 * jt
                value = (
                    leads[8 * h + r] * cycle[h, pl.ds(at, 8), :]
                    + trails[8 * h + r] * cycle[h, pl.ds(at + 1, 8), :]
                )
                to = (8 - r) % 8
                if to != r:
                    value = pltpu.roll(value, (to - r) % 8 * 16, 1)
                total = jnp.where(((lane8 + 2) & (LANES - 1)) // 16 == to, value, total)
            ghosts[h, pl.ds(8 * jt, 8), :] = total

    for copy in rims:
        copy.wait()

    def mirror(side):
        def body(q, carry):
            for m in range(NCOMP):
                sign = -1.0 if m == 3 else 1.0
                for i in range(2):
                    halo[side, m, q, i] = sign * own[side, m, q, 1 - i]
            return carry

        lax.fori_loop(0, planes // 2, body, 0)

    @pl.when(flags[0] == 1)
    def _():
        mirror(0)

    @pl.when(flags[1] == 1)
    def _():
        mirror(1)

    def rim(q, carry):
        low = [[halo[0, m, q, i] for m in range(NCOMP)] for i in range(2)]
        high = [[own[1, m, q, i] for m in range(NCOMP)] for i in range(2)]
        high += [[halo[1, m, q, i] for m in range(NCOMP)] for i in range(2)]
        low_fields = [primitives(x) for x in low]
        fields = [primitives(x) for x in high]
        p = [x[0] for x in fields]
        flux = face_flux(
            3,
            [[high[d][m] for d in range(4)] for m in range(NCOMP)],
            p[1:3],
            [fields[1][1], fields[2][1]],
            [fields[1][4], fields[2][4]],
            [sensor_of(p[2], p[1], p[0]), sensor_of(p[3], p[2], p[1])],
            None,
        )
        for m in range(NCOMP):
            top_flux[m, q] = flux[m]
        for e in range(2):
            at = 2 * q + e + 2
            for c in range(chunks):
                w = 4 * e + c
                for m in range(NCOMP):
                    for i in range(2):
                        cons[m, at, c, FIRST - 2 + i : FIRST - 1 + i, :] = low[i][m][w : w + 1]
                    cons[m, at, c, FIRST + 16 : FIRST + 17, :] = high[2][m][w : w + 1]
                for i in range(2):
                    prim[0, at, c, FIRST - 2 + i : FIRST - 1 + i, :] = low_fields[i][0][w : w + 1]
                prim[0, at, c, FIRST + 16 : FIRST + 17, :] = fields[2][0][w : w + 1]
                prim[1, at, c, FIRST - 1 : FIRST, :] = low_fields[1][1][w : w + 1]
                prim[2, at, c, FIRST - 1 : FIRST, :] = low_fields[1][4][w : w + 1]
        return carry

    lax.fori_loop(0, planes // 2, rim, 0)

    def place(source_of, at):
        for c in range(chunks):
            values = [source_of(m, pl.ds(c * LANES, LANES)) for m in range(NCOMP)]
            fields = primitives(values)
            for m in range(NCOMP):
                cons[m, at, c, cells, :] = values[m]
            prim[0, at, c, cells, :] = fields[0]
            prim[1, at, c, cells, :] = fields[1]
            prim[2, at, c, cells, :] = fields[4]

    def prepare(j, carry):
        place(lambda m, cols: result[m, j, :, cols], j + 2)
        return carry

    def prepare_side(i, carry):
        for side, first in ((0, 0), (1, planes + 2)):
            place(lambda m, cols: beside[side, m, i, :, cols], first + i)
        return carry

    for g in range(groups):
        loads[g].wait()
        lax.fori_loop(g * group, (g + 1) * group, prepare, 0)
    for copy in sides:
        copy.wait()
    lax.fori_loop(0, 2, prepare_side, 0)
    spin = GRID_SPEED * rotor.astype(jnp.float32)

    def swirl(j, c):
        return cons[2, j, c, cells, :] / cons[0, j, c, cells, :]

    def circ_edges(c, carry):
        cols = pl.ds(pl.multiple_of(c * LANES, LANES), LANES)
        for base in (1, planes - 1):
            before = sensor_of(*[prim[0, base + d, c, cells, :] for d in (1, 0, -1)])
            fluxes = []
            for f in range(3):
                at = base + f
                flux, before = circ_face(
                    lambda m, d: cons[m, at + d, c, cells, :],
                    at,
                    [prim[0, at + d, c, cells, :] for d in (0, 1, 2)],
                    [prim[1, at + d, c, cells, :] for d in (0, 1)],
                    [swirl(at + d, c) for d in (0, 1)],
                    before,
                    spin,
                )
                fluxes.append(flux)
            for f in range(2):
                j = base - 1 + f
                for m in range(NCOMP):
                    partial[m, j, :, cols] = (
                        partial[m, j, :, cols] + fluxes[f + 1][m] - fluxes[f][m]
                    )
        return carry

    ghost_lanes = (lane < 64) == (jnp.where(rotor == 1, 1, 0) == 0)
    end_chunk = jnp.where(rotor == 1, 0, chunks - 1)
    end_cols = pl.ds(pl.multiple_of(end_chunk * LANES, LANES), LANES)
    end_lanes = (lane - jnp.where(rotor == 1, 0, LANES - 2)).astype(jnp.uint32) < 2

    def ends_at(j):
        at = j + 2
        spread = jnp.concatenate(
            [
                pltpu.roll(
                    jnp.broadcast_to(ghosts[h, pl.ds(j, 1), :], (8, LANES)),
                    0,
                    1,
                    stride=16,
                    stride_axis=0,
                )
                for h in range(2)
            ],
            axis=0,
        )
        joined = []
        for m in range(NCOMP):
            moved = pltpu.roll(spread, LANES - 2 * m, 1) if m else spread
            joined.append(jnp.where(ghost_lanes, moved, cons[m, at, end_chunk, cells, :]))
        p, sound, speed = primitives(joined)[:3]
        p_before = pltpu.roll(p, 1, 1)
        sensor = sensor_of(pltpu.roll(p, LANES - 1, 1), p, p_before)
        flux = face_flux(
            1,
            [
                (pltpu.roll(x, 2, 1), pltpu.roll(x, 1, 1), x, pltpu.roll(x, LANES - 1, 1))
                for x in joined
            ],
            [p_before, p],
            [pltpu.roll(sound, 1, 1), sound],
            [pltpu.roll(speed, 1, 1), speed],
            [pltpu.roll(sensor, 1, 1), sensor],
            None,
        )
        for m in range(NCOMP):
            value = pltpu.roll(flux[m], LANES - 1, 1) - flux[m]
            partial[m, j, :, end_cols] = partial[m, j, :, end_cols] + jnp.where(
                end_lanes, value, 0.0
            )

    def ends(g, carry):
        partial_copy(g).wait()
        for e in range(group):
            ends_at(group * g + e)
        return carry

    lax.fori_loop(0, groups, ends, 0)
    lax.fori_loop(0, chunks, circ_edges, 0)
    for copy in late:
        copy.wait()

    def radial_chunk(j, c, e, q):
        at = j + 2
        p = [prim[0, at, c, pl.ds(FIRST + d, 16), :] for d in (-2, -1, 0, 1)]
        flux = face_flux(
            3,
            [
                [cons[m, at, c, pl.ds(FIRST + d, 16), :] for d in (-2, -1, 0, 1)]
                for m in range(NCOMP)
            ],
            p[1:3],
            [prim[1, at, c, pl.ds(FIRST + d, 16), :] for d in (-1, 0)],
            [prim[2, at, c, pl.ds(FIRST + d, 16), :] for d in (-1, 0)],
            [sensor_of(p[2], p[1], p[0]), sensor_of(p[3], p[2], p[1])],
            None,
        )
        cols = pl.ds(c * LANES, LANES)
        pace = step[j, :, cols]
        for m in range(NCOMP):
            rad_flux[m, e, c, 0:16, :] = flux[m]
            rad_flux[m, e, c, 16:17, :] = top_flux[m, q, 4 * e + c : 4 * e + c + 1, :]
            raw = pace * (partial[m, j, :, cols] + (rad_flux[m, e, c, 1:17, :] - flux[m]))
            high = raw.astype(jnp.bfloat16)
            raw_high[m, j, :, cols] = high
            raw_low[m, j, :, cols] = (raw - high.astype(jnp.float32)).astype(jnp.bfloat16)

    length = chunks * LANES
    quad = 4

    def radial(i):
        for e in range(quad):
            for c in range(chunks):
                radial_chunk(quad * i + e, c, e % 2, (quad // 2) * i + e // 2)

    def product(i):
        part = pl.ds(quad * i, quad)
        high = raw_high[:, part].reshape(NCOMP * quad * 16, length)
        low = raw_low[:, part].reshape(NCOMP * quad * 16, length)
        value = (
            jnp.dot(high, tables[0], preferred_element_type=jnp.float32)
            + jnp.dot(high, tables[1], preferred_element_type=jnp.float32)
            + jnp.dot(low, tables[0], preferred_element_type=jnp.float32)
        )
        result[:, part] = value.reshape(NCOMP, quad, 16, length)

    def both(i, carry):
        product(i - 1)
        radial(i)
        return carry

    stores = []
    quads = planes // quad
    per = group // quad
    radial(0)
    for g in range(groups):
        lax.fori_loop(g * per + 1, min((g + 1) * per + 1, quads), both, 0)
        if g == groups - 1:
            product(quads - 1)
        part = pl.ds(g * group, group)
        stores.append(begin(result.at[:, part], out.at[:, part], sems.at[k]))
        k += 1
    stores += [
        begin(result.at[:, 0:2], out_circ_low, sems.at[k]),
        begin(result.at[:, planes - 2 : planes], out_circ_high, sems.at[k + 1]),
    ]
    k += 2

    def pick(j, carry):
        for m in range(NCOMP):
            for c in range(chunks):
                cols = pl.ds(c * LANES, LANES)
                packs[1 - odd, m, j, pl.ds(2 * c, 2), :] = result[m, j, 0:2, cols]
                packs[odd, m, j, pl.ds(2 * c, 2), :] = result[m, j, 14:16, cols]
        return carry

    lax.fori_loop(0, planes, pick, 0)
    for i, (whole, low, high) in enumerate(
        ((out_a, out_low_a, out_high_a), (out_b, out_low_b, out_high_b))
    ):
        stores.append(begin(packs.at[i], whole, sems.at[k]))
        stores.append(begin(packs.at[i, :, 0:2], low, sems.at[k + 1]))
        stores.append(begin(packs.at[i, :, planes - 2 : planes], high, sems.at[k + 2]))
        k += 3
    for copy in stores:
        copy.wait()


def outer_parts(flags, offsets, weights, cells, partial, pseudo, circs, own, halos, plane):
    planes, rows, length = cells.shape[1:]
    chunks = length // LANES
    table = -axial_table(length).astype(np.float32)
    table_high = table.astype(jnp.bfloat16)
    table_low = (table - table_high.astype(np.float32)).astype(jnp.bfloat16)
    f32 = jnp.float32
    rad = jax.ShapeDtypeStruct((NCOMP, planes, 8, LANES), f32)
    corner = jax.ShapeDtypeStruct((NCOMP, 2, 8, LANES), f32)
    circ = jax.ShapeDtypeStruct((NCOMP, 2, rows, length), f32)
    groups = planes // 8
    buffer = (planes + 4, chunks, ROWS, LANES)
    rims = (2, NCOMP, planes // 2, 2, 8, LANES)
    return pl.pallas_call(
        outer_kernel,
        out_shape=(jax.ShapeDtypeStruct(cells.shape, f32), circ, circ, rad, rad) + (corner,) * 4,
        in_specs=[smem()] * 3 + [hbm()] * 9 + [vmem()] + [hbm()] * 2,
        out_specs=(hbm(),) * 9,
        scratch_shapes=[
            pltpu.VMEM((NCOMP,) + buffer, f32),
            pltpu.VMEM((3,) + buffer, f32),
            pltpu.VMEM(cells.shape, f32),
            pltpu.VMEM(pseudo.shape, f32),
            pltpu.VMEM(cells.shape, jnp.bfloat16),
            pltpu.VMEM(cells.shape, jnp.bfloat16),
            pltpu.VMEM(cells.shape, f32),
            pltpu.VMEM((2, length, length), jnp.bfloat16),
            pltpu.VMEM(rims, f32),
            pltpu.VMEM(rims, f32),
            pltpu.VMEM((NCOMP, planes // 2, 8, LANES), f32),
            pltpu.VMEM((2, plane.shape[0] * planes + planes + 8, LANES), f32),
            pltpu.VMEM((2, planes, LANES), f32),
            pltpu.VMEM((NCOMP, 2, chunks, 24, LANES), f32),
            pltpu.VMEM((2, NCOMP, planes, 8, LANES), f32),
            pltpu.VMEM((2,) + circ.shape, f32),
            pltpu.SemaphoreType.DMA((3 * groups + 18,)),
        ],
        compiler_params=pltpu.CompilerParams(vmem_limit_bytes=58 * MIB),
        name="outer_parts",
    )(
        flags,
        offsets,
        weights,
        cells,
        partial,
        pseudo,
        *circs,
        *own,
        *halos,
        plane,
        jnp.asarray(table_high),
        jnp.asarray(table_low),
    )


def smooth_kernel(
    flags,
    field,
    circ_low,
    circ_high,
    rim_a,
    rim_b,
    low_a,
    low_b,
    high_a,
    high_b,
    out,
    buf,
    mid,
    done,
    rims,
    land,
    beside,
    sems,
):
    planes = field.shape[1]
    chunks = field.shape[3] // LANES
    cells = pl.ds(FIRST, 16)
    group = 8

    odd = flags[3]
    groups = planes // group
    copies = []
    for g in range(groups):
        part = pl.ds(g * group, group)
        copies.append(begin(field.at[:, part], land.at[:, part], sems.at[g]))
    k = groups
    copies += [
        begin(circ_low, beside.at[0], sems.at[k]),
        begin(circ_high, beside.at[1], sems.at[k + 1]),
    ]
    k += 2
    pieces = []
    for side, parts in ((1 - odd, (low_a, rim_a, high_a)), (odd, (low_b, rim_b, high_b))):
        for part, first, count in zip(parts, (0, 2, planes + 2), (2, planes, 2)):
            pieces.append(begin(part, rims.at[side, :, pl.ds(first, count)], sems.at[k]))
            k += 1
    for copy in pieces:
        copy.wait()

    def put(j, carry):
        for m in range(NCOMP):
            for c in range(chunks):
                buf[m, j, c, pl.ds(FIRST - 2, 2), :] = rims[0, m, j, pl.ds(2 * c, 2), :]
                buf[m, j, c, pl.ds(FIRST + 16, 2), :] = rims[1, m, j, pl.ds(2 * c, 2), :]
        return carry

    lax.fori_loop(0, planes + 4, put, 0)

    def place(j, carry):
        for m in range(NCOMP):
            for c in range(chunks):
                buf[m, j + 2, c, cells, :] = land[m, j, :, c * LANES : (c + 1) * LANES]
        return carry

    for copy in copies[groups:]:
        copy.wait()

    def place_side(i, carry):
        for side, first in ((0, 0), (1, planes + 2)):
            for m in range(NCOMP):
                for c in range(chunks):
                    buf[m, first + i, c, cells, :] = beside[side, m, i, :, c * LANES : (c + 1) * LANES]
        return carry

    lax.fori_loop(0, 2, place_side, 0)

    def wall(first, count, zero_row, odd_row, from_row):
        def body(j, carry):
            for m in range(NCOMP):
                for c in range(chunks):
                    buf[m, j, c, pl.ds(zero_row, 1), :] = jnp.zeros((1, LANES), jnp.float32)
                    buf[m, j, c, pl.ds(odd_row, 1), :] = -buf[m, j, c, pl.ds(from_row, 1), :]
            return carry

        lax.fori_loop(first, first + count, body, 0)

    def walls(first, count):
        @pl.when(flags[0] == 1)
        def _():
            wall(first, count, FIRST - 1, FIRST - 2, FIRST)

        @pl.when(flags[1] == 1)
        def _():
            wall(first, count, FIRST + 16, FIRST + 17, FIRST + 15)

    def weights(coupling):
        own = 1.0 / (1.0 + 2.0 * coupling)
        side = coupling / (1.0 + 2.0 * coupling)
        return own * own + 2.0 * side * side, 2.0 * own * side, side * side

    def radial(j, carry):
        w0, w1, w2 = weights(RADIAL_COUPLING)
        for m in range(NCOMP):
            for c in range(chunks):
                x = [buf[m, j, c, pl.ds(FIRST + d, 16), :] for d in (-2, -1, 0, 1, 2)]
                mid[m, j, c] = w0 * x[2] + w1 * (x[1] + x[3]) + w2 * (x[0] + x[4])
        return carry

    def around(j, carry):
        w0, w1, w2 = weights(CIRC_COUPLING)
        for m in range(NCOMP):
            for c in range(chunks):
                x = [mid[m, j + d, c] for d in range(5)]
                done[m, j, :, pl.ds(c * LANES, LANES)] = (
                    w0 * x[2] + w1 * (x[1] + x[3]) + w2 * (x[0] + x[4])
                )
        return carry

    stores = []
    walls(0, 2)
    walls(planes + 2, 2)
    lax.fori_loop(0, 2, radial, 0)
    lax.fori_loop(planes + 2, planes + 4, radial, 0)
    for g in range(groups):
        copies[g].wait()
        lax.fori_loop(g * group, (g + 1) * group, place, 0)
        walls(g * group + 2, group)
        lax.fori_loop(g * group + 2, (g + 1) * group + 2, radial, 0)
        low = max(g * group - 2, 0)
        high = (g + 1) * group - 2 if g < groups - 1 else planes
        lax.fori_loop(low, high, around, 0)
        part = pl.ds(low, high - low)
        stores.append(begin(done.at[:, part], out.at[:, part], sems.at[k]))
        k += 1
    for copy in stores:
        copy.wait()


def smoothed(flags, field, halos):
    planes, rows, length = field.shape[1:]
    chunks = length // LANES
    f32 = jnp.float32
    return pl.pallas_call(
        smooth_kernel,
        out_shape=jax.ShapeDtypeStruct(field.shape, f32),
        in_specs=[smem()] + [hbm()] * 9,
        out_specs=hbm(),
        scratch_shapes=[
            pltpu.VMEM((NCOMP, planes + 4, chunks, ROWS, LANES), f32),
            pltpu.VMEM((NCOMP, planes + 4, chunks, rows, LANES), f32),
            pltpu.VMEM(field.shape, f32),
            pltpu.VMEM((2, NCOMP, planes + 4, 8, LANES), f32),
            pltpu.VMEM(field.shape, f32),
            pltpu.VMEM((2, NCOMP, 2, rows, length), f32),
            pltpu.SemaphoreType.DMA((2 * (planes // 8) + 8,)),
        ],
        compiler_params=pltpu.CompilerParams(vmem_limit_bytes=50 * MIB),
        name="smoothing",
    )(flags, field, *halos)


def ring(count):
    return [(i, (i + 1) % count) for i in range(count)]


def back(pairs):
    return [(b, a) for a, b in pairs]


def rims_of(count):
    first = [(i, i ^ 1) for i in range(count)]
    second = [(i, ((i + 1) ^ 1) - 1 if 0 < i < count - 1 else i) for i in range(count)]
    return first, second


def crossed(circ_pairs, rad_pairs, rads):
    return [(a * rads + c, b * rads + d) for a, b in circ_pairs for c, d in rad_pairs]


def on_device(state, time_source, pseudo_step, offsets, weights):
    cells = state[0]
    source = time_source[0]
    pseudo = pseudo_step[0]
    planes = cells.shape[1]
    circs = lax.axis_size("circ")
    rads = lax.axis_size("rad")
    row = lax.axis_index("row")
    rad = lax.axis_index("rad")
    flags = jnp.stack(
        [
            (rad == 0).astype(jnp.int32),
            (rad == rads - 1).astype(jnp.int32),
            row.astype(jnp.int32),
            (rad % 2).astype(jnp.int32),
            (lax.axis_index("circ") * planes).astype(jnp.int32),
        ]
    )
    up = ring(circs)
    down = back(up)
    pairs_a, pairs_b = rims_of(rads)

    own_a, own_b, circ_low, circ_high, face = edges(flags, cells)
    facing = lax.ppermute(face, "row", [(0, 1), (1, 0)])
    side = math.isqrt(circs)
    near = [[a * side + b for b in range(side)] for a in range(side)]
    far = [[a * side + b for a in range(side)] for b in range(side)]

    def gathered(x, groups):
        return lax.all_to_all(
            jnp.broadcast_to(x[None], (side, *x.shape)),
            "circ",
            0,
            0,
            axis_index_groups=groups,
            tiled=True,
        )

    line = gathered(facing, near)
    halo_circs = (lax.ppermute(circ_high, "circ", up), lax.ppermute(circ_low, "circ", down))
    halo_rads = (lax.ppermute(own_a, "rad", pairs_a), lax.ppermute(own_b, "rad", pairs_b))
    plane = gathered(line, far).reshape(circs, *facing.shape)
    partial = inner_parts(flags, cells, source)

    field, circ_low, circ_high, rim_a, rim_b, low_a, low_b, high_a, high_b = outer_parts(
        flags,
        offsets,
        weights,
        cells,
        partial,
        pseudo,
        halo_circs,
        (own_a, own_b),
        halo_rads,
        plane,
    )
    both = ("circ", "rad")
    halos = (
        lax.ppermute(circ_high, "circ", up),
        lax.ppermute(circ_low, "circ", down),
        lax.ppermute(rim_a, "rad", pairs_a),
        lax.ppermute(rim_b, "rad", pairs_b),
        lax.ppermute(high_a, both, crossed(up, pairs_a, rads)),
        lax.ppermute(high_b, both, crossed(up, pairs_b, rads)),
        lax.ppermute(low_a, both, crossed(down, pairs_a, rads)),
        lax.ppermute(low_b, both, crossed(down, pairs_b, rads)),
    )
    return smoothed(flags, field, halos)[None]


def solution(mesh):
    return jax.shard_map(
        on_device,
        mesh=mesh,
        in_specs=(
            P("row", None, "circ", "rad", None),
            P("row", None, "circ", "rad", None),
            P("row", "circ", "rad", None),
            P("rad"),
            P("rad"),
        ),
        out_specs=P("row", None, "circ", "rad", None),
        check_vma=False,
    )
```

```python
import jax
import jax.numpy as jnp
import numpy as np
from jax import lax
from jax.experimental import pallas as pl
from jax.experimental.pallas import tpu as pltpu
from jax.sharding import PartitionSpec as P

GAMMA = 1.4
GAMMA_LESS = 0.4
SECOND_COEF = 0.5
FOURTH_COEF = 0.03125
RATE = 0.75
GRID_SPEED = 0.5
AXIAL_COUPLING = 0.8
CIRC_COUPLING = 0.6
RADIAL_COUPLING = 0.6

NCOMP = 5
LANES = 128
ROWS = 32
FIRST = 8
MIB = 1 << 20


def axial_table(length):
    modes_index = np.arange(1, length + 1) * 1.0
    angle = np.pi / (length + 1)
    modes = np.sin(np.outer(modes_index, modes_index) * angle)
    eigen = 1.0 + 2.0 * AXIAL_COUPLING - 2.0 * AXIAL_COUPLING * np.cos(modes_index * angle)
    return modes / eigen[None, :] @ modes.T * (2.0 / (length + 1))


def vmem():
    return pl.BlockSpec(memory_space=pltpu.VMEM)


def smem():
    return pl.BlockSpec(memory_space=pltpu.SMEM)


def hbm():
    return pl.BlockSpec(memory_space=pltpu.HBM)


def lane_index(rows):
    return lax.broadcasted_iota(jnp.int32, (rows, LANES), 1)


def begin(a, b, s):
    copy = pltpu.make_async_copy(a, b, s)
    copy.start()
    return copy


def edges_kernel(flags, state, pack_a, pack_b, circ_low, circ_high, face, buf, packs, sems):
    planes = state.shape[1]
    chunks = state.shape[3] // LANES
    group = 8
    groups = planes // group
    loads = []
    for g in range(groups):
        part = pl.ds(g * group, group)
        loads.append(begin(state.at[:, part], buf.at[:, part], sems.at[g]))
    k = groups
    rotor = flags[2]
    odd = flags[3]
    end_cols = pl.ds(pl.multiple_of(jnp.where(rotor == 1, 0, (chunks - 1) * LANES), LANES), LANES)
    lane = lane_index(8)
    sub = lax.broadcasted_iota(jnp.int32, (8, LANES), 0)
    behind_by = jnp.where(rotor == 1, 0, 2)
    for g in range(groups):
        loads[g].wait()

        def body(q, carry):
            for m in range(NCOMP):
                for e in range(2):
                    for c in range(chunks):
                        at = pl.ds(4 * e + c, 1)
                        for i in range(2):
                            cols = pl.ds(c * LANES, LANES)
                            low = buf[m, 2 * q + e, i : i + 1, cols]
                            high = buf[m, 2 * q + e, 14 + i : 15 + i, cols]
                            packs[1 - odd, m, q, i, at, :] = low
                            packs[odd, m, q, i, at, :] = high
            for e in range(2):
                j = 2 * q + e
                for h in range(2):
                    total = jnp.zeros((8, LANES), jnp.float32)
                    for m in range(NCOMP):
                        moved = pltpu.roll(
                            buf[m, j, 8 * h : 8 * h + 8, end_cols], 2 * m, 1, stride=16, stride_axis=0
                        )
                        at = (lane + behind_by - sub * 16 - 2 * m) & (LANES - 1)
                        total = jnp.where(at < 2, moved, total)
                    face[h, pl.ds(j, 1), :] = jnp.sum(total, axis=0, keepdims=True)
            return carry

        lax.fori_loop(g * group // 2, (g + 1) * group // 2, body, 0)
    edge = [
        begin(buf.at[:, 0:2], circ_low, sems.at[k]),
        begin(buf.at[:, planes - 2 : planes], circ_high, sems.at[k + 1]),
        begin(packs.at[0], pack_a, sems.at[k + 2]),
        begin(packs.at[1], pack_b, sems.at[k + 3]),
    ]
    for copy in edge:
        copy.wait()


def edges(flags, cells):
    planes, rows, length = cells.shape[1:]
    chunks = length // LANES
    f32 = jnp.float32
    rad = jax.ShapeDtypeStruct((NCOMP, planes // 2, 2, 8, LANES), f32)
    circ = jax.ShapeDtypeStruct((NCOMP, 2, rows, length), f32)
    face = jax.ShapeDtypeStruct((2, planes, LANES), f32)
    return pl.pallas_call(
        edges_kernel,
        out_shape=(rad, rad, circ, circ, face),
        in_specs=[smem(), hbm()],
        out_specs=(hbm(),) * 4 + (vmem(),),
        scratch_shapes=[
            pltpu.VMEM(cells.shape, f32),
            pltpu.VMEM((2,) + rad.shape, f32),
            pltpu.SemaphoreType.DMA((planes // 8 + 4,)),
        ],
        compiler_params=pltpu.CompilerParams(vmem_limit_bytes=59 * MIB),
        name="state_edges",
    )(flags, cells)


def primitives(cons):
    inverse = 1.0 / cons[0]
    velocity = [cons[m] * inverse for m in (1, 2, 3)]
    kinetic = cons[1] * velocity[0] + cons[2] * velocity[1] + cons[3] * velocity[2]
    pressure = GAMMA_LESS * (cons[4] - 0.5 * kinetic)
    square = GAMMA * pressure * inverse
    sound = square * lax.rsqrt(square)
    return [pressure, sound, *velocity]


def sensor_of(upper, middle, lower):
    outer = upper + lower
    twice = 2.0 * middle
    return jnp.abs(outer - twice) / (outer + twice)


def face_flux(component, cons, pressure, sound, velocity, sensor, grid_speed):
    half = [0.5 * (v - grid_speed) if grid_speed is not None else 0.5 * v for v in velocity]
    speed = jnp.abs(half[0]) + jnp.abs(half[1]) + 0.5 * (sound[0] + sound[1])
    second = SECOND_COEF * jnp.maximum(sensor[0], sensor[1])
    fourth = jnp.maximum(0.0, FOURTH_COEF - second)
    outer = speed * fourth
    inner = speed * (second + 3.0 * fourth)
    near = half[0] + inner
    far = half[1] - inner
    fluxes = []
    for m in range(NCOMP):
        before, left, right, beyond = cons[m]
        flux = right * far + left * near + outer * (beyond - before)
        if m == component:
            flux = flux + 0.5 * (pressure[0] + pressure[1])
        if m == 4:
            flux = flux + 0.5 * (pressure[0] * velocity[0] + pressure[1] * velocity[1])
        fluxes.append(flux)
    return fluxes


def circ_face(cons, at, pressure, sound, velocity, sensor_before, spin):
    sensor = sensor_of(pressure[2], pressure[1], pressure[0])
    flux = face_flux(
        2,
        [[cons(m, d) for d in (-1, 0, 1, 2)] for m in range(NCOMP)],
        pressure[:2],
        sound,
        velocity,
        [sensor_before, sensor],
        spin,
    )
    return flux, sensor


def inner_kernel(flags, state, source, out, cons, prim, src, partial, circ_flux, circ_sensor, sems):
    planes = state.shape[1]
    chunks = state.shape[3] // LANES
    group = 8
    groups = planes // group
    loads = []
    for g in range(groups):
        part = pl.ds(g * group, group)
        loads.append(
            [
                begin(state.at[:, part], cons.at[:, part], sems.at[2 * g]),
                begin(source.at[:, part], src.at[:, part], sems.at[2 * g + 1]),
            ]
        )
    k = 2 * groups
    rotor = flags[2]
    spin = GRID_SPEED * rotor.astype(jnp.float32)
    lane = lane_index(16)

    def cell(m, j, c):
        return cons[m, j, :, c * LANES : (c + 1) * LANES]

    def prepare(j, carry):
        for c in range(chunks):
            fields = primitives([cell(m, j, c) for m in range(NCOMP)])
            for f in range(4):
                prim[f, j, c] = fields[f]
        return carry

    keep_first = lane >= jnp.where(rotor == 1, 2, 0)
    keep_last = lane < jnp.where(rotor == 1, LANES, LANES - 2)

    def behind(parts):
        turned = [pltpu.roll(x, 1, 1) for x in parts]
        before = [parts[0]] + turned[:-1]
        return [jnp.where(lane < 1, before[c], turned[c]) for c in range(chunks)]

    def behind_two(parts, behind_one):
        turned = [pltpu.roll(x, 2, 1) for x in parts]
        before = [behind_one[0]] + turned[:-1]
        return [jnp.where(lane < 2, before[c], turned[c]) for c in range(chunks)]

    def ahead(parts, end):
        turned = [pltpu.roll(x, LANES - 1, 1) for x in parts]
        after = turned[1:] + [end]
        return [jnp.where(lane < LANES - 1, turned[c], after[c]) for c in range(chunks)]

    def axial_part(j):
        state_parts = [[cell(m, j, c) for c in range(chunks)] for m in range(NCOMP)]
        p, sound, speed = [[prim[f, j, c] for c in range(chunks)] for f in (0, 1, 2)]
        p_before = behind(p)
        p_after = ahead(p, p[-1])
        sensor = [sensor_of(p_after[c], p[c], p_before[c]) for c in range(chunks)]
        turned = [pltpu.roll(x, 1, 1) for x in sensor]
        before = [jnp.zeros((16, LANES), jnp.float32)] + turned[:-1]
        sensor_before = [jnp.where(lane < 1, before[c], turned[c]) for c in range(chunks)]
        sound_before = behind(sound)
        speed_before = behind(speed)
        shifted = []
        for x in state_parts:
            one = behind(x)
            shifted.append((behind_two(x, one), one, x, ahead(x, x[-1])))
        flux = [
            face_flux(
                1,
                [[shifted[m][d][c] for d in range(4)] for m in range(NCOMP)],
                [p_before[c], p[c]],
                [sound_before[c], sound[c]],
                [speed_before[c], speed[c]],
                [sensor_before[c], sensor[c]],
                None,
            )
            for c in range(chunks)
        ]
        e = chunks - 1
        end = face_flux(
            1,
            [
                (shifted[m][1][e], state_parts[m][e], state_parts[m][e], state_parts[m][e])
                for m in range(NCOMP)
            ],
            [p[e], p[e]],
            [sound[e], sound[e]],
            [speed[e], speed[e]],
            [sensor[e], sensor[e]],
            None,
        )
        for m in range(NCOMP):
            parts = [flux[c][m] for c in range(chunks)]
            upper = ahead(parts, end[m])
            for c in range(chunks):
                value = upper[c] - parts[c]
                if c == 0:
                    value = jnp.where(keep_first, value, 0.0)
                if c == chunks - 1:
                    value = jnp.where(keep_last, value, 0.0)
                cols = pl.ds(c * LANES, LANES)
                partial[m, j, :, cols] = value + RATE * state_parts[m][c] + src[m, j, :, cols]

    def circ_part(j):
        for c in range(chunks):
            flux, sensor = circ_face(
                lambda m, d: cell(m, j + d, c),
                j,
                [prim[0, j + d, c] for d in (0, 1, 2)],
                [prim[1, j + d, c] for d in (0, 1)],
                [prim[3, j + d, c] for d in (0, 1)],
                circ_sensor[c],
                spin,
            )
            circ_sensor[c] = sensor
            cols = pl.ds(c * LANES, LANES)
            for m in range(NCOMP):
                value = flux[m] - circ_flux[m, c]
                circ_flux[m, c] = flux[m]
                partial[m, j, :, cols] = partial[m, j, :, cols] + jnp.where(j >= 2, value, 0.0)

    def body(j, carry):
        prepare(j + 2, 0)
        axial_part(j)
        circ_part(j)
        return carry

    stores = []

    def store(g):
        stores.append(
            begin(
                partial.at[:, pl.ds(g * group, group)],
                out.at[:, pl.ds(g * group, group)],
                sems.at[k + g],
            )
        )

    for copy in loads[0]:
        copy.wait()
    lax.fori_loop(0, 3, prepare, 0)
    for c in range(chunks):
        circ_sensor[c] = sensor_of(prim[0, 2, c], prim[0, 1, c], prim[0, 0, c])
    axial_part(0)
    done = 1
    for g in range(groups):
        stop = (g + 1) * group - 2
        lax.fori_loop(done, stop, body, 0)
        done = stop
        if g + 1 < groups:
            for copy in loads[g + 1]:
                copy.wait()
        if g > 0:
            store(g - 1)

    def last(j, carry):
        axial_part(j)
        return carry

    lax.fori_loop(planes - 2, planes, last, 0)
    store(groups - 1)
    for copy in stores:
        copy.wait()


def inner_parts(flags, cells, source):
    planes, rows, length = cells.shape[1:]
    chunks = length // LANES
    f32 = jnp.float32
    chunked = (planes, chunks, rows, LANES)
    return pl.pallas_call(
        inner_kernel,
        out_shape=jax.ShapeDtypeStruct(cells.shape, f32),
        in_specs=[smem()] + [hbm()] * 2,
        out_specs=hbm(),
        scratch_shapes=[
            pltpu.VMEM(cells.shape, f32),
            pltpu.VMEM((4,) + chunked, f32),
            pltpu.VMEM(cells.shape, f32),
            pltpu.VMEM(cells.shape, f32),
            pltpu.VMEM((NCOMP, chunks, rows, LANES), f32),
            pltpu.VMEM((chunks, rows, LANES), f32),
            pltpu.SemaphoreType.DMA((planes // 8 * (chunks + 2),)),
        ],
        compiler_params=pltpu.CompilerParams(vmem_limit_bytes=50 * MIB),
        cost_estimate=pl.CostEstimate(
            flops=30_000_000_000, transcendentals=0, bytes_accessed=15_000_000
        ),
        name="inner_parts",
    )(flags, cells, source)


def outer_kernel(
    flags,
    offsets,
    weights,
    state,
    partial_in,
    pseudo,
    circ_low,
    circ_high,
    own_a,
    own_b,
    halo_a,
    halo_b,
    plane,
    table_high,
    table_low,
    out,
    out_circ_low,
    out_circ_high,
    out_a,
    out_b,
    out_low_a,
    out_low_b,
    out_high_a,
    out_high_b,
    cons,
    prim,
    partial,
    step,
    raw_high,
    raw_low,
    result,
    tables,
    own,
    halo,
    top_flux,
    cycle,
    ghosts,
    rad_flux,
    packs,
    beside,
    sems,
):
    planes = state.shape[1]
    chunks = state.shape[3] // LANES
    group = 8
    groups = planes // group
    cells = pl.ds(FIRST, 16)
    rotor = flags[2]
    odd = flags[3]

    loads = []
    for g in range(groups):
        part = pl.ds(g * group, group)
        loads.append(begin(state.at[:, part], result.at[:, part], sems.at[g]))
    k = groups
    rims = [
        begin(own_a, own.at[1 - odd], sems.at[k]),
        begin(own_b, own.at[odd], sems.at[k + 1]),
        begin(halo_a, halo.at[1 - odd], sems.at[k + 2]),
        begin(halo_b, halo.at[odd], sems.at[k + 3]),
    ]
    k += 4
    sides = [
        begin(circ_low, beside.at[0], sems.at[k]),
        begin(circ_high, beside.at[1], sems.at[k + 1]),
    ]
    k += 2
    first_partial = k

    def partial_copy(g):
        part = pl.ds(g * group, group)
        return pltpu.make_async_copy(
            partial_in.at[:, part], partial.at[:, part], sems.at[first_partial + g]
        )

    for g in range(groups):
        partial_copy(g).start()
    k += groups
    late = [
        begin(pseudo, step, sems.at[k]),
        begin(table_high, tables.at[0], sems.at[k + 1]),
        begin(table_low, tables.at[1], sems.at[k + 2]),
    ]
    k += 3
    lane8 = lane_index(8)
    lane = lane_index(16)

    count = plane.shape[0]
    width = plane.shape[2]
    for h in range(2):
        for s in range(count):
            cycle[h, pl.ds(s * width, width), :] = plane[s, h]
        cycle[h, pl.ds(count * width, width), :] = plane[0, h]
        cycle[h, pl.ds((count + 1) * width, 8), :] = plane[1, h, 0:8]
    around = count * width
    starts, leads, trails = [], [], []
    for r in range(16):
        ahead_by = jnp.where(rotor == 1, flags[4] + offsets[r], flags[4] - offsets[r] - 1 + around)
        starts.append(jnp.where(ahead_by >= around, ahead_by - around, ahead_by))
        leads.append(jnp.where(rotor == 1, 1.0 - weights[r], weights[r]))
        trails.append(jnp.where(rotor == 1, weights[r], 1.0 - weights[r]))
    for h in range(2):
        for jt in range(planes // 8):
            total = jnp.zeros((8, LANES), jnp.float32)
            for r in range(8):
                at = starts[8 * h + r] + 8 * jt
                value = (
                    leads[8 * h + r] * cycle[h, pl.ds(at, 8), :]
                    + trails[8 * h + r] * cycle[h, pl.ds(at + 1, 8), :]
                )
                to = (8 - r) % 8
                if to != r:
                    value = pltpu.roll(value, (to - r) % 8 * 16, 1)
                total = jnp.where(((lane8 + 2) & (LANES - 1)) // 16 == to, value, total)
            ghosts[h, pl.ds(8 * jt, 8), :] = total

    for copy in rims:
        copy.wait()

    def mirror(side):
        def body(q, carry):
            for m in range(NCOMP):
                sign = -1.0 if m == 3 else 1.0
                for i in range(2):
                    halo[side, m, q, i] = sign * own[side, m, q, 1 - i]
            return carry

        lax.fori_loop(0, planes // 2, body, 0)

    @pl.when(flags[0] == 1)
    def _():
        mirror(0)

    @pl.when(flags[1] == 1)
    def _():
        mirror(1)

    def rim(q, carry):
        low = [[halo[0, m, q, i] for m in range(NCOMP)] for i in range(2)]
        high = [[own[1, m, q, i] for m in range(NCOMP)] for i in range(2)]
        high += [[halo[1, m, q, i] for m in range(NCOMP)] for i in range(2)]
        low_fields = [primitives(x) for x in low]
        fields = [primitives(x) for x in high]
        p = [x[0] for x in fields]
        flux = face_flux(
            3,
            [[high[d][m] for d in range(4)] for m in range(NCOMP)],
            p[1:3],
            [fields[1][1], fields[2][1]],
            [fields[1][4], fields[2][4]],
            [sensor_of(p[2], p[1], p[0]), sensor_of(p[3], p[2], p[1])],
            None,
        )
        for m in range(NCOMP):
            top_flux[m, q] = flux[m]
        for e in range(2):
            at = 2 * q + e + 2
            for c in range(chunks):
                w = 4 * e + c
                for m in range(NCOMP):
                    for i in range(2):
                        cons[m, at, c, FIRST - 2 + i : FIRST - 1 + i, :] = low[i][m][w : w + 1]
                    cons[m, at, c, FIRST + 16 : FIRST + 17, :] = high[2][m][w : w + 1]
                for i in range(2):
                    prim[0, at, c, FIRST - 2 + i : FIRST - 1 + i, :] = low_fields[i][0][w : w + 1]
                prim[0, at, c, FIRST + 16 : FIRST + 17, :] = fields[2][0][w : w + 1]
                prim[1, at, c, FIRST - 1 : FIRST, :] = low_fields[1][1][w : w + 1]
                prim[2, at, c, FIRST - 1 : FIRST, :] = low_fields[1][4][w : w + 1]
        return carry

    lax.fori_loop(0, planes // 2, rim, 0)

    def place(source_of, at):
        for c in range(chunks):
            values = [source_of(m, pl.ds(c * LANES, LANES)) for m in range(NCOMP)]
            fields = primitives(values)
            for m in range(NCOMP):
                cons[m, at, c, cells, :] = values[m]
            prim[0, at, c, cells, :] = fields[0]
            prim[1, at, c, cells, :] = fields[1]
            prim[2, at, c, cells, :] = fields[4]

    def prepare(j, carry):
        place(lambda m, cols: result[m, j, :, cols], j + 2)
        return carry

    def prepare_side(i, carry):
        for side, first in ((0, 0), (1, planes + 2)):
            place(lambda m, cols: beside[side, m, i, :, cols], first + i)
        return carry

    for g in range(groups):
        loads[g].wait()
        lax.fori_loop(g * group, (g + 1) * group, prepare, 0)
    for copy in sides:
        copy.wait()
    lax.fori_loop(0, 2, prepare_side, 0)
    spin = GRID_SPEED * rotor.astype(jnp.float32)

    def swirl(j, c):
        return cons[2, j, c, cells, :] / cons[0, j, c, cells, :]

    def circ_edges(c, carry):
        cols = pl.ds(pl.multiple_of(c * LANES, LANES), LANES)
        for base in (1, planes - 1):
            before = sensor_of(*[prim[0, base + d, c, cells, :] for d in (1, 0, -1)])
            fluxes = []
            for f in range(3):
                at = base + f
                flux, before = circ_face(
                    lambda m, d: cons[m, at + d, c, cells, :],
                    at,
                    [prim[0, at + d, c, cells, :] for d in (0, 1, 2)],
                    [prim[1, at + d, c, cells, :] for d in (0, 1)],
                    [swirl(at + d, c) for d in (0, 1)],
                    before,
                    spin,
                )
                fluxes.append(flux)
            for f in range(2):
                j = base - 1 + f
                for m in range(NCOMP):
                    partial[m, j, :, cols] = (
                        partial[m, j, :, cols] + fluxes[f + 1][m] - fluxes[f][m]
                    )
        return carry

    ghost_lanes = (lane < 64) == (jnp.where(rotor == 1, 1, 0) == 0)
    end_chunk = jnp.where(rotor == 1, 0, chunks - 1)
    end_cols = pl.ds(pl.multiple_of(end_chunk * LANES, LANES), LANES)
    end_lanes = (lane - jnp.where(rotor == 1, 0, LANES - 2)).astype(jnp.uint32) < 2

    def ends_at(j):
        at = j + 2
        spread = jnp.concatenate(
            [
                pltpu.roll(
                    jnp.broadcast_to(ghosts[h, pl.ds(j, 1), :], (8, LANES)),
                    0,
                    1,
                    stride=16,
                    stride_axis=0,
                )
                for h in range(2)
            ],
            axis=0,
        )
        joined = []
        for m in range(NCOMP):
            moved = pltpu.roll(spread, LANES - 2 * m, 1) if m else spread
            joined.append(jnp.where(ghost_lanes, moved, cons[m, at, end_chunk, cells, :]))
        p, sound, speed = primitives(joined)[:3]
        p_before = pltpu.roll(p, 1, 1)
        sensor = sensor_of(pltpu.roll(p, LANES - 1, 1), p, p_before)
        flux = face_flux(
            1,
            [
                (pltpu.roll(x, 2, 1), pltpu.roll(x, 1, 1), x, pltpu.roll(x, LANES - 1, 1))
                for x in joined
            ],
            [p_before, p],
            [pltpu.roll(sound, 1, 1), sound],
            [pltpu.roll(speed, 1, 1), speed],
            [pltpu.roll(sensor, 1, 1), sensor],
            None,
        )
        for m in range(NCOMP):
            value = pltpu.roll(flux[m], LANES - 1, 1) - flux[m]
            partial[m, j, :, end_cols] = partial[m, j, :, end_cols] + jnp.where(
                end_lanes, value, 0.0
            )

    for g in range(groups):
        partial_copy(g).wait()
    lax.fori_loop(0, chunks, circ_edges, 0)
    for copy in late:
        copy.wait()

    def radial_chunk(j, c, e, q):
        at = j + 2
        p = [prim[0, at, c, pl.ds(FIRST + d, 16), :] for d in (-2, -1, 0, 1)]
        flux = face_flux(
            3,
            [
                [cons[m, at, c, pl.ds(FIRST + d, 16), :] for d in (-2, -1, 0, 1)]
                for m in range(NCOMP)
            ],
            p[1:3],
            [prim[1, at, c, pl.ds(FIRST + d, 16), :] for d in (-1, 0)],
            [prim[2, at, c, pl.ds(FIRST + d, 16), :] for d in (-1, 0)],
            [sensor_of(p[2], p[1], p[0]), sensor_of(p[3], p[2], p[1])],
            None,
        )
        cols = pl.ds(c * LANES, LANES)
        pace = step[j, :, cols]
        for m in range(NCOMP):
            rad_flux[m, e, c, 0:16, :] = flux[m]
            rad_flux[m, e, c, 16:17, :] = top_flux[m, q, 4 * e + c : 4 * e + c + 1, :]
            raw = pace * (partial[m, j, :, cols] + (rad_flux[m, e, c, 1:17, :] - flux[m]))
            high = raw.astype(jnp.bfloat16)
            raw_high[m, j, :, cols] = high
            raw_low[m, j, :, cols] = (raw - high.astype(jnp.float32)).astype(jnp.bfloat16)

    length = chunks * LANES
    quad = 4

    def radial(i):
        for e in range(quad):
            for c in range(chunks):
                radial_chunk(quad * i + e, c, e % 2, (quad // 2) * i + e // 2)

    def product(i):
        part = pl.ds(quad * i, quad)
        high = raw_high[:, part].reshape(NCOMP * quad * 16, length)
        low = raw_low[:, part].reshape(NCOMP * quad * 16, length)
        value = (
            jnp.dot(high, tables[0], preferred_element_type=jnp.float32)
            + jnp.dot(high, tables[1], preferred_element_type=jnp.float32)
            + jnp.dot(low, tables[0], preferred_element_type=jnp.float32)
        )
        result[:, part] = value.reshape(NCOMP, quad, 16, length)

    def both(i, carry):
        product(i - 1)
        radial(i)
        for e in range(quad):
            ends_at(quad * (i + 1) + e)
        return carry

    stores = []
    quads = planes // quad
    per = group // quad
    for e in range(2 * quad):
        ends_at(e)
    radial(0)
    for g in range(groups):
        lax.fori_loop(g * per + 1, min((g + 1) * per + 1, quads - 1), both, 0)
        if g == groups - 1:
            product(quads - 2)
            radial(quads - 1)
            product(quads - 1)
        part = pl.ds(g * group, group)
        stores.append(begin(result.at[:, part], out.at[:, part], sems.at[k]))
        k += 1
    stores += [
        begin(result.at[:, 0:2], out_circ_low, sems.at[k]),
        begin(result.at[:, planes - 2 : planes], out_circ_high, sems.at[k + 1]),
    ]
    k += 2

    def pick(j, carry):
        for m in range(NCOMP):
            for c in range(chunks):
                cols = pl.ds(c * LANES, LANES)
                packs[1 - odd, m, j, pl.ds(2 * c, 2), :] = result[m, j, 0:2, cols]
                packs[odd, m, j, pl.ds(2 * c, 2), :] = result[m, j, 14:16, cols]
        return carry

    lax.fori_loop(0, planes, pick, 0)
    for i, (whole, low, high) in enumerate(
        ((out_a, out_low_a, out_high_a), (out_b, out_low_b, out_high_b))
    ):
        stores.append(begin(packs.at[i], whole, sems.at[k]))
        stores.append(begin(packs.at[i, :, 0:2], low, sems.at[k + 1]))
        stores.append(begin(packs.at[i, :, planes - 2 : planes], high, sems.at[k + 2]))
        k += 3
    for copy in stores:
        copy.wait()


def outer_parts(flags, offsets, weights, cells, partial, pseudo, circs, own, halos, plane):
    planes, rows, length = cells.shape[1:]
    chunks = length // LANES
    table = -axial_table(length).astype(np.float32)
    table_high = table.astype(jnp.bfloat16)
    table_low = (table - table_high.astype(np.float32)).astype(jnp.bfloat16)
    f32 = jnp.float32
    rad = jax.ShapeDtypeStruct((NCOMP, planes, 8, LANES), f32)
    corner = jax.ShapeDtypeStruct((NCOMP, 2, 8, LANES), f32)
    circ = jax.ShapeDtypeStruct((NCOMP, 2, rows, length), f32)
    groups = planes // 8
    buffer = (planes + 4, chunks, ROWS, LANES)
    rims = (2, NCOMP, planes // 2, 2, 8, LANES)
    return pl.pallas_call(
        outer_kernel,
        out_shape=(jax.ShapeDtypeStruct(cells.shape, f32), circ, circ, rad, rad) + (corner,) * 4,
        in_specs=[smem()] * 3 + [hbm()] * 9 + [vmem()] + [hbm()] * 2,
        out_specs=(hbm(),) * 9,
        scratch_shapes=[
            pltpu.VMEM((NCOMP,) + buffer, f32),
            pltpu.VMEM((3,) + buffer, f32),
            pltpu.VMEM(cells.shape, f32),
            pltpu.VMEM(pseudo.shape, f32),
            pltpu.VMEM(cells.shape, jnp.bfloat16),
            pltpu.VMEM(cells.shape, jnp.bfloat16),
            pltpu.VMEM(cells.shape, f32),
            pltpu.VMEM((2, length, length), jnp.bfloat16),
            pltpu.VMEM(rims, f32),
            pltpu.VMEM(rims, f32),
            pltpu.VMEM((NCOMP, planes // 2, 8, LANES), f32),
            pltpu.VMEM((2, plane.shape[0] * planes + planes + 8, LANES), f32),
            pltpu.VMEM((2, planes, LANES), f32),
            pltpu.VMEM((NCOMP, 2, chunks, 24, LANES), f32),
            pltpu.VMEM((2, NCOMP, planes, 8, LANES), f32),
            pltpu.VMEM((2,) + circ.shape, f32),
            pltpu.SemaphoreType.DMA((3 * groups + 18,)),
        ],
        compiler_params=pltpu.CompilerParams(vmem_limit_bytes=58 * MIB),
        name="outer_parts",
    )(
        flags,
        offsets,
        weights,
        cells,
        partial,
        pseudo,
        *circs,
        *own,
        *halos,
        plane,
        jnp.asarray(table_high),
        jnp.asarray(table_low),
    )


def smooth_kernel(
    flags,
    field,
    circ_low,
    circ_high,
    rim_a,
    rim_b,
    low_a,
    low_b,
    high_a,
    high_b,
    out,
    buf,
    mid,
    done,
    rims,
    land,
    beside,
    sems,
):
    planes = field.shape[1]
    chunks = field.shape[3] // LANES
    cells = pl.ds(FIRST, 16)
    group = 8

    odd = flags[3]
    groups = planes // group
    copies = []
    for g in range(groups):
        part = pl.ds(g * group, group)
        copies.append(begin(field.at[:, part], land.at[:, part], sems.at[g]))
    k = groups
    copies += [
        begin(circ_low, beside.at[0], sems.at[k]),
        begin(circ_high, beside.at[1], sems.at[k + 1]),
    ]
    k += 2
    pieces = []
    for side, parts in ((1 - odd, (low_a, rim_a, high_a)), (odd, (low_b, rim_b, high_b))):
        for part, first, count in zip(parts, (0, 2, planes + 2), (2, planes, 2)):
            pieces.append(begin(part, rims.at[side, :, pl.ds(first, count)], sems.at[k]))
            k += 1
    for copy in pieces:
        copy.wait()

    def put(j, carry):
        for m in range(NCOMP):
            for c in range(chunks):
                buf[m, j, c, pl.ds(FIRST - 2, 2), :] = rims[0, m, j, pl.ds(2 * c, 2), :]
                buf[m, j, c, pl.ds(FIRST + 16, 2), :] = rims[1, m, j, pl.ds(2 * c, 2), :]
        return carry

    lax.fori_loop(0, planes + 4, put, 0)

    def place(j, carry):
        for m in range(NCOMP):
            for c in range(chunks):
                buf[m, j + 2, c, cells, :] = land[m, j, :, c * LANES : (c + 1) * LANES]
        return carry

    for copy in copies[groups:]:
        copy.wait()

    def place_side(i, carry):
        for side, first in ((0, 0), (1, planes + 2)):
            for m in range(NCOMP):
                for c in range(chunks):
                    buf[m, first + i, c, cells, :] = beside[side, m, i, :, c * LANES : (c + 1) * LANES]
        return carry

    lax.fori_loop(0, 2, place_side, 0)

    def wall(first, count, zero_row, odd_row, from_row):
        def body(j, carry):
            for m in range(NCOMP):
                for c in range(chunks):
                    buf[m, j, c, pl.ds(zero_row, 1), :] = jnp.zeros((1, LANES), jnp.float32)
                    buf[m, j, c, pl.ds(odd_row, 1), :] = -buf[m, j, c, pl.ds(from_row, 1), :]
            return carry

        lax.fori_loop(first, first + count, body, 0)

    def walls(first, count):
        @pl.when(flags[0] == 1)
        def _():
            wall(first, count, FIRST - 1, FIRST - 2, FIRST)

        @pl.when(flags[1] == 1)
        def _():
            wall(first, count, FIRST + 16, FIRST + 17, FIRST + 15)

    def weights(coupling):
        own = 1.0 / (1.0 + 2.0 * coupling)
        side = coupling / (1.0 + 2.0 * coupling)
        return own * own + 2.0 * side * side, 2.0 * own * side, side * side

    def radial(j, carry):
        w0, w1, w2 = weights(RADIAL_COUPLING)
        for m in range(NCOMP):
            for c in range(chunks):
                x = [buf[m, j, c, pl.ds(FIRST + d, 16), :] for d in (-2, -1, 0, 1, 2)]
                mid[m, j, c] = w0 * x[2] + w1 * (x[1] + x[3]) + w2 * (x[0] + x[4])
        return carry

    def around(j, carry):
        w0, w1, w2 = weights(CIRC_COUPLING)
        for m in range(NCOMP):
            for c in range(chunks):
                x = [mid[m, j + d, c] for d in range(5)]
                done[m, j, :, pl.ds(c * LANES, LANES)] = (
                    w0 * x[2] + w1 * (x[1] + x[3]) + w2 * (x[0] + x[4])
                )
        return carry

    stores = []
    walls(0, 2)
    walls(planes + 2, 2)
    lax.fori_loop(0, 2, radial, 0)
    lax.fori_loop(planes + 2, planes + 4, radial, 0)
    for g in range(groups):
        copies[g].wait()
        lax.fori_loop(g * group, (g + 1) * group, place, 0)
        walls(g * group + 2, group)
        lax.fori_loop(g * group + 2, (g + 1) * group + 2, radial, 0)
        low = max(g * group - 2, 0)
        high = (g + 1) * group - 2 if g < groups - 1 else planes
        lax.fori_loop(low, high, around, 0)
        part = pl.ds(low, high - low)
        stores.append(begin(done.at[:, part], out.at[:, part], sems.at[k]))
        k += 1
    for copy in stores:
        copy.wait()


def smoothed(flags, field, halos):
    planes, rows, length = field.shape[1:]
    chunks = length // LANES
    f32 = jnp.float32
    return pl.pallas_call(
        smooth_kernel,
        out_shape=jax.ShapeDtypeStruct(field.shape, f32),
        in_specs=[smem()] + [hbm()] * 9,
        out_specs=hbm(),
        scratch_shapes=[
            pltpu.VMEM((NCOMP, planes + 4, chunks, ROWS, LANES), f32),
            pltpu.VMEM((NCOMP, planes + 4, chunks, rows, LANES), f32),
            pltpu.VMEM(field.shape, f32),
            pltpu.VMEM((2, NCOMP, planes + 4, 8, LANES), f32),
            pltpu.VMEM(field.shape, f32),
            pltpu.VMEM((2, NCOMP, 2, rows, length), f32),
            pltpu.SemaphoreType.DMA((2 * (planes // 8) + 8,)),
        ],
        compiler_params=pltpu.CompilerParams(vmem_limit_bytes=50 * MIB),
        name="smoothing",
    )(flags, field, *halos)


def ring(count):
    return [(i, (i + 1) % count) for i in range(count)]


def back(pairs):
    return [(b, a) for a, b in pairs]


def rims_of(count):
    first = [(i, i ^ 1) for i in range(count)]
    second = [(i, ((i + 1) ^ 1) - 1 if 0 < i < count - 1 else i) for i in range(count)]
    return first, second


def crossed(circ_pairs, rad_pairs, rads):
    return [(a * rads + c, b * rads + d) for a, b in circ_pairs for c, d in rad_pairs]


def on_device(state, time_source, pseudo_step, offsets, weights):
    cells = state[0]
    source = time_source[0]
    pseudo = pseudo_step[0]
    planes = cells.shape[1]
    circs = lax.axis_size("circ")
    rads = lax.axis_size("rad")
    row = lax.axis_index("row")
    rad = lax.axis_index("rad")
    flags = jnp.stack(
        [
            (rad == 0).astype(jnp.int32),
            (rad == rads - 1).astype(jnp.int32),
            row.astype(jnp.int32),
            (rad % 2).astype(jnp.int32),
            (lax.axis_index("circ") * planes).astype(jnp.int32),
        ]
    )
    up = ring(circs)
    down = back(up)
    pairs_a, pairs_b = rims_of(rads)

    own_a, own_b, circ_low, circ_high, face = edges(flags, cells)
    facing = lax.ppermute(face, "row", [(0, 1), (1, 0)])
    halo_circs = (lax.ppermute(circ_high, "circ", up), lax.ppermute(circ_low, "circ", down))
    halo_rads = (lax.ppermute(own_a, "rad", pairs_a), lax.ppermute(own_b, "rad", pairs_b))
    plane = lax.all_to_all(
        jnp.broadcast_to(facing[None], (circs, *facing.shape)), "circ", 0, 0, tiled=True
    )
    partial = inner_parts(flags, cells, source)

    field, circ_low, circ_high, rim_a, rim_b, low_a, low_b, high_a, high_b = outer_parts(
        flags,
        offsets,
        weights,
        cells,
        partial,
        pseudo,
        halo_circs,
        (own_a, own_b),
        halo_rads,
        plane,
    )
    both = ("circ", "rad")
    halos = (
        lax.ppermute(circ_high, "circ", up),
        lax.ppermute(circ_low, "circ", down),
        lax.ppermute(rim_a, "rad", pairs_a),
        lax.ppermute(rim_b, "rad", pairs_b),
        lax.ppermute(high_a, both, crossed(up, pairs_a, rads)),
        lax.ppermute(high_b, both, crossed(up, pairs_b, rads)),
        lax.ppermute(low_a, both, crossed(down, pairs_a, rads)),
        lax.ppermute(low_b, both, crossed(down, pairs_b, rads)),
    )
    return smoothed(flags, field, halos)[None]


def solution(mesh):
    return jax.shard_map(
        on_device,
        mesh=mesh,
        in_specs=(
            P("row", None, "circ", "rad", None),
            P("row", None, "circ", "rad", None),
            P("row", "circ", "rad", None),
            P("rad"),
            P("rad"),
        ),
        out_specs=P("row", None, "circ", "rad", None),
        check_vma=False,
    )
```

```python
import jax
import jax.numpy as jnp
import numpy as np
from jax import lax
from jax.experimental import pallas as pl
from jax.experimental.pallas import tpu as pltpu
from jax.sharding import PartitionSpec as P

GAMMA = 1.4
GAMMA_LESS = 0.4
SECOND_COEF = 0.5
FOURTH_COEF = 0.03125
RATE = 0.75
GRID_SPEED = 0.5
AXIAL_COUPLING = 0.8
CIRC_COUPLING = 0.6
RADIAL_COUPLING = 0.6

NCOMP = 5
LANES = 128
ROWS = 32
FIRST = 8
MIB = 1 << 20


def axial_table(length):
    modes_index = np.arange(1, length + 1) * 1.0
    angle = np.pi / (length + 1)
    modes = np.sin(np.outer(modes_index, modes_index) * angle)
    eigen = 1.0 + 2.0 * AXIAL_COUPLING - 2.0 * AXIAL_COUPLING * np.cos(modes_index * angle)
    return modes / eigen[None, :] @ modes.T * (2.0 / (length + 1))


def vmem():
    return pl.BlockSpec(memory_space=pltpu.VMEM)


def smem():
    return pl.BlockSpec(memory_space=pltpu.SMEM)


def hbm():
    return pl.BlockSpec(memory_space=pltpu.HBM)


def lane_index(rows):
    return lax.broadcasted_iota(jnp.int32, (rows, LANES), 1)


def begin(a, b, s):
    copy = pltpu.make_async_copy(a, b, s)
    copy.start()
    return copy


def edges_kernel(flags, state, pack_a, pack_b, circ_low, circ_high, face, buf, packs, sems):
    planes = state.shape[1]
    chunks = state.shape[3] // LANES
    group = 8
    groups = planes // group
    loads = []
    for g in range(groups):
        part = pl.ds(g * group, group)
        loads.append(begin(state.at[:, part], buf.at[:, part], sems.at[g]))
    k = groups
    rotor = flags[2]
    odd = flags[3]
    end_cols = pl.ds(pl.multiple_of(jnp.where(rotor == 1, 0, (chunks - 1) * LANES), LANES), LANES)
    lane = lane_index(8)
    sub = lax.broadcasted_iota(jnp.int32, (8, LANES), 0)
    behind_by = jnp.where(rotor == 1, 0, 2)
    for g in range(groups):
        loads[g].wait()

        def body(q, carry):
            for m in range(NCOMP):
                for e in range(2):
                    for c in range(chunks):
                        at = pl.ds(4 * e + c, 1)
                        for i in range(2):
                            cols = pl.ds(c * LANES, LANES)
                            low = buf[m, 2 * q + e, i : i + 1, cols]
                            high = buf[m, 2 * q + e, 14 + i : 15 + i, cols]
                            packs[1 - odd, m, q, i, at, :] = low
                            packs[odd, m, q, i, at, :] = high
            for e in range(2):
                j = 2 * q + e
                for h in range(2):
                    total = jnp.zeros((8, LANES), jnp.float32)
                    for m in range(NCOMP):
                        moved = pltpu.roll(
                            buf[m, j, 8 * h : 8 * h + 8, end_cols], 2 * m, 1, stride=16, stride_axis=0
                        )
                        at = (lane + behind_by - sub * 16 - 2 * m) & (LANES - 1)
                        total = jnp.where(at < 2, moved, total)
                    face[h, pl.ds(j, 1), :] = jnp.sum(total, axis=0, keepdims=True)
            return carry

        lax.fori_loop(g * group // 2, (g + 1) * group // 2, body, 0)
    edge = [
        begin(buf.at[:, 0:2], circ_low, sems.at[k]),
        begin(buf.at[:, planes - 2 : planes], circ_high, sems.at[k + 1]),
        begin(packs.at[0], pack_a, sems.at[k + 2]),
        begin(packs.at[1], pack_b, sems.at[k + 3]),
    ]
    for copy in edge:
        copy.wait()


def edges(flags, cells):
    planes, rows, length = cells.shape[1:]
    chunks = length // LANES
    f32 = jnp.float32
    rad = jax.ShapeDtypeStruct((NCOMP, planes // 2, 2, 8, LANES), f32)
    circ = jax.ShapeDtypeStruct((NCOMP, 2, rows, length), f32)
    face = jax.ShapeDtypeStruct((2, planes, LANES), f32)
    return pl.pallas_call(
        edges_kernel,
        out_shape=(rad, rad, circ, circ, face),
        in_specs=[smem(), hbm()],
        out_specs=(hbm(),) * 4 + (vmem(),),
        scratch_shapes=[
            pltpu.VMEM(cells.shape, f32),
            pltpu.VMEM((2,) + rad.shape, f32),
            pltpu.SemaphoreType.DMA((planes // 8 + 4,)),
        ],
        compiler_params=pltpu.CompilerParams(vmem_limit_bytes=59 * MIB),
        name="state_edges",
    )(flags, cells)


def primitives(cons):
    inverse = 1.0 / cons[0]
    velocity = [cons[m] * inverse for m in (1, 2, 3)]
    kinetic = cons[1] * velocity[0] + cons[2] * velocity[1] + cons[3] * velocity[2]
    pressure = GAMMA_LESS * (cons[4] - 0.5 * kinetic)
    square = GAMMA * pressure * inverse
    sound = square * lax.rsqrt(square)
    return [pressure, sound, *velocity]


def sensor_of(upper, middle, lower):
    outer = upper + lower
    twice = 2.0 * middle
    return jnp.abs(outer - twice) / (outer + twice)


def face_flux(component, cons, pressure, sound, velocity, sensor, grid_speed):
    half = [0.5 * (v - grid_speed) if grid_speed is not None else 0.5 * v for v in velocity]
    speed = jnp.abs(half[0]) + jnp.abs(half[1]) + 0.5 * (sound[0] + sound[1])
    second = SECOND_COEF * jnp.maximum(sensor[0], sensor[1])
    fourth = jnp.maximum(0.0, FOURTH_COEF - second)
    outer = speed * fourth
    inner = speed * (second + 3.0 * fourth)
    near = half[0] + inner
    far = half[1] - inner
    fluxes = []
    for m in range(NCOMP):
        before, left, right, beyond = cons[m]
        flux = right * far + left * near + outer * (beyond - before)
        if m == component:
            flux = flux + 0.5 * (pressure[0] + pressure[1])
        if m == 4:
            flux = flux + 0.5 * (pressure[0] * velocity[0] + pressure[1] * velocity[1])
        fluxes.append(flux)
    return fluxes


def circ_face(cons, at, pressure, sound, velocity, sensor_before, spin):
    sensor = sensor_of(pressure[2], pressure[1], pressure[0])
    flux = face_flux(
        2,
        [[cons(m, d) for d in (-1, 0, 1, 2)] for m in range(NCOMP)],
        pressure[:2],
        sound,
        velocity,
        [sensor_before, sensor],
        spin,
    )
    return flux, sensor


def inner_kernel(flags, state, source, out, cons, prim, src, partial, circ_flux, circ_sensor, sems):
    planes = state.shape[1]
    chunks = state.shape[3] // LANES
    group = 8
    groups = planes // group
    loads = []
    for g in range(groups):
        part = pl.ds(g * group, group)
        loads.append(
            [
                begin(state.at[:, part], cons.at[:, part], sems.at[2 * g]),
                begin(source.at[:, part], src.at[:, part], sems.at[2 * g + 1]),
            ]
        )
    k = 2 * groups
    rotor = flags[2]
    spin = GRID_SPEED * rotor.astype(jnp.float32)
    lane = lane_index(16)

    def cell(m, j, c):
        return cons[m, j, :, c * LANES : (c + 1) * LANES]

    def prepare(j, carry):
        for c in range(chunks):
            fields = primitives([cell(m, j, c) for m in range(NCOMP)])
            for f in range(4):
                prim[f, j, c] = fields[f]
        return carry

    keep_first = lane >= jnp.where(rotor == 1, 2, 0)
    keep_last = lane < jnp.where(rotor == 1, LANES, LANES - 2)

    def behind(parts):
        turned = [pltpu.roll(x, 1, 1) for x in parts]
        before = [parts[0]] + turned[:-1]
        return [jnp.where(lane < 1, before[c], turned[c]) for c in range(chunks)]

    def behind_two(parts, behind_one):
        turned = [pltpu.roll(x, 2, 1) for x in parts]
        before = [behind_one[0]] + turned[:-1]
        return [jnp.where(lane < 2, before[c], turned[c]) for c in range(chunks)]

    def ahead(parts, end):
        turned = [pltpu.roll(x, LANES - 1, 1) for x in parts]
        after = turned[1:] + [end]
        return [jnp.where(lane < LANES - 1, turned[c], after[c]) for c in range(chunks)]

    def axial_part(j):
        state_parts = [[cell(m, j, c) for c in range(chunks)] for m in range(NCOMP)]
        p, sound, speed = [[prim[f, j, c] for c in range(chunks)] for f in (0, 1, 2)]
        p_before = behind(p)
        p_after = ahead(p, p[-1])
        sensor = [sensor_of(p_after[c], p[c], p_before[c]) for c in range(chunks)]
        turned = [pltpu.roll(x, 1, 1) for x in sensor]
        before = [jnp.zeros((16, LANES), jnp.float32)] + turned[:-1]
        sensor_before = [jnp.where(lane < 1, before[c], turned[c]) for c in range(chunks)]
        sound_before = behind(sound)
        speed_before = behind(speed)
        shifted = []
        for x in state_parts:
            one = behind(x)
            shifted.append((behind_two(x, one), one, x, ahead(x, x[-1])))
        flux = [
            face_flux(
                1,
                [[shifted[m][d][c] for d in range(4)] for m in range(NCOMP)],
                [p_before[c], p[c]],
                [sound_before[c], sound[c]],
                [speed_before[c], speed[c]],
                [sensor_before[c], sensor[c]],
                None,
            )
            for c in range(chunks)
        ]
        e = chunks - 1
        end = face_flux(
            1,
            [
                (shifted[m][1][e], state_parts[m][e], state_parts[m][e], state_parts[m][e])
                for m in range(NCOMP)
            ],
            [p[e], p[e]],
            [sound[e], sound[e]],
            [speed[e], speed[e]],
            [sensor[e], sensor[e]],
            None,
        )
        for m in range(NCOMP):
            parts = [flux[c][m] for c in range(chunks)]
            upper = ahead(parts, end[m])
            for c in range(chunks):
                value = upper[c] - parts[c]
                if c == 0:
                    value = jnp.where(keep_first, value, 0.0)
                if c == chunks - 1:
                    value = jnp.where(keep_last, value, 0.0)
                cols = pl.ds(c * LANES, LANES)
                partial[m, j, :, cols] = value + RATE * state_parts[m][c] + src[m, j, :, cols]

    def circ_part(j):
        for c in range(chunks):
            flux, sensor = circ_face(
                lambda m, d: cell(m, j + d, c),
                j,
                [prim[0, j + d, c] for d in (0, 1, 2)],
                [prim[1, j + d, c] for d in (0, 1)],
                [prim[3, j + d, c] for d in (0, 1)],
                circ_sensor[c],
                spin,
            )
            circ_sensor[c] = sensor
            cols = pl.ds(c * LANES, LANES)
            for m in range(NCOMP):
                value = flux[m] - circ_flux[m, c]
                circ_flux[m, c] = flux[m]
                partial[m, j, :, cols] = partial[m, j, :, cols] + jnp.where(j >= 2, value, 0.0)

    def body(j, carry):
        prepare(j + 2, 0)
        axial_part(j)
        circ_part(j)
        return carry

    stores = []

    def store(g):
        stores.append(
            begin(
                partial.at[:, pl.ds(g * group, group)],
                out.at[:, pl.ds(g * group, group)],
                sems.at[k + g],
            )
        )

    for copy in loads[0]:
        copy.wait()
    lax.fori_loop(0, 3, prepare, 0)
    for c in range(chunks):
        circ_sensor[c] = sensor_of(prim[0, 2, c], prim[0, 1, c], prim[0, 0, c])
    axial_part(0)
    done = 1
    for g in range(groups):
        stop = (g + 1) * group - 2
        lax.fori_loop(done, stop, body, 0)
        done = stop
        if g + 1 < groups:
            for copy in loads[g + 1]:
                copy.wait()
        if g > 0:
            store(g - 1)

    def last(j, carry):
        axial_part(j)
        return carry

    lax.fori_loop(planes - 2, planes, last, 0)
    store(groups - 1)
    for copy in stores:
        copy.wait()


def inner_parts(flags, cells, source):
    planes, rows, length = cells.shape[1:]
    chunks = length // LANES
    f32 = jnp.float32
    chunked = (planes, chunks, rows, LANES)
    return pl.pallas_call(
        inner_kernel,
        out_shape=jax.ShapeDtypeStruct(cells.shape, f32),
        in_specs=[smem()] + [hbm()] * 2,
        out_specs=hbm(),
        scratch_shapes=[
            pltpu.VMEM(cells.shape, f32),
            pltpu.VMEM((4,) + chunked, f32),
            pltpu.VMEM(cells.shape, f32),
            pltpu.VMEM(cells.shape, f32),
            pltpu.VMEM((NCOMP, chunks, rows, LANES), f32),
            pltpu.VMEM((chunks, rows, LANES), f32),
            pltpu.SemaphoreType.DMA((planes // 8 * (chunks + 2),)),
        ],
        compiler_params=pltpu.CompilerParams(vmem_limit_bytes=50 * MIB),
        cost_estimate=pl.CostEstimate(
            flops=30_000_000_000, transcendentals=0, bytes_accessed=15_000_000
        ),
        name="inner_parts",
    )(flags, cells, source)


def outer_kernel(
    flags,
    offsets,
    weights,
    state,
    partial_in,
    pseudo,
    circ_low,
    circ_high,
    own_a,
    own_b,
    halo_a,
    halo_b,
    plane,
    table_high,
    table_low,
    out,
    out_circ_low,
    out_circ_high,
    out_a,
    out_b,
    out_low_a,
    out_low_b,
    out_high_a,
    out_high_b,
    cons,
    prim,
    partial,
    step,
    raw_high,
    raw_low,
    result,
    tables,
    own,
    halo,
    top_flux,
    cycle,
    ghosts,
    rad_flux,
    packs,
    beside,
    sems,
):
    planes = state.shape[1]
    chunks = state.shape[3] // LANES
    group = 8
    groups = planes // group
    cells = pl.ds(FIRST, 16)
    rotor = flags[2]
    odd = flags[3]

    k = groups
    rims = [
        begin(own_a, own.at[1 - odd], sems.at[k]),
        begin(own_b, own.at[odd], sems.at[k + 1]),
        begin(halo_a, halo.at[1 - odd], sems.at[k + 2]),
        begin(halo_b, halo.at[odd], sems.at[k + 3]),
    ]
    k += 4
    loads = []
    for g in range(groups):
        part = pl.ds(g * group, group)
        loads.append(begin(state.at[:, part], result.at[:, part], sems.at[g]))
    sides = [
        begin(circ_low, beside.at[0], sems.at[k]),
        begin(circ_high, beside.at[1], sems.at[k + 1]),
    ]
    k += 2
    first_partial = k

    def partial_copy(g):
        part = pl.ds(g * group, group)
        return pltpu.make_async_copy(
            partial_in.at[:, part], partial.at[:, part], sems.at[first_partial + g]
        )

    for g in range(groups):
        partial_copy(g).start()
    k += groups
    late = [
        begin(pseudo, step, sems.at[k]),
        begin(table_high, tables.at[0], sems.at[k + 1]),
        begin(table_low, tables.at[1], sems.at[k + 2]),
    ]
    k += 3
    lane8 = lane_index(8)
    lane = lane_index(16)

    count = plane.shape[0]
    width = plane.shape[2]
    for h in range(2):
        for s in range(count):
            cycle[h, pl.ds(s * width, width), :] = plane[s, h]
        cycle[h, pl.ds(count * width, width), :] = plane[0, h]
        cycle[h, pl.ds((count + 1) * width, 8), :] = plane[1, h, 0:8]
    around = count * width
    starts, leads, trails = [], [], []
    for r in range(16):
        ahead_by = jnp.where(rotor == 1, flags[4] + offsets[r], flags[4] - offsets[r] - 1 + around)
        starts.append(jnp.where(ahead_by >= around, ahead_by - around, ahead_by))
        leads.append(jnp.where(rotor == 1, 1.0 - weights[r], weights[r]))
        trails.append(jnp.where(rotor == 1, weights[r], 1.0 - weights[r]))
    for h in range(2):
        for jt in range(planes // 8):
            total = jnp.zeros((8, LANES), jnp.float32)
            for r in range(8):
                at = starts[8 * h + r] + 8 * jt
                value = (
                    leads[8 * h + r] * cycle[h, pl.ds(at, 8), :]
                    + trails[8 * h + r] * cycle[h, pl.ds(at + 1, 8), :]
                )
                to = (8 - r) % 8
                if to != r:
                    value = pltpu.roll(value, (to - r) % 8 * 16, 1)
                total = jnp.where(((lane8 + 2) & (LANES - 1)) // 16 == to, value, total)
            ghosts[h, pl.ds(8 * jt, 8), :] = total

    for copy in rims:
        copy.wait()

    def mirror(side):
        def body(q, carry):
            for m in range(NCOMP):
                sign = -1.0 if m == 3 else 1.0
                for i in range(2):
                    halo[side, m, q, i] = sign * own[side, m, q, 1 - i]
            return carry

        lax.fori_loop(0, planes // 2, body, 0)

    @pl.when(flags[0] == 1)
    def _():
        mirror(0)

    @pl.when(flags[1] == 1)
    def _():
        mirror(1)

    def rim(q, carry):
        low = [[halo[0, m, q, i] for m in range(NCOMP)] for i in range(2)]
        high = [[own[1, m, q, i] for m in range(NCOMP)] for i in range(2)]
        high += [[halo[1, m, q, i] for m in range(NCOMP)] for i in range(2)]
        low_fields = [primitives(x) for x in low]
        fields = [primitives(x) for x in high]
        p = [x[0] for x in fields]
        flux = face_flux(
            3,
            [[high[d][m] for d in range(4)] for m in range(NCOMP)],
            p[1:3],
            [fields[1][1], fields[2][1]],
            [fields[1][4], fields[2][4]],
            [sensor_of(p[2], p[1], p[0]), sensor_of(p[3], p[2], p[1])],
            None,
        )
        for m in range(NCOMP):
            top_flux[m, q] = flux[m]
        for e in range(2):
            at = 2 * q + e + 2
            for c in range(chunks):
                w = 4 * e + c
                for m in range(NCOMP):
                    for i in range(2):
                        cons[m, at, c, FIRST - 2 + i : FIRST - 1 + i, :] = low[i][m][w : w + 1]
                    cons[m, at, c, FIRST + 16 : FIRST + 17, :] = high[2][m][w : w + 1]
                for i in range(2):
                    prim[0, at, c, FIRST - 2 + i : FIRST - 1 + i, :] = low_fields[i][0][w : w + 1]
                prim[0, at, c, FIRST + 16 : FIRST + 17, :] = fields[2][0][w : w + 1]
                prim[1, at, c, FIRST - 1 : FIRST, :] = low_fields[1][1][w : w + 1]
                prim[2, at, c, FIRST - 1 : FIRST, :] = low_fields[1][4][w : w + 1]
        return carry

    lax.fori_loop(0, planes // 2, rim, 0)

    def place(source_of, at):
        for c in range(chunks):
            values = [source_of(m, pl.ds(c * LANES, LANES)) for m in range(NCOMP)]
            fields = primitives(values)
            for m in range(NCOMP):
                cons[m, at, c, cells, :] = values[m]
            prim[0, at, c, cells, :] = fields[0]
            prim[1, at, c, cells, :] = fields[1]
            prim[2, at, c, cells, :] = fields[4]

    def prepare(j, carry):
        place(lambda m, cols: result[m, j, :, cols], j + 2)
        return carry

    def prepare_side(i, carry):
        for side, first in ((0, 0), (1, planes + 2)):
            place(lambda m, cols: beside[side, m, i, :, cols], first + i)
        return carry

    for g in range(groups):
        loads[g].wait()
        lax.fori_loop(g * group, (g + 1) * group, prepare, 0)
    for copy in sides:
        copy.wait()
    lax.fori_loop(0, 2, prepare_side, 0)
    spin = GRID_SPEED * rotor.astype(jnp.float32)

    def swirl(j, c):
        return cons[2, j, c, cells, :] / cons[0, j, c, cells, :]

    def circ_edges(c, carry):
        cols = pl.ds(pl.multiple_of(c * LANES, LANES), LANES)
        for base in (1, planes - 1):
            before = sensor_of(*[prim[0, base + d, c, cells, :] for d in (1, 0, -1)])
            fluxes = []
            for f in range(3):
                at = base + f
                flux, before = circ_face(
                    lambda m, d: cons[m, at + d, c, cells, :],
                    at,
                    [prim[0, at + d, c, cells, :] for d in (0, 1, 2)],
                    [prim[1, at + d, c, cells, :] for d in (0, 1)],
                    [swirl(at + d, c) for d in (0, 1)],
                    before,
                    spin,
                )
                fluxes.append(flux)
            for f in range(2):
                j = base - 1 + f
                for m in range(NCOMP):
                    partial[m, j, :, cols] = (
                        partial[m, j, :, cols] + fluxes[f + 1][m] - fluxes[f][m]
                    )
        return carry

    ghost_lanes = (lane < 64) == (jnp.where(rotor == 1, 1, 0) == 0)
    end_chunk = jnp.where(rotor == 1, 0, chunks - 1)
    end_cols = pl.ds(pl.multiple_of(end_chunk * LANES, LANES), LANES)
    end_lanes = (lane - jnp.where(rotor == 1, 0, LANES - 2)).astype(jnp.uint32) < 2

    def ends_at(j):
        at = j + 2
        spread = jnp.concatenate(
            [
                pltpu.roll(
                    jnp.broadcast_to(ghosts[h, pl.ds(j, 1), :], (8, LANES)),
                    0,
                    1,
                    stride=16,
                    stride_axis=0,
                )
                for h in range(2)
            ],
            axis=0,
        )
        joined = []
        for m in range(NCOMP):
            moved = pltpu.roll(spread, LANES - 2 * m, 1) if m else spread
            joined.append(jnp.where(ghost_lanes, moved, cons[m, at, end_chunk, cells, :]))
        p, sound, speed = primitives(joined)[:3]
        p_before = pltpu.roll(p, 1, 1)
        sensor = sensor_of(pltpu.roll(p, LANES - 1, 1), p, p_before)
        flux = face_flux(
            1,
            [
                (pltpu.roll(x, 2, 1), pltpu.roll(x, 1, 1), x, pltpu.roll(x, LANES - 1, 1))
                for x in joined
            ],
            [p_before, p],
            [pltpu.roll(sound, 1, 1), sound],
            [pltpu.roll(speed, 1, 1), speed],
            [pltpu.roll(sensor, 1, 1), sensor],
            None,
        )
        for m in range(NCOMP):
            value = pltpu.roll(flux[m], LANES - 1, 1) - flux[m]
            partial[m, j, :, end_cols] = partial[m, j, :, end_cols] + jnp.where(
                end_lanes, value, 0.0
            )

    for g in range(groups):
        partial_copy(g).wait()
    lax.fori_loop(0, chunks, circ_edges, 0)
    for copy in late:
        copy.wait()

    def radial_chunk(j, c, e, q):
        at = j + 2
        p = [prim[0, at, c, pl.ds(FIRST + d, 16), :] for d in (-2, -1, 0, 1)]
        flux = face_flux(
            3,
            [
                [cons[m, at, c, pl.ds(FIRST + d, 16), :] for d in (-2, -1, 0, 1)]
                for m in range(NCOMP)
            ],
            p[1:3],
            [prim[1, at, c, pl.ds(FIRST + d, 16), :] for d in (-1, 0)],
            [prim[2, at, c, pl.ds(FIRST + d, 16), :] for d in (-1, 0)],
            [sensor_of(p[2], p[1], p[0]), sensor_of(p[3], p[2], p[1])],
            None,
        )
        cols = pl.ds(c * LANES, LANES)
        pace = step[j, :, cols]
        for m in range(NCOMP):
            rad_flux[m, e, c, 0:16, :] = flux[m]
            rad_flux[m, e, c, 16:17, :] = top_flux[m, q, 4 * e + c : 4 * e + c + 1, :]
            raw = pace * (partial[m, j, :, cols] + (rad_flux[m, e, c, 1:17, :] - flux[m]))
            high = raw.astype(jnp.bfloat16)
            raw_high[m, j, :, cols] = high
            raw_low[m, j, :, cols] = (raw - high.astype(jnp.float32)).astype(jnp.bfloat16)

    length = chunks * LANES
    quad = 4

    def radial(i):
        for e in range(quad):
            for c in range(chunks):
                radial_chunk(quad * i + e, c, e % 2, (quad // 2) * i + e // 2)

    def product(i):
        part = pl.ds(quad * i, quad)
        high = raw_high[:, part].reshape(NCOMP * quad * 16, length)
        low = raw_low[:, part].reshape(NCOMP * quad * 16, length)
        value = (
            jnp.dot(high, tables[0], preferred_element_type=jnp.float32)
            + jnp.dot(high, tables[1], preferred_element_type=jnp.float32)
            + jnp.dot(low, tables[0], preferred_element_type=jnp.float32)
        )
        result[:, part] = value.reshape(NCOMP, quad, 16, length)

    def both(i, carry):
        product(i - 1)
        radial(i)
        for e in range(quad):
            ends_at(quad * (i + 1) + e)
        return carry

    stores = []
    quads = planes // quad
    per = group // quad
    for e in range(2 * quad):
        ends_at(e)
    radial(0)
    for g in range(groups):
        lax.fori_loop(g * per + 1, min((g + 1) * per + 1, quads - 1), both, 0)
        if g == groups - 1:
            product(quads - 2)
            radial(quads - 1)
            product(quads - 1)
        part = pl.ds(g * group, group)
        stores.append(begin(result.at[:, part], out.at[:, part], sems.at[k]))
        k += 1
    stores += [
        begin(result.at[:, 0:2], out_circ_low, sems.at[k]),
        begin(result.at[:, planes - 2 : planes], out_circ_high, sems.at[k + 1]),
    ]
    k += 2

    def pick(j, carry):
        for m in range(NCOMP):
            for c in range(chunks):
                cols = pl.ds(c * LANES, LANES)
                packs[1 - odd, m, j, pl.ds(2 * c, 2), :] = result[m, j, 0:2, cols]
                packs[odd, m, j, pl.ds(2 * c, 2), :] = result[m, j, 14:16, cols]
        return carry

    lax.fori_loop(0, planes, pick, 0)
    for i, (whole, low, high) in enumerate(
        ((out_a, out_low_a, out_high_a), (out_b, out_low_b, out_high_b))
    ):
        stores.append(begin(packs.at[i], whole, sems.at[k]))
        stores.append(begin(packs.at[i, :, 0:2], low, sems.at[k + 1]))
        stores.append(begin(packs.at[i, :, planes - 2 : planes], high, sems.at[k + 2]))
        k += 3
    for copy in stores:
        copy.wait()


def outer_parts(flags, offsets, weights, cells, partial, pseudo, circs, own, halos, plane):
    planes, rows, length = cells.shape[1:]
    chunks = length // LANES
    table = -axial_table(length).astype(np.float32)
    table_high = table.astype(jnp.bfloat16)
    table_low = (table - table_high.astype(np.float32)).astype(jnp.bfloat16)
    f32 = jnp.float32
    rad = jax.ShapeDtypeStruct((NCOMP, planes, 8, LANES), f32)
    corner = jax.ShapeDtypeStruct((NCOMP, 2, 8, LANES), f32)
    circ = jax.ShapeDtypeStruct((NCOMP, 2, rows, length), f32)
    groups = planes // 8
    buffer = (planes + 4, chunks, ROWS, LANES)
    rims = (2, NCOMP, planes // 2, 2, 8, LANES)
    return pl.pallas_call(
        outer_kernel,
        out_shape=(jax.ShapeDtypeStruct(cells.shape, f32), circ, circ, rad, rad) + (corner,) * 4,
        in_specs=[smem()] * 3 + [hbm()] * 9 + [vmem()] + [hbm()] * 2,
        out_specs=(hbm(),) * 9,
        scratch_shapes=[
            pltpu.VMEM((NCOMP,) + buffer, f32),
            pltpu.VMEM((3,) + buffer, f32),
            pltpu.VMEM(cells.shape, f32),
            pltpu.VMEM(pseudo.shape, f32),
            pltpu.VMEM(cells.shape, jnp.bfloat16),
            pltpu.VMEM(cells.shape, jnp.bfloat16),
            pltpu.VMEM(cells.shape, f32),
            pltpu.VMEM((2, length, length), jnp.bfloat16),
            pltpu.VMEM(rims, f32),
            pltpu.VMEM(rims, f32),
            pltpu.VMEM((NCOMP, planes // 2, 8, LANES), f32),
            pltpu.VMEM((2, plane.shape[0] * planes + planes + 8, LANES), f32),
            pltpu.VMEM((2, planes, LANES), f32),
            pltpu.VMEM((NCOMP, 2, chunks, 24, LANES), f32),
            pltpu.VMEM((2, NCOMP, planes, 8, LANES), f32),
            pltpu.VMEM((2,) + circ.shape, f32),
            pltpu.SemaphoreType.DMA((3 * groups + 18,)),
        ],
        compiler_params=pltpu.CompilerParams(vmem_limit_bytes=58 * MIB),
        name="outer_parts",
    )(
        flags,
        offsets,
        weights,
        cells,
        partial,
        pseudo,
        *circs,
        *own,
        *halos,
        plane,
        jnp.asarray(table_high),
        jnp.asarray(table_low),
    )


def smooth_kernel(
    flags,
    field,
    circ_low,
    circ_high,
    rim_a,
    rim_b,
    low_a,
    low_b,
    high_a,
    high_b,
    out,
    buf,
    mid,
    done,
    rims,
    land,
    beside,
    sems,
):
    planes = field.shape[1]
    chunks = field.shape[3] // LANES
    cells = pl.ds(FIRST, 16)
    group = 8

    odd = flags[3]
    groups = planes // group
    copies = []
    for g in range(groups):
        part = pl.ds(g * group, group)
        copies.append(begin(field.at[:, part], land.at[:, part], sems.at[g]))
    k = groups
    pieces = []
    for side, parts in ((1 - odd, (low_a, rim_a, high_a)), (odd, (low_b, rim_b, high_b))):
        for part, first, count in zip(parts, (0, 2, planes + 2), (2, planes, 2)):
            pieces.append(begin(part, rims.at[side, :, pl.ds(first, count)], sems.at[k]))
            k += 1
    sides = [
        begin(circ_low, beside.at[0], sems.at[k]),
        begin(circ_high, beside.at[1], sems.at[k + 1]),
    ]
    k += 2
    for copy in pieces:
        copy.wait()

    def put(j, carry):
        for m in range(NCOMP):
            for c in range(chunks):
                buf[m, j, c, pl.ds(FIRST - 2, 2), :] = rims[0, m, j, pl.ds(2 * c, 2), :]
                buf[m, j, c, pl.ds(FIRST + 16, 2), :] = rims[1, m, j, pl.ds(2 * c, 2), :]
        return carry

    lax.fori_loop(0, planes + 4, put, 0)

    def place(j, carry):
        for m in range(NCOMP):
            for c in range(chunks):
                buf[m, j + 2, c, cells, :] = land[m, j, :, c * LANES : (c + 1) * LANES]
        return carry

    for copy in sides:
        copy.wait()

    def place_side(i, carry):
        for side, first in ((0, 0), (1, planes + 2)):
            for m in range(NCOMP):
                for c in range(chunks):
                    buf[m, first + i, c, cells, :] = beside[side, m, i, :, c * LANES : (c + 1) * LANES]
        return carry

    lax.fori_loop(0, 2, place_side, 0)

    def wall(first, count, zero_row, odd_row, from_row):
        def body(j, carry):
            for m in range(NCOMP):
                for c in range(chunks):
                    buf[m, j, c, pl.ds(zero_row, 1), :] = jnp.zeros((1, LANES), jnp.float32)
                    buf[m, j, c, pl.ds(odd_row, 1), :] = -buf[m, j, c, pl.ds(from_row, 1), :]
            return carry

        lax.fori_loop(first, first + count, body, 0)

    def walls(first, count):
        @pl.when(flags[0] == 1)
        def _():
            wall(first, count, FIRST - 1, FIRST - 2, FIRST)

        @pl.when(flags[1] == 1)
        def _():
            wall(first, count, FIRST + 16, FIRST + 17, FIRST + 15)

    def weights(coupling):
        own = 1.0 / (1.0 + 2.0 * coupling)
        side = coupling / (1.0 + 2.0 * coupling)
        return own * own + 2.0 * side * side, 2.0 * own * side, side * side

    def radial(j, carry):
        w0, w1, w2 = weights(RADIAL_COUPLING)
        for m in range(NCOMP):
            for c in range(chunks):
                x = [buf[m, j, c, pl.ds(FIRST + d, 16), :] for d in (-2, -1, 0, 1, 2)]
                mid[m, j, c] = w0 * x[2] + w1 * (x[1] + x[3]) + w2 * (x[0] + x[4])
        return carry

    def around(j, carry):
        w0, w1, w2 = weights(CIRC_COUPLING)
        for m in range(NCOMP):
            for c in range(chunks):
                x = [mid[m, j + d, c] for d in range(5)]
                done[m, j, :, pl.ds(c * LANES, LANES)] = (
                    w0 * x[2] + w1 * (x[1] + x[3]) + w2 * (x[0] + x[4])
                )
        return carry

    stores = []
    walls(0, 2)
    walls(planes + 2, 2)
    lax.fori_loop(0, 2, radial, 0)
    lax.fori_loop(planes + 2, planes + 4, radial, 0)
    for g in range(groups):
        copies[g].wait()
        lax.fori_loop(g * group, (g + 1) * group, place, 0)
        walls(g * group + 2, group)
        lax.fori_loop(g * group + 2, (g + 1) * group + 2, radial, 0)
        low = max(g * group - 2, 0)
        high = (g + 1) * group - 2 if g < groups - 1 else planes
        lax.fori_loop(low, high, around, 0)
        part = pl.ds(low, high - low)
        stores.append(begin(done.at[:, part], out.at[:, part], sems.at[k]))
        k += 1
    for copy in stores:
        copy.wait()


def smoothed(flags, field, halos):
    planes, rows, length = field.shape[1:]
    chunks = length // LANES
    f32 = jnp.float32
    return pl.pallas_call(
        smooth_kernel,
        out_shape=jax.ShapeDtypeStruct(field.shape, f32),
        in_specs=[smem()] + [hbm()] * 9,
        out_specs=hbm(),
        scratch_shapes=[
            pltpu.VMEM((NCOMP, planes + 4, chunks, ROWS, LANES), f32),
            pltpu.VMEM((NCOMP, planes + 4, chunks, rows, LANES), f32),
            pltpu.VMEM(field.shape, f32),
            pltpu.VMEM((2, NCOMP, planes + 4, 8, LANES), f32),
            pltpu.VMEM(field.shape, f32),
            pltpu.VMEM((2, NCOMP, 2, rows, length), f32),
            pltpu.SemaphoreType.DMA((2 * (planes // 8) + 8,)),
        ],
        compiler_params=pltpu.CompilerParams(vmem_limit_bytes=50 * MIB),
        name="smoothing",
    )(flags, field, *halos)


def ring(count):
    return [(i, (i + 1) % count) for i in range(count)]


def back(pairs):
    return [(b, a) for a, b in pairs]


def rims_of(count):
    first = [(i, i ^ 1) for i in range(count)]
    second = [(i, ((i + 1) ^ 1) - 1 if 0 < i < count - 1 else i) for i in range(count)]
    return first, second


def crossed(circ_pairs, rad_pairs, rads):
    return [(a * rads + c, b * rads + d) for a, b in circ_pairs for c, d in rad_pairs]


def on_device(state, time_source, pseudo_step, offsets, weights):
    cells = state[0]
    source = time_source[0]
    pseudo = pseudo_step[0]
    planes = cells.shape[1]
    circs = lax.axis_size("circ")
    rads = lax.axis_size("rad")
    row = lax.axis_index("row")
    rad = lax.axis_index("rad")
    flags = jnp.stack(
        [
            (rad == 0).astype(jnp.int32),
            (rad == rads - 1).astype(jnp.int32),
            row.astype(jnp.int32),
            (rad % 2).astype(jnp.int32),
            (lax.axis_index("circ") * planes).astype(jnp.int32),
        ]
    )
    up = ring(circs)
    down = back(up)
    pairs_a, pairs_b = rims_of(rads)

    own_a, own_b, circ_low, circ_high, face = edges(flags, cells)
    facing = lax.ppermute(face, "row", [(0, 1), (1, 0)])
    halo_circs = (lax.ppermute(circ_high, "circ", up), lax.ppermute(circ_low, "circ", down))
    halo_rads = (lax.ppermute(own_a, "rad", pairs_a), lax.ppermute(own_b, "rad", pairs_b))
    plane = lax.all_to_all(
        jnp.broadcast_to(facing[None], (circs, *facing.shape)), "circ", 0, 0, tiled=True
    )
    partial = inner_parts(flags, cells, source)

    field, circ_low, circ_high, rim_a, rim_b, low_a, low_b, high_a, high_b = outer_parts(
        flags,
        offsets,
        weights,
        cells,
        partial,
        pseudo,
        halo_circs,
        (own_a, own_b),
        halo_rads,
        plane,
    )
    both = ("circ", "rad")
    halos = (
        lax.ppermute(circ_high, "circ", up),
        lax.ppermute(circ_low, "circ", down),
        lax.ppermute(rim_a, "rad", pairs_a),
        lax.ppermute(rim_b, "rad", pairs_b),
        lax.ppermute(high_a, both, crossed(up, pairs_a, rads)),
        lax.ppermute(high_b, both, crossed(up, pairs_b, rads)),
        lax.ppermute(low_a, both, crossed(down, pairs_a, rads)),
        lax.ppermute(low_b, both, crossed(down, pairs_b, rads)),
    )
    return smoothed(flags, field, halos)[None]


def solution(mesh):
    return jax.shard_map(
        on_device,
        mesh=mesh,
        in_specs=(
            P("row", None, "circ", "rad", None),
            P("row", None, "circ", "rad", None),
            P("row", "circ", "rad", None),
            P("rad"),
            P("rad"),
        ),
        out_specs=P("row", None, "circ", "rad", None),
        check_vma=False,
    )
```
